8 devices in a mesh: dp: 1 (over z), tp: 2 (over y), sp: 4 (over x, core).
Axes of the slice: x: 2, y: 2, z: 1, core: 2. Of those that a mesh axis runs over, the one named last changes fastest.
Arguments:
- hidden: bfloat16 [512, 2048], P('dp')
- ln_gain: bfloat16 [2048], replicated
- ln_bias: bfloat16 [2048], replicated
- w_q: bfloat16 [2048, 2048], P(None, 'tp')
- w_k: bfloat16 [2048, 512], P(None, 'tp')
- w_v: bfloat16 [2048, 512], P(None, 'tp')
- w_o: bfloat16 [2048, 2048], P('tp')
- k_cache: bfloat16 [512, 1024, 8, 64], P('dp', 'sp', 'tp')
- v_cache: bfloat16 [512, 1024, 8, 64], P('dp', 'sp', 'tp')
- lengths: int32 [512], P('dp')
Outputs:
- output 1: bfloat16 [512, 2048], P('dp')
- output 2: bfloat16 [512, 8, 64], P('dp', 'tp')
- output 3: bfloat16 [512, 8, 64], P('dp', 'tp')
All inputs are finite; a program needn't handle non-finite values.
Results may differ from the reference program's by a relative error of at most 0.00379527.
Values sent between devices are 32-bit elements.
A program may use at most 1 GiB of HBM per device.

```python
import jax
import jax.numpy as jnp
from jax import lax

D_MODEL = 2048
Q_HEADS = 32
KV_HEADS = 8
HEAD_DIM = 64
BATCH_ROWS = 512
SEQ_LEN = 1024
GROUP_SIZE = Q_HEADS // KV_HEADS
ROT_DIM = HEAD_DIM // 2


def norm_one_plus(hidden, ln_gain, ln_bias):
    wide = hidden.astype(jnp.float32)
    row_mean = jnp.mean(wide, axis=-1, keepdims=True)
    centred = wide - row_mean
    row_var = jnp.mean(centred * centred, axis=-1, keepdims=True)
    scaled = centred * lax.rsqrt(row_var + 1e-5)
    return (scaled * (1.0 + ln_gain.astype(jnp.float32)) + ln_bias.astype(jnp.float32)).astype(jnp.bfloat16)


def rotate_first(head_vecs, rot_pos):
    half_rot = ROT_DIM // 2
    inv_freq = 10000.0 ** (-2.0 * jnp.arange(half_rot, dtype=jnp.float32) / ROT_DIM)
    rot_angle = rot_pos.astype(jnp.float32)[..., None] * inv_freq
    cos_part = jnp.cos(rot_angle)
    sin_part = jnp.sin(rot_angle)
    lead_part = head_vecs[..., :half_rot]
    tail_part = head_vecs[..., half_rot:ROT_DIM]
    return jnp.concatenate([lead_part * cos_part - tail_part * sin_part, tail_part * cos_part + lead_part * sin_part, head_vecs[..., ROT_DIM:]], axis=-1)


def setup_inputs(seed: int = 0, part: int = 0) -> dict:
    shared_keys = jax.random.split(jax.random.key(seed), 6)
    part_keys = jax.random.split(jax.random.fold_in(jax.random.key(seed), part), 6)
    q_width = Q_HEADS * HEAD_DIM
    kv_width = KV_HEADS * HEAD_DIM
    seg_count = 16
    seg_len = SEQ_LEN // seg_count
    hidden = jax.random.normal(part_keys[0], (BATCH_ROWS, D_MODEL), jnp.float32)
    ln_gain = 0.5 * jax.random.normal(shared_keys[0], (D_MODEL,), jnp.float32)
    ln_bias = 0.5 * jax.random.normal(shared_keys[1], (D_MODEL,), jnp.float32)
    w_q = jax.random.normal(shared_keys[2], (D_MODEL, q_width), jnp.float32) * D_MODEL ** -0.5
    w_k = jax.random.normal(shared_keys[3], (D_MODEL, kv_width), jnp.float32) * D_MODEL ** -0.5
    w_v = jax.random.normal(shared_keys[4], (D_MODEL, kv_width), jnp.float32) * D_MODEL ** -0.5
    w_o = jax.random.normal(shared_keys[5], (q_width, D_MODEL), jnp.float32) * q_width ** -0.5
    seg_shape = (BATCH_ROWS, seg_count, 1, KV_HEADS, HEAD_DIM)
    full_shape = (BATCH_ROWS, seg_count, seg_len, KV_HEADS, HEAD_DIM)
    cache_shape = (BATCH_ROWS, SEQ_LEN, KV_HEADS, HEAD_DIM)
    k_cache = (jax.random.normal(part_keys[1], seg_shape, jnp.float32) + jax.random.normal(part_keys[2], full_shape, jnp.float32)).reshape(cache_shape)
    v_cache = (1.5 * jax.random.normal(part_keys[3], seg_shape, jnp.float32) + 0.5 * jax.random.normal(part_keys[4], full_shape, jnp.float32)).reshape(cache_shape)
    lengths = jax.random.randint(part_keys[5], (BATCH_ROWS,), SEQ_LEN // 8, SEQ_LEN, dtype=jnp.int32)
    lengths = lengths.at[0].set(SEQ_LEN - 1).at[BATCH_ROWS - 1].set(SEQ_LEN // 8)
    return {'hidden': hidden.astype(jnp.bfloat16), 'ln_gain': ln_gain.astype(jnp.bfloat16), 'ln_bias': ln_bias.astype(jnp.bfloat16), 'w_q': w_q.astype(jnp.bfloat16), 'w_k': w_k.astype(jnp.bfloat16), 'w_v': w_v.astype(jnp.bfloat16), 'w_o': w_o.astype(jnp.bfloat16), 'k_cache': k_cache.astype(jnp.bfloat16), 'v_cache': v_cache.astype(jnp.bfloat16), 'lengths': lengths}


def reference(hidden, ln_gain, ln_bias, w_q, w_k, w_v, w_o, k_cache, v_cache, lengths):
    normed = norm_one_plus(hidden, ln_gain, ln_bias)
    q_proj = jnp.dot(normed, w_q, preferred_element_type=jnp.float32).reshape(BATCH_ROWS, KV_HEADS, GROUP_SIZE, HEAD_DIM)
    queries = rotate_first(q_proj, lengths[:, None, None]).astype(jnp.bfloat16)
    k_proj = jnp.dot(normed, w_k, preferred_element_type=jnp.float32).reshape(BATCH_ROWS, KV_HEADS, HEAD_DIM)
    k_new = rotate_first(k_proj, lengths[:, None]).astype(jnp.bfloat16)
    v_new = jnp.dot(normed, w_v, preferred_element_type=jnp.float32).astype(jnp.bfloat16).reshape(BATCH_ROWS, KV_HEADS, HEAD_DIM)
    score_scale = HEAD_DIM ** -0.5
    positions = jnp.arange(SEQ_LEN)

    def one_sequence(row_args):
        q_row, k_row, v_row, k_self, v_self, length = row_args
        q_wide = q_row.astype(jnp.float32)
        scores = jnp.einsum('kgd,skd->kgs', q_wide, k_row.astype(jnp.float32)) * score_scale
        scores = jnp.where(positions < length, scores, -jnp.inf)
        self_score = jnp.einsum('kgd,kd->kg', q_wide, k_self.astype(jnp.float32)) * score_scale
        row_max = jnp.maximum(jnp.max(scores, axis=-1), self_score)
        weights = jnp.exp(scores - row_max[..., None])
        self_weight = jnp.exp(self_score - row_max)
        weight_sum = jnp.sum(weights, axis=-1) + self_weight
        narrow_w = weights.astype(jnp.bfloat16).astype(jnp.float32)
        weighted = jnp.einsum('kgs,skd->kgd', narrow_w, v_row.astype(jnp.float32))
        weighted = weighted + self_weight[..., None] * v_self.astype(jnp.float32)[:, None, :]
        return (weighted / weight_sum[..., None]).astype(jnp.bfloat16)

    context = lax.map(one_sequence, (queries, k_cache, v_cache, k_new, v_new, lengths))
    attn_out = jnp.dot(context.reshape(BATCH_ROWS, Q_HEADS * HEAD_DIM), w_o, preferred_element_type=jnp.float32)
    out = (hidden.astype(jnp.float32) + attn_out).astype(jnp.bfloat16)
    return (out, k_new, v_new)
```

```python
import functools

import jax
import jax.numpy as jnp
import numpy as np
from jax import lax
from jax.experimental import pallas as pl
from jax.experimental.pallas import tpu as pltpu
from jax.sharding import PartitionSpec as P

MESH = pl.DeviceIdType.MESH
F32 = jnp.float32
BF16 = jnp.bfloat16
LOWEST = float(jnp.finfo(jnp.float32).min)

GROUP = 16
BLOCK = 4 * GROUP + 8
CHUNKS = (4, 8, 8, 8, 4)
SLOTS = 7
LAGS = (0, 2, 6, 10, 15, 17)
PITCH = 520


def attention_kernel(len_sm, len_row, inv_freq, gain, bias, hid_hbm, wq_hbm, wk_hbm, wv_hbm, wo_hbm, k_hbm, v_hbm,
                     out_hbm, knt_ref, vnt_ref,
                     hid, wq, wk, wv, wo, kring, vring, stage, cos_t, sin_t, qx, kn, vn,
                     own, part, send2, mine, recv2, ctx, proj, recv3, total,
                     ring_sem, load_sem, out_sem, send_sem, recv_sem):
    rows, width = hid.shape
    groups = rows // GROUP
    span = k_hbm.shape[2]
    tp = lax.axis_index('tp')
    sp = lax.axis_index('sp')
    x, core = sp // 2, sp % 2

    def ring_copy(g, slot):
        src = pl.ds(g * GROUP, GROUP)
        return (pltpu.make_async_copy(k_hbm.at[src], kring.at[slot], ring_sem.at[slot, 0]),
                pltpu.make_async_copy(v_hbm.at[src], vring.at[slot], ring_sem.at[slot, 1]))

    load_hid = pltpu.make_async_copy(hid_hbm, hid, load_sem.at[0])
    load_wk = pltpu.make_async_copy(wk_hbm, wk, load_sem.at[1])
    load_wv = pltpu.make_async_copy(wv_hbm, wv, load_sem.at[2])
    load_wq = pltpu.make_async_copy(wq_hbm, wq, load_sem.at[3])
    load_wo = pltpu.make_async_copy(wo_hbm, wo, load_sem.at[4])
    load_hid.start()
    load_wk.start()
    load_wv.start()
    load_wq.start()
    for g in range(SLOTS):
        for copy in ring_copy(g, g):
            copy.start()
    load_wo.start()

    def device(dx, dcore, dtp):
        return {'sp': (x ^ dx) * 2 + (core ^ dcore), 'tp': tp ^ dtp}

    barrier = pltpu.get_barrier_semaphore()
    for peer in ((0, 1, 0), (1, 0, 0), (0, 0, 1), (1, 0, 1)):
        pl.semaphore_signal(barrier, inc=1, device_id=device(*peer), device_id_type=MESH)

    angle = inv_freq[:, 0:1] * len_row[0:1, :].astype(F32)
    cos_a, sin_a = jnp.cos(angle), jnp.sin(angle)
    one, zero = jnp.ones((32, rows), F32), jnp.zeros((32, rows), F32)
    cos_full = jnp.concatenate([cos_a, cos_a, one] * 2, axis=0)
    sin_full = jnp.concatenate([-sin_a, sin_a, zero] * 2, axis=0)
    for blk in range(rows // 128):
        cut = slice(blk * 128, blk * 128 + 128)
        cos_t[cut, :] = cos_full[:, cut].T
        sin_t[cut, :] = sin_full[:, cut].T

    load_hid.wait()
    gain_f = 1.0 + gain[...].astype(F32)
    bias_f = bias[...].astype(F32)

    def norm(i, _):
        at = pl.ds(pl.multiple_of(i * 16, 16), 16)
        wide = hid[at, :].astype(F32)
        centred = wide - jnp.mean(wide, axis=-1, keepdims=True)
        var = jnp.mean(centred * centred, axis=-1, keepdims=True)
        stage[at, :] = (centred * lax.rsqrt(var + 1e-5) * gain_f + bias_f).astype(BF16)
        return 0

    lax.fori_loop(0, rows // 16, norm, 0)

    load_wk.wait()
    load_wv.wait()
    load_wq.wait()
    lane_rb = lax.broadcasted_iota(jnp.int32, (128, 128), 1)
    low_half = lane_rb < 64
    first_rot = (lane_rb % 64) < 16

    def rotate(u, cos_b, sin_b):
        partner = jnp.where(first_rot, pltpu.roll(u, 112, 1), pltpu.roll(u, 16, 1))
        return (u * cos_b + partner * sin_b).astype(BF16).astype(F32)

    def project(i, _):
        start = pl.multiple_of(i * 128, 128)
        at = pl.ds(start, 128)
        normed = stage[at, :]
        cos_b, sin_b = cos_t[at, :], sin_t[at, :]
        for head in range(4):
            q = jnp.dot(normed, wq[:, head * 256:head * 256 + 256], preferred_element_type=F32)
            for j in range(2):
                u = rotate(q[:, j * 128:j * 128 + 128], cos_b, sin_b) * 0.125
                swap = pltpu.roll(u, 64, 1)
                if head % 2 == 0:
                    a, b = jnp.where(low_half, u, 0.0), jnp.where(low_half, swap, 0.0)
                else:
                    a, b = jnp.where(low_half, 0.0, swap), jnp.where(low_half, 0.0, u)
                r = head * 4 + 2 * j
                qx[pl.ds(pl.multiple_of(r * PITCH + start, 8), 128), :] = a
                qx[pl.ds(pl.multiple_of((r + 1) * PITCH + start, 8), 128), :] = b
        kp = jnp.dot(normed, wk[...], preferred_element_type=F32)
        vp = jnp.dot(normed, wv[...], preferred_element_type=F32)
        for j in range(2):
            cut = slice(j * 128, j * 128 + 128)
            ku = rotate(kp[:, cut], cos_b, sin_b)
            vu = vp[:, cut].astype(BF16).astype(F32)
            kn[at, cut] = ku
            vn[at, cut] = vu
            knt_ref[cut, at] = ku.T.astype(BF16)
            vnt_ref[cut, at] = vu.T.astype(BF16)
        return 0

    lax.fori_loop(0, rows // 128, project, 0)
    pl.semaphore_wait(barrier, 4)

    lane = lax.broadcasted_iota(jnp.int32, (8, 128), 1)
    row = lax.broadcasted_iota(jnp.int32, (8, 128), 0)
    low = lane < 64
    keep_w = (row < 4) == low
    stat = lane % 8
    even = (lane % 2) == 0
    keep_s = (row < 4) == even
    pair_of = lane // 8
    pos = lax.broadcasted_iota(jnp.int32, (16, span), 1)
    zero8 = jnp.zeros((8, 128), F32)
    first_pos = sp * span

    def pack(a, b, pick, keep):
        same = jnp.where(pick, a, b)
        other = pltpu.roll(jnp.where(pick, b, a), 4, 0)
        return jnp.where(keep, same, other)

    def one_sequence(b, keys, values):
        qa = qx[pl.ds(b, 8, stride=PITCH), :]
        qb = qx[pl.ds(b + 8 * PITCH, 8, stride=PITCH), :]
        q = jnp.concatenate([jnp.concatenate([qa, zero8], 1), jnp.concatenate([zero8, qb], 1)], 0).astype(BF16)
        s = jnp.dot(q, keys, preferred_element_type=F32)
        left = len_sm[b] - first_pos
        s = jnp.where(pos < left, s, -jnp.inf)
        k_self, v_self = kn[pl.ds(b, 1), :], vn[pl.ds(b, 1), :]
        s_self = jnp.sum(jnp.concatenate([qa * k_self[:, :128], qb * k_self[:, 128:]], 0), axis=1, keepdims=True)
        owner = jnp.logical_and(left >= 0, left < span)
        s_self = s_self + jnp.where(owner, 0.0, -jnp.inf)
        top = jnp.maximum(jnp.maximum(jnp.max(s, axis=1, keepdims=True), s_self), LOWEST)
        w = jnp.exp(s - top)
        w_self = jnp.exp(s_self - top)
        denom = jnp.sum(w, axis=1, keepdims=True) + w_self
        ctx_b = lax.dot_general(w.astype(BF16), values, (((1,), (1,)), ((), ())), preferred_element_type=F32)
        ca = ctx_b[:8, :128] + w_self[:8] * v_self[:, :128]
        cb = ctx_b[8:, 128:] + w_self[8:] * v_self[:, 128:]
        stats = jnp.where(stat < 2, top[:8], jnp.where(stat < 4, top[8:], jnp.where(stat < 6, denom[:8], denom[8:])))
        return ca, cb, stats

    def attend(g, slot):
        tile = zero8
        for p in range(GROUP // 2):
            b = g * GROUP + 2 * p
            e = one_sequence(b, kring[slot, 2 * p], vring[slot, 2 * p])
            o = one_sequence(b + 1, kring[slot, 2 * p + 1], vring[slot, 2 * p + 1])
            own[g, 8 * p:8 * p + 8, 0:128] = pack(e[0], o[0], low, keep_w)
            own[g, 8 * p:8 * p + 8, 128:256] = pack(e[1], o[1], low, keep_w)
            tile = jnp.where(pair_of == p, pack(e[2], o[2], even, keep_s), tile)
        own[g, 4 * GROUP:BLOCK, 0:128] = tile
        own[g, 4 * GROUP:BLOCK, 128:256] = zero8

    is_top = stat < 4

    def spread(f, p, t):
        c = p * 8 + 2 * t
        return jnp.where(low, jnp.broadcast_to(f[:, c:c + 1], (8, 128)), jnp.broadcast_to(f[:, c + 1:c + 2], (8, 128)))

    def merge(a_ref, a, b_ref, b, emit):
        sa, sb = a_ref[a, 4 * GROUP:BLOCK, 0:128], b_ref[b, 4 * GROUP:BLOCK, 0:128]
        top = jnp.maximum(sa, sb)
        fa, fb = jnp.exp(sa - top), jnp.exp(sb - top)
        denom = sa * pltpu.roll(fa, 4, 1) + sb * pltpu.roll(fb, 4, 1)
        emit(None, None, jnp.where(is_top, top, denom))
        for p in range(GROUP // 2):
            r = slice(8 * p, 8 * p + 8)
            for t in range(2):
                c = slice(t * 128, t * 128 + 128)
                w = a_ref[a, r, c] * spread(fa, p, t) + b_ref[b, r, c] * spread(fb, p, t)
                emit(r, c, w / spread(denom, p, 2 + t) if emit.final else w)

    def store_to(ref, index, final):
        def emit(r, c, value):
            if r is None:
                if not final:
                    ref[index, 4 * GROUP:BLOCK, 0:128] = value
                    ref[index, 4 * GROUP:BLOCK, 128:256] = zero8
            elif final:
                base = c.start // 128 * (ref.shape[0] // 2)
                ref[pl.ds(pl.multiple_of(base + index * 4 * GROUP + r.start, 8), 8), :] = value
            else:
                ref[index, r, c] = value
        emit.final = final
        return emit

    starts = [sum(CHUNKS[:c]) for c in range(len(CHUNKS))]

    def remote(c, kind, src, dst, peer):
        return pltpu.make_async_remote_copy(
            src_ref=src, dst_ref=dst, send_sem=send_sem.at[c, kind], recv_sem=recv_sem.at[c, kind],
            device_id=device(*peer), device_id_type=MESH)

    def quarter(c):
        return CHUNKS[c] // 4

    def to_partner(c):
        n = quarter(c)
        src = own.at[pl.ds(starts[c] + (1 - core) * 2 * n, 2 * n)]
        return remote(c, 0, src, part.at[pl.ds(starts[c] // 2, 2 * n)], (0, 1, 0))

    def over_x(c):
        at = pl.ds(starts[c] // 4, quarter(c))
        return remote(c, 1, send2.at[at], recv2.at[at], (1, 0, 0))

    def over_y(c):
        half = quarter(c) * GROUP // 2
        src = proj.at[pl.ds(pl.multiple_of(starts[c] // 4 * GROUP + (1 - tp) * half, 8), half)]
        return remote(c, 2, src, recv3.at[pl.ds(starts[c] // 4 * GROUP // 2, half)], (0, 0, 1))

    def home(c, dx, dcore, dtp):
        half = quarter(c) * GROUP // 2
        index = ((core ^ dcore) * 2 + (x ^ dx)) * 2 + (tp ^ dtp)
        return total.at[pl.ds(pl.multiple_of(starts[c] * GROUP + index * half, 8), half)]

    def spread_own(c, kind, peer):
        return remote(c, kind, home(c, 0, 0, 0), home(c, 0, 0, 0), peer)

    def forward(c, kind, origin):
        return remote(c, kind, home(c, *origin), home(c, *origin), (0, 1, 0))

    direct = ((3, (0, 1, 0)), (4, (1, 0, 0)), (5, (0, 0, 1)), (6, (1, 0, 1)))
    passed = ((7, (1, 0, 0)), (8, (0, 0, 1)), (9, (1, 0, 1)))

    def step1(c):
        to_partner(c).start()

    def step2(c):
        n = quarter(c)
        to_partner(c).wait_recv()
        for dx in (1, 0):
            side = x ^ dx

            def body(i, _):
                out = (send2, mine)[1 - dx]
                merge(own, starts[c] + (core * 2 + side) * n + i, part, starts[c] // 2 + side * n + i,
                      store_to(out, starts[c] // 4 + i, False))
                return 0

            lax.fori_loop(0, n, body, 0)
            if dx == 1:
                over_x(c).start()

    def step3(c):
        n = quarter(c)
        if c == 0:
            load_wo.wait()
        over_x(c).wait_recv()

        def body(i, _):
            at = starts[c] // 4 + i
            merge(mine, at, recv2, at, store_to(ctx, i, True))
            return 0

        lax.fori_loop(0, n, body, 0)
        m = n * GROUP
        side = ctx.shape[0] // 2
        lhs = [jnp.concatenate([ctx[pl.ds(t * side + g, m, stride=4), :] for t in range(2)], 1).astype(BF16) for g in range(4)]
        for col in range(width // 256):
            cut = slice(col * 256, col * 256 + 256)
            acc = None
            for g in range(4):
                rhs = jnp.concatenate([wo[h * 256 + g * 64:h * 256 + g * 64 + 64, cut] for h in range(4)], 0)
                term = jnp.dot(lhs[g], rhs, preferred_element_type=F32)
                acc = term if acc is None else acc + term
            proj[starts[c] // 4 * GROUP:starts[c] // 4 * GROUP + m, cut] = acc
        over_y(c).start()

    def step4(c):
        half = quarter(c) * GROUP // 2
        over_y(c).wait_recv()
        src = pl.ds(pl.multiple_of(starts[c] // 4 * GROUP + tp * half, 8), half)
        other = starts[c] // 4 * GROUP // 2
        home(c, 0, 0, 0)[...] = proj[src, :] + recv3[other:other + half, :]
        for kind, peer in direct:
            spread_own(c, kind, peer).start()

    def step5(c):
        for (kind, origin), (arrived, _) in zip(passed, direct[1:]):
            spread_own(c, arrived, (0, 1, 0)).wait_recv()
            forward(c, kind, origin).start()

    def out_copy(c):
        at = pl.ds(starts[c] * GROUP, CHUNKS[c] * GROUP)
        return pltpu.make_async_copy(stage.at[at], out_hbm.at[at], out_sem.at[c])

    def step6(c):
        spread_own(c, 3, (0, 1, 0)).wait_recv()
        for kind, origin in passed:
            forward(c, kind, origin).wait_recv()

        def body(i, _):
            at = pl.ds(pl.multiple_of((starts[c] + i) * GROUP, GROUP), GROUP)
            stage[at, :] = (hid[at, :].astype(F32) + total[at, :]).astype(BF16)
            return 0

        lax.fori_loop(0, CHUNKS[c], body, 0)
        out_copy(c).start()

    steps = (step1, step2, step3, step4, step5, step6)
    events = sorted((starts[c] + CHUNKS[c] - 1 + LAGS[i], c, i) for c in range(len(CHUNKS)) for i in range(6))

    def loop(g, _):
        slot = lax.rem(g, SLOTS)
        for copy in ring_copy(g, slot):
            copy.wait()
        attend(g, slot)

        @pl.when(g + SLOTS < groups)
        def _():
            for copy in ring_copy(g + SLOTS, slot):
                copy.start()

        for when, c, i in events:
            if when < groups:
                pl.when(g == when)(functools.partial(steps[i], c))
        return 0

    lax.fori_loop(0, groups, loop, 0)
    for when, c, i in events:
        if when >= groups:
            steps[i](c)
    for c in range(len(CHUNKS)):
        to_partner(c).wait_send()
        over_x(c).wait_send()
        over_y(c).wait_send()
        for kind, peer in direct:
            spread_own(c, kind, peer).wait_send()
        for kind, origin in passed:
            forward(c, kind, origin).wait_send()
        out_copy(c).wait()


def solution(mesh):
    def local_step(hidden, ln_gain, ln_bias, w_q, w_k, w_v, w_o, k_cache, v_cache, lengths):
        rows, span, kv_local, head_dim = k_cache.shape
        width = hidden.shape[1]
        kv_width = kv_local * head_dim
        q_width = w_q.shape[1]
        groups = rows // GROUP
        keys = jnp.transpose(k_cache, (0, 2, 3, 1)).reshape(rows, kv_width, span)
        values = jnp.transpose(v_cache, (0, 2, 3, 1)).reshape(rows, kv_width, span)
        half_rot = head_dim // 4
        inv_freq = np.power(10000.0, -2.0 * np.arange(half_rot) / (2 * half_rot)).astype(np.float32)
        inv_freq = jnp.asarray(np.broadcast_to(inv_freq[:, None], (half_rot, 128)).copy())
        vmem = pl.BlockSpec(memory_space=pltpu.VMEM)
        smem = pl.BlockSpec(memory_space=pltpu.SMEM)
        hbm = pl.BlockSpec(memory_space=pl.ANY)
        n = len(CHUNKS)
        out, k_new, v_new = pl.pallas_call(
            attention_kernel,
            out_shape=(jax.ShapeDtypeStruct((rows, width), BF16),
                       jax.ShapeDtypeStruct((kv_width, rows), BF16),
                       jax.ShapeDtypeStruct((kv_width, rows), BF16)),
            in_specs=[smem, vmem, vmem, vmem, vmem] + [hbm] * 7,
            out_specs=(hbm, vmem, vmem),
            scratch_shapes=[
                pltpu.VMEM((rows, width), BF16),
                pltpu.VMEM((width, q_width), BF16),
                pltpu.VMEM((width, kv_width), BF16),
                pltpu.VMEM((width, kv_width), BF16),
                pltpu.VMEM((q_width, width), BF16),
                pltpu.VMEM((SLOTS, GROUP, kv_width, span), BF16),
                pltpu.VMEM((SLOTS, GROUP, kv_width, span), BF16),
                pltpu.VMEM((rows, width), BF16),
                pltpu.VMEM((rows, 128), F32),
                pltpu.VMEM((rows, 128), F32),
                pltpu.VMEM((16 * PITCH, 128), F32),
                pltpu.VMEM((rows, kv_width), F32),
                pltpu.VMEM((rows, kv_width), F32),
                pltpu.VMEM((groups, BLOCK, 256), F32),
                pltpu.VMEM((groups // 2, BLOCK, 256), F32),
                pltpu.VMEM((groups // 4, BLOCK, 256), F32),
                pltpu.VMEM((groups // 4, BLOCK, 256), F32),
                pltpu.VMEM((groups // 4, BLOCK, 256), F32),
                pltpu.VMEM((2 * (max(CHUNKS) // 4) * GROUP * 4, 128), F32),
                pltpu.VMEM((rows // 4, width), F32),
                pltpu.VMEM((rows // 8, width), F32),
                pltpu.VMEM((rows, width), F32),
                pltpu.SemaphoreType.DMA((SLOTS, 2)),
                pltpu.SemaphoreType.DMA((5,)),
                pltpu.SemaphoreType.DMA((n,)),
                pltpu.SemaphoreType.DMA((n, 10)),
                pltpu.SemaphoreType.DMA((n, 10)),
            ],
            compiler_params=pltpu.CompilerParams(
                collective_id=0, has_side_effects=True, vmem_limit_bytes=67043328),
        )(lengths, lengths.reshape(1, rows), inv_freq, ln_gain.reshape(1, width), ln_bias.reshape(1, width),
          hidden, w_q, w_k, w_v, w_o, keys, values)
        k_new = jnp.transpose(k_new.reshape(kv_local, head_dim, rows), (2, 0, 1))
        v_new = jnp.transpose(v_new.reshape(kv_local, head_dim, rows), (2, 0, 1))
        return out, k_new, v_new

    row_spec = P('dp', None)
    cache_spec = P('dp', 'sp', 'tp', None)
    head_spec = P('dp', 'tp', None)
    return jax.shard_map(local_step, mesh=mesh, in_specs=(row_spec, P(None), P(None), P(None, 'tp'), P(None, 'tp'), P(None, 'tp'), P('tp', None), cache_spec, cache_spec, P('dp')), out_specs=(row_spec, head_spec, head_spec), check_vma=False)
```

```python
import functools
import math

import jax
import jax.numpy as jnp
import numpy as np
from jax import lax
from jax.experimental import pallas as pl
from jax.experimental.pallas import tpu as pltpu
from jax.sharding import PartitionSpec as P

MESH = pl.DeviceIdType.MESH
F32 = jnp.float32
BF16 = jnp.bfloat16
LOWEST = float(jnp.finfo(jnp.float32).min)

GROUP = 16
BLOCK = 4 * GROUP + 8
DIRECT = (3, 4)
CHUNKS = (8, 8, 8, 4, 4)
SLOTS = 7
LAGS = (0, 0.9, 2.9, 4.8, 6.8, 7.7, 8.6)
PITCH = 520


def attention_kernel(len_sm, len_row, inv_freq, gain, bias, hid_hbm, wq_hbm, wk_hbm, wv_hbm, wo_hbm, k_hbm, v_hbm,
                     out_hbm, knt_ref, vnt_ref,
                     hid, wq, wk, wv, wo, kring, vring, stage, cos_t, sin_t, qx, kn, vn,
                     prob, self_w, own, part, send2, mine, recv2, ctx, proj, recv3, total,
                     ring_sem, load_sem, out_sem, send_sem, recv_sem):
    rows, width = hid.shape
    groups = rows // GROUP
    span = k_hbm.shape[2]
    tp = lax.axis_index('tp')
    sp = lax.axis_index('sp')
    x, core = sp // 2, sp % 2

    def ring_copy(which, g):
        slot = lax.rem(g, SLOTS)
        src, ring = ((k_hbm, kring), (v_hbm, vring))[which]
        return pltpu.make_async_copy(src.at[pl.ds(g * GROUP, GROUP)], ring.at[slot], ring_sem.at[slot, which])

    blocks = rows // 128

    def load_hid(i):
        at = pl.ds(i * 128, 128)
        return pltpu.make_async_copy(hid_hbm.at[at], hid.at[at], load_sem.at[4 + i])

    load_wk = pltpu.make_async_copy(wk_hbm, wk, load_sem.at[0])
    load_wv = pltpu.make_async_copy(wv_hbm, wv, load_sem.at[1])
    load_wq = pltpu.make_async_copy(wq_hbm, wq, load_sem.at[2])
    load_wo = pltpu.make_async_copy(wo_hbm, wo, load_sem.at[3])
    for i in range(blocks):
        load_hid(i).start()
    load_wq.start()
    load_wk.start()
    load_wv.start()
    for which in range(2):
        ring_copy(which, 0).start()

    def device(dx, dcore, dtp):
        return {'sp': (x ^ dx) * 2 + (core ^ dcore), 'tp': tp ^ dtp}

    barrier = pltpu.get_barrier_semaphore()
    for peer in ((0, 1, 0), (1, 0, 0), (0, 0, 1), (1, 0, 1)):
        pl.semaphore_signal(barrier, inc=1, device_id=device(*peer), device_id_type=MESH)

    angle = inv_freq[:, 0:1] * len_row[0:1, :].astype(F32)
    cos_a, sin_a = jnp.cos(angle), jnp.sin(angle)
    one, zero = jnp.ones((32, rows), F32), jnp.zeros((32, rows), F32)
    cos_full = jnp.concatenate([cos_a, cos_a, one] * 2, axis=0)
    sin_full = jnp.concatenate([-sin_a, sin_a, zero] * 2, axis=0)
    for blk in range(rows // 128):
        cut = slice(blk * 128, blk * 128 + 128)
        cos_t[cut, :] = cos_full[:, cut].T
        sin_t[cut, :] = sin_full[:, cut].T

    with jax.named_scope('load_hid'):
        for i in range(blocks):
            load_hid(i).wait()
    for g in range(1, SLOTS):
        for which in range(2):
            ring_copy(which, g).start()
    load_wo.start()
    gain_f, bias_f = gain[...].astype(F32), bias[...].astype(F32)
    gain_f = 1.0 + jnp.concatenate([gain_f[i:i + 1] for i in range(width // 128)], 1)
    bias_f = jnp.concatenate([bias_f[i:i + 1] for i in range(width // 128)], 1)

    def norm(i, _):
        for j in range(4):
            at = pl.ds(pl.multiple_of(i * 64 + j * 16, 16), 16)
            wide = hid[at, :].astype(F32)
            centred = wide - jnp.mean(wide, axis=-1, keepdims=True)
            var = jnp.mean(centred * centred, axis=-1, keepdims=True)
            stage[at, :] = (centred * lax.rsqrt(var + 1e-5) * gain_f + bias_f).astype(BF16)
        return 0

    with jax.named_scope('norm'):
        lax.fori_loop(0, rows // 64, norm, 0)

    with jax.named_scope('load_w'):
        load_wk.wait()
        load_wv.wait()
        load_wq.wait()
    lane_rb = lax.broadcasted_iota(jnp.int32, (128, 128), 1)
    low_half = lane_rb < 64
    first_rot = (lane_rb % 64) < 16

    def rotate(u, cos_b, sin_b):
        partner = jnp.where(first_rot, pltpu.roll(u, 112, 1), pltpu.roll(u, 16, 1))
        return (u * cos_b + partner * sin_b).astype(BF16).astype(F32)

    def project(i, _):
        start = pl.multiple_of(i * 128, 128)
        at = pl.ds(start, 128)
        normed = stage[at, :]
        cos_b, sin_b = cos_t[at, :], sin_t[at, :]
        for head in range(4):
            q = jnp.dot(normed, wq[:, head * 256:head * 256 + 256], preferred_element_type=F32)
            for j in range(2):
                u = rotate(q[:, j * 128:j * 128 + 128], cos_b, sin_b) * 0.125
                swap = pltpu.roll(u, 64, 1)
                if head % 2 == 0:
                    a, b = jnp.where(low_half, u, 0.0), jnp.where(low_half, swap, 0.0)
                else:
                    a, b = jnp.where(low_half, 0.0, swap), jnp.where(low_half, 0.0, u)
                r = head * 4 + 2 * j
                qx[pl.ds(pl.multiple_of(r * PITCH + start, 8), 128), :] = a
                qx[pl.ds(pl.multiple_of((r + 1) * PITCH + start, 8), 128), :] = b
        kp = jnp.dot(normed, wk[...], preferred_element_type=F32)
        vp = jnp.dot(normed, wv[...], preferred_element_type=F32)
        for j in range(2):
            cut = slice(j * 128, j * 128 + 128)
            ku = rotate(kp[:, cut], cos_b, sin_b)
            vu = vp[:, cut].astype(BF16).astype(F32)
            kn[at, cut] = ku
            vn[at, cut] = vu
            knt_ref[cut, at] = ku.T.astype(BF16)
            vnt_ref[cut, at] = vu.T.astype(BF16)
        return 0

    with jax.named_scope('project'):
        lax.fori_loop(0, rows // 128, project, 0)
    with jax.named_scope('barrier'):
        pl.semaphore_wait(barrier, 4)

    lane = lax.broadcasted_iota(jnp.int32, (8, 128), 1)
    row = lax.broadcasted_iota(jnp.int32, (8, 128), 0)
    low = lane < 64
    keep_w = (row < 4) == low
    stat = lane % 8
    even = (lane % 2) == 0
    keep_s = (row < 4) == even
    pair_of = lane // 8
    pos = lax.broadcasted_iota(jnp.int32, (16, span), 1)
    zero8 = jnp.zeros((8, 128), F32)
    first_pos = sp * span

    def pack(a, b, pick, keep):
        same = jnp.where(pick, a, b)
        other = pltpu.roll(jnp.where(pick, b, a), 4, 0)
        return jnp.where(keep, same, other)

    def queries(b):
        qa = qx[pl.ds(b, 8, stride=PITCH), :]
        qb = qx[pl.ds(b + 8 * PITCH, 8, stride=PITCH), :]
        return qa, qb

    def score(g, j):
        qa, qb = queries(g * GROUP + j)
        q = jnp.concatenate([jnp.concatenate([qa, zero8], 1), jnp.concatenate([zero8, qb], 1)], 0).astype(BF16)
        return jnp.dot(q, kring[lax.rem(g, SLOTS), j], preferred_element_type=F32)

    def weigh(g, side, j, s):
        b = g * GROUP + j
        qa, qb = queries(b)
        left = len_sm[b] - first_pos
        s = jnp.where(pos < left, s, -jnp.inf)
        k_self = kn[pl.ds(b, 1), :]
        s_self = jnp.sum(jnp.concatenate([qa * k_self[:, :128], qb * k_self[:, 128:]], 0), axis=1, keepdims=True)
        owner = jnp.logical_and(left >= 0, left < span)
        s_self = s_self + jnp.where(owner, 0.0, -jnp.inf)
        top = jnp.maximum(jnp.maximum(jnp.max(s, axis=1, keepdims=True), s_self), LOWEST)
        w = jnp.exp(s - top)
        w_self = jnp.exp(s_self - top)
        denom = jnp.sum(w, axis=1, keepdims=True) + w_self
        prob[side, 16 * j:16 * j + 16, :] = w.astype(BF16)
        self_w[side, 16 * j:16 * j + 16, :] = jnp.broadcast_to(w_self, (16, 128))
        return jnp.where(stat < 2, top[:8], jnp.where(stat < 4, top[8:], jnp.where(stat < 6, denom[:8], denom[8:])))

    def value(g, side, j):
        v_self = vn[pl.ds(g * GROUP + j, 1), :]
        part_b = lax.dot_general(prob[side, 16 * j:16 * j + 16, :], vring[lax.rem(g, SLOTS), j],
                                 (((1,), (1,)), ((), ())), preferred_element_type=F32)
        ca = part_b[:8, :128] + self_w[side, 16 * j:16 * j + 8, :] * v_self[:, :128]
        cb = part_b[8:, 128:] + self_w[side, 16 * j + 8:16 * j + 16, :] * v_self[:, 128:]
        return ca, cb

    def attend(score_g, value_g):
        if score_g is not None:
            g, side = score_g
            scores = [score(g, j) for j in range(GROUP)]
            tile = zero8
        for p in range(GROUP // 2):
            if value_g is not None:
                v, vside = value_g
                e, o = value(v, vside, 2 * p), value(v, vside, 2 * p + 1)
                own[v, 8 * p:8 * p + 8, 0:128] = pack(e[0], o[0], low, keep_w)
                own[v, 8 * p:8 * p + 8, 128:256] = pack(e[1], o[1], low, keep_w)
            if score_g is not None:
                e = weigh(g, side, 2 * p, scores[2 * p])
                o = weigh(g, side, 2 * p + 1, scores[2 * p + 1])
                tile = jnp.where(pair_of == p, pack(e, o, even, keep_s), tile)
        if score_g is not None:
            own[g, 4 * GROUP:BLOCK, 0:128] = tile
            own[g, 4 * GROUP:BLOCK, 128:256] = zero8

    is_top = stat < 4

    def spread(f, p, t):
        c = p * 8 + 2 * t
        return jnp.where(low, jnp.broadcast_to(f[:, c:c + 1], (8, 128)), jnp.broadcast_to(f[:, c + 1:c + 2], (8, 128)))

    def merge(a_ref, a, b_ref, b, emit):
        sa, sb = a_ref[a, 4 * GROUP:BLOCK, 0:128], b_ref[b, 4 * GROUP:BLOCK, 0:128]
        top = jnp.maximum(sa, sb)
        fa, fb = jnp.exp(sa - top), jnp.exp(sb - top)
        denom = sa * pltpu.roll(fa, 4, 1) + sb * pltpu.roll(fb, 4, 1)
        emit(None, None, jnp.where(is_top, top, denom))
        for p in range(GROUP // 2):
            r = slice(8 * p, 8 * p + 8)
            for t in range(2):
                c = slice(t * 128, t * 128 + 128)
                w = a_ref[a, r, c] * spread(fa, p, t) + b_ref[b, r, c] * spread(fb, p, t)
                emit(r, c, w / spread(denom, p, 2 + t) if emit.final else w)

    def store_to(ref, index, final):
        def emit(r, c, value):
            if r is None:
                if not final:
                    ref[index, 4 * GROUP:BLOCK, 0:128] = value
                    ref[index, 4 * GROUP:BLOCK, 128:256] = zero8
            elif final:
                base = c.start // 128 * (ref.shape[0] // 2)
                ref[pl.ds(pl.multiple_of(base + index * 4 * GROUP + r.start, 8), 8), :] = value
            else:
                ref[index, r, c] = value
        emit.final = final
        return emit

    starts = [sum(CHUNKS[:c]) for c in range(len(CHUNKS))]

    def remote(c, kind, src, dst, peer):
        return pltpu.make_async_remote_copy(
            src_ref=src, dst_ref=dst, send_sem=send_sem.at[c, kind], recv_sem=recv_sem.at[c, kind],
            device_id=device(*peer), device_id_type=MESH)

    def quarter(c):
        return CHUNKS[c] // 4

    def to_partner(c):
        n = quarter(c)
        src = own.at[pl.ds(starts[c] + (1 - core) * 2 * n, 2 * n)]
        return remote(c, 0, src, part.at[pl.ds(starts[c] // 2, 2 * n)], (0, 1, 0))

    def over_x(c):
        at = pl.ds(starts[c] // 4, quarter(c))
        return remote(c, 1, send2.at[at], recv2.at[at], (1, 0, 0))

    def over_y(c):
        half = quarter(c) * GROUP // 2
        src = proj.at[pl.ds(pl.multiple_of(starts[c] // 4 * GROUP + (1 - tp) * half, 8), half)]
        return remote(c, 2, src, recv3.at[pl.ds(starts[c] // 4 * GROUP // 2, half)], (0, 0, 1))

    def home(c, dx, dcore, dtp):
        half = quarter(c) * GROUP // 2
        index = ((core ^ dcore) * 2 + (x ^ dx)) * 2 + (tp ^ dtp)
        return total.at[pl.ds(pl.multiple_of(starts[c] * GROUP + index * half, 8), half)]

    def spread_own(c, kind, peer):
        return remote(c, kind, home(c, 0, 0, 0), home(c, 0, 0, 0), peer)

    def forward(c, kind, origin):
        return remote(c, kind, home(c, *origin), home(c, *origin), (0, 1, 0))

    passed = ((7, (1, 0, 0)), (8, (0, 0, 1)), (9, (1, 0, 1)))
    first_peer, other_peer = (1 - core, 0, core), (core, 0, 1 - core)

    def sent(c):
        copies = [spread_own(c, 4, (1, 0, 0)), spread_own(c, 5, (0, 0, 1)), spread_own(c, 3, (0, 1, 0))]
        if c in DIRECT:
            copies.append(spread_own(c, 6, (1, 0, 1)))
        return copies

    def relay(c):
        return remote(c, 6, home(c, *first_peer), home(c, *first_peer), other_peer)

    def step1(c):
        to_partner(c).start()

    def step2(c):
        n = quarter(c)
        with jax.named_scope(f'wait2_{c}'):
            to_partner(c).wait_recv()
        for dx in (1, 0):
            side = x ^ dx

            def body(i, _):
                out = (send2, mine)[1 - dx]
                merge(own, starts[c] + (core * 2 + side) * n + i, part, starts[c] // 2 + side * n + i,
                      store_to(out, starts[c] // 4 + i, False))
                return 0

            lax.fori_loop(0, n, body, 0)
            if dx == 1:
                over_x(c).start()

    def step3(c):
        n = quarter(c)
        if c == 0:
            load_wo.wait()
        with jax.named_scope(f'wait3_{c}'):
            over_x(c).wait_recv()

        def body(i, _):
            at = starts[c] // 4 + i
            merge(mine, at, recv2, at, store_to(ctx, i, True))
            return 0

        lax.fori_loop(0, n, body, 0)
        m = n * GROUP
        side = ctx.shape[0] // 2
        lhs = [jnp.concatenate([ctx[pl.ds(t * side + g, m, stride=4), :] for t in range(2)], 1).astype(BF16) for g in range(4)]
        for col in range(width // 256):
            cut = slice(col * 256, col * 256 + 256)
            acc = None
            for g in range(4):
                rhs = jnp.concatenate([wo[h * 256 + g * 64:h * 256 + g * 64 + 64, cut] for h in range(4)], 0)
                term = jnp.dot(lhs[g], rhs, preferred_element_type=F32)
                acc = term if acc is None else acc + term
            proj[starts[c] // 4 * GROUP:starts[c] // 4 * GROUP + m, cut] = acc
        over_y(c).start()

    def step4(c):
        half = quarter(c) * GROUP // 2
        with jax.named_scope(f'wait4_{c}'):
            over_y(c).wait_recv()
        src = pl.ds(pl.multiple_of(starts[c] // 4 * GROUP + tp * half, 8), half)
        other = starts[c] // 4 * GROUP // 2
        home(c, 0, 0, 0)[...] = proj[src, :] + recv3[other:other + half, :]
        for copy in sent(c):
            copy.start()

    def step5(c):
        with jax.named_scope(f'wait5_{c}'):
            spread_own(c, 4 + core, (0, 1, 0)).wait_recv()
        if c not in DIRECT:
            relay(c).start()
        forward(c, 7 + core, first_peer).start()

    def step6(c):
        with jax.named_scope(f'wait6a_{c}'):
            spread_own(c, 5 - core, (0, 1, 0)).wait_recv()
        forward(c, 8 - core, other_peer).start()
        with jax.named_scope(f'wait6b_{c}'):
            spread_own(c, 6, (0, 1, 0)).wait_recv()
        forward(c, 9, (1, 0, 1)).start()

    def out_copy(c):
        at = pl.ds(starts[c] * GROUP, CHUNKS[c] * GROUP)
        return pltpu.make_async_copy(stage.at[at], out_hbm.at[at], out_sem.at[c])

    def step7(c):
        with jax.named_scope(f'wait7_{c}'):
            spread_own(c, 3, (0, 1, 0)).wait_recv()
            for kind, origin in passed:
                forward(c, kind, origin).wait_recv()

        def body(i, _):
            at = pl.ds(pl.multiple_of((starts[c] + i) * GROUP, GROUP), GROUP)
            stage[at, :] = (hid[at, :].astype(F32) + total[at, :]).astype(BF16)
            return 0

        lax.fori_loop(0, CHUNKS[c], body, 0)
        out_copy(c).start()

    def scoped(i, c):
        with jax.named_scope(f'step{i + 1}_{c}'):
            steps[i](c)

    steps = (step1, step2, step3, step4, step5, step6, step7)
    events = sorted(((starts[c] + CHUNKS[c]) / 2 - 1 + LAGS[i], c, i) for c in range(len(CHUNKS)) for i in range(7))

    def wait_for(keys, values):
        for g in keys:
            ring_copy(0, g).wait()
        for g in values:
            ring_copy(1, g).wait()

    def refill(which, g):
        @pl.when(g + SLOTS < groups)
        def _():
            ring_copy(which, g + SLOTS).start()

    wait_for((0,), ())
    with jax.named_scope('attend'):
        attend((0, 0), None)
    refill(0, 0)

    def loop(i, _):
        g = 2 * i
        with jax.named_scope('ring_wait'):
            wait_for((g + 1, g + 2), (g, g + 1))
        with jax.named_scope('attend'):
            attend((g + 1, 1), (g, 0))
            attend((g + 2, 0), (g + 1, 1))
        refill(0, g + 1)
        refill(1, g)
        refill(0, g + 2)
        refill(1, g + 1)
        for when, c, k in events:
            if when <= trips - 1:
                pl.when(i == math.ceil(when))(functools.partial(scoped, k, c))
        return 0

    trips = groups // 2 - 1
    lax.fori_loop(0, trips, loop, 0)
    last = groups - 2
    with jax.named_scope('ring_wait'):
        wait_for((last + 1,), (last, last + 1))
    with jax.named_scope('attend'):
        attend((last + 1, 1), (last, 0))
        attend(None, (last + 1, 1))
    for when, c, k in events:
        if when > trips - 1:
            scoped(k, c)
    with jax.named_scope('finish'):
        for c in range(len(CHUNKS)):
            to_partner(c).wait_send()
            over_x(c).wait_send()
            over_y(c).wait_send()
            for copy in sent(c):
                copy.wait_send()
            if c not in DIRECT:
                relay(c).wait_send()
            for kind, origin in passed:
                forward(c, kind, origin).wait_send()
            out_copy(c).wait()


def solution(mesh):
    def local_step(hidden, ln_gain, ln_bias, w_q, w_k, w_v, w_o, k_cache, v_cache, lengths):
        rows, span, kv_local, head_dim = k_cache.shape
        width = hidden.shape[1]
        kv_width = kv_local * head_dim
        q_width = w_q.shape[1]
        groups = rows // GROUP
        keys = jnp.transpose(k_cache, (0, 2, 3, 1)).reshape(rows, kv_width, span)
        values = jnp.transpose(v_cache, (0, 2, 3, 1)).reshape(rows, kv_width, span)
        half_rot = head_dim // 4
        inv_freq = np.power(10000.0, -2.0 * np.arange(half_rot) / (2 * half_rot)).astype(np.float32)
        inv_freq = jnp.asarray(np.broadcast_to(inv_freq[:, None], (half_rot, 128)).copy())
        vmem = pl.BlockSpec(memory_space=pltpu.VMEM)
        smem = pl.BlockSpec(memory_space=pltpu.SMEM)
        hbm = pl.BlockSpec(memory_space=pl.ANY)
        n = len(CHUNKS)
        out, k_new, v_new = pl.pallas_call(
            attention_kernel,
            out_shape=(jax.ShapeDtypeStruct((rows, width), BF16),
                       jax.ShapeDtypeStruct((kv_width, rows), BF16),
                       jax.ShapeDtypeStruct((kv_width, rows), BF16)),
            in_specs=[smem, vmem, vmem, vmem, vmem] + [hbm] * 7,
            out_specs=(hbm, vmem, vmem),
            scratch_shapes=[
                pltpu.VMEM((rows, width), BF16),
                pltpu.VMEM((width, q_width), BF16),
                pltpu.VMEM((width, kv_width), BF16),
                pltpu.VMEM((width, kv_width), BF16),
                pltpu.VMEM((q_width, width), BF16),
                pltpu.VMEM((SLOTS, GROUP, kv_width, span), BF16),
                pltpu.VMEM((SLOTS, GROUP, kv_width, span), BF16),
                pltpu.VMEM((rows, width), BF16),
                pltpu.VMEM((rows, 128), F32),
                pltpu.VMEM((rows, 128), F32),
                pltpu.VMEM((16 * PITCH, 128), F32),
                pltpu.VMEM((rows, kv_width), F32),
                pltpu.VMEM((rows, kv_width), F32),
                pltpu.VMEM((2, 16 * GROUP, span), BF16),
                pltpu.VMEM((2, 16 * GROUP, 128), F32),
                pltpu.VMEM((groups, BLOCK, 256), F32),
                pltpu.VMEM((groups // 2, BLOCK, 256), F32),
                pltpu.VMEM((groups // 4, BLOCK, 256), F32),
                pltpu.VMEM((groups // 4, BLOCK, 256), F32),
                pltpu.VMEM((groups // 4, BLOCK, 256), F32),
                pltpu.VMEM((2 * (max(CHUNKS) // 4) * GROUP * 4, 128), F32),
                pltpu.VMEM((rows // 4, width), F32),
                pltpu.VMEM((rows // 8, width), F32),
                pltpu.VMEM((rows, width), F32),
                pltpu.SemaphoreType.DMA((SLOTS, 2)),
                pltpu.SemaphoreType.DMA((4 + rows // 128,)),
                pltpu.SemaphoreType.DMA((n,)),
                pltpu.SemaphoreType.DMA((n, 10)),
                pltpu.SemaphoreType.DMA((n, 10)),
            ],
            compiler_params=pltpu.CompilerParams(
                collective_id=0, has_side_effects=True, vmem_limit_bytes=67043328),
        )(lengths, lengths.reshape(1, rows), inv_freq, ln_gain.reshape(width // 128, 128), ln_bias.reshape(width // 128, 128),
          hidden, w_q, w_k, w_v, w_o, keys, values)
        k_new = jnp.transpose(k_new.reshape(kv_local, head_dim, rows), (2, 0, 1))
        v_new = jnp.transpose(v_new.reshape(kv_local, head_dim, rows), (2, 0, 1))
        return out, k_new, v_new

    row_spec = P('dp', None)
    cache_spec = P('dp', 'sp', 'tp', None)
    head_spec = P('dp', 'tp', None)
    return jax.shard_map(local_step, mesh=mesh, in_specs=(row_spec, P(None), P(None), P(None, 'tp'), P(None, 'tp'), P(None, 'tp'), P('tp', None), cache_spec, cache_spec, P('dp')), out_specs=(row_spec, head_spec, head_spec), check_vma=False)
```

```python
import functools

import jax
import jax.numpy as jnp
import numpy as np
from jax import lax
from jax.experimental import pallas as pl
from jax.experimental.pallas import tpu as pltpu
from jax.sharding import PartitionSpec as P

MESH = pl.DeviceIdType.MESH
F32 = jnp.float32
BF16 = jnp.bfloat16
LOWEST = float(jnp.finfo(jnp.float32).min)

GROUP = 16
BLOCK = 4 * GROUP + 8
DIRECT = (3, 4)
CHUNKS = (8, 8, 4, 4, 4, 4)
DIRECT = (5,)
INSIDE = ((3, 0, 1), (4, 0, 2), (7, 1, 1), (8, 1, 2), (8, 0, 3), (9, 2, 1), (10, 1, 3), (10, 2, 2), (11, 0, 4), (11, 3, 1),
          (12, 2, 3), (12, 3, 2), (12, 1, 4), (13, 4, 1), (14, 4, 2), (14, 0, 5), (14, 3, 3))
AFTER = ((2, 4), (5, 1), (5, 2), (1, 5), (4, 3), (3, 4), (5, 3), (4, 4), (3, 5), (5, 4), (1, 6), (2, 5), (5, 5), (0, 6), (3, 6),
         (4, 5), (1, 7), (2, 6), (5, 6), (3, 7), (4, 6), (0, 7), (5, 7), (4, 7), (2, 7))
SLOTS = 7
TALL = 256
PITCH = 520


def attention_kernel(len_sm, len_row, inv_freq, gain, bias, hid_hbm, wq_hbm, wk_hbm, wv_hbm, wo_hbm, k_hbm, v_hbm,
                     out_hbm, knt_ref, vnt_ref,
                     hid, wq, wk, wv, wo, kring, vring, stage, cos_t, sin_t, qx, kn, vn,
                     prob, self_w, own, part, send2, mine, recv2, ctx, proj, recv3, total,
                     ring_sem, load_sem, out_sem, send_sem, recv_sem):
    rows, width = hid.shape
    groups = rows // GROUP
    span = k_hbm.shape[2]
    tp = lax.axis_index('tp')
    sp = lax.axis_index('sp')
    x, core = sp // 2, sp % 2

    def ring_copy(which, g):
        slot = lax.rem(g, SLOTS)
        src, ring = ((k_hbm, kring), (v_hbm, vring))[which]
        return pltpu.make_async_copy(src.at[pl.ds(g * GROUP, GROUP)], ring.at[slot], ring_sem.at[slot, which])

    blocks = rows // 128

    def load_hid(i):
        at = pl.ds(i * 128, 128)
        return pltpu.make_async_copy(hid_hbm.at[at], hid.at[at], load_sem.at[4 + i])

    load_wk = pltpu.make_async_copy(wk_hbm, wk, load_sem.at[0])
    load_wv = pltpu.make_async_copy(wv_hbm, wv, load_sem.at[1])
    load_wq = pltpu.make_async_copy(wq_hbm, wq, load_sem.at[2])
    load_wo = pltpu.make_async_copy(wo_hbm, wo, load_sem.at[3])
    for i in range(blocks):
        load_hid(i).start()
    load_wq.start()
    load_wk.start()
    load_wv.start()
    for which in range(2):
        ring_copy(which, 0).start()

    def device(dx, dcore, dtp):
        return {'sp': (x ^ dx) * 2 + (core ^ dcore), 'tp': tp ^ dtp}

    barrier = pltpu.get_barrier_semaphore()
    for peer in ((0, 1, 0), (1, 0, 0), (0, 0, 1), (1, 0, 1)):
        pl.semaphore_signal(barrier, inc=1, device_id=device(*peer), device_id_type=MESH)

    angle = inv_freq[:, 0:1] * len_row[0:1, :].astype(F32)
    cos_a, sin_a = jnp.cos(angle), jnp.sin(angle)
    one, zero = jnp.ones((32, rows), F32), jnp.zeros((32, rows), F32)
    cos_full = jnp.concatenate([cos_a, cos_a, one] * 2, axis=0)
    sin_full = jnp.concatenate([-sin_a, sin_a, zero] * 2, axis=0)
    for blk in range(rows // 128):
        cut = slice(blk * 128, blk * 128 + 128)
        cos_t[cut, :] = cos_full[:, cut].T
        sin_t[cut, :] = sin_full[:, cut].T

    with jax.named_scope('load_hid'):
        for i in range(blocks):
            load_hid(i).wait()
    for g in range(1, SLOTS):
        for which in range(2):
            ring_copy(which, g).start()
    load_wo.start()
    gain_f, bias_f = gain[...].astype(F32), bias[...].astype(F32)
    gain_f = 1.0 + jnp.concatenate([gain_f[i:i + 1] for i in range(width // 128)], 1)
    bias_f = jnp.concatenate([bias_f[i:i + 1] for i in range(width // 128)], 1)

    def norm(i, _):
        for j in range(4):
            at = pl.ds(pl.multiple_of(i * 64 + j * 16, 16), 16)
            wide = hid[at, :].astype(F32)
            centred = wide - jnp.mean(wide, axis=-1, keepdims=True)
            var = jnp.mean(centred * centred, axis=-1, keepdims=True)
            stage[at, :] = (centred * lax.rsqrt(var + 1e-5) * gain_f + bias_f).astype(BF16)
        return 0

    with jax.named_scope('norm'):
        lax.fori_loop(0, rows // 64, norm, 0)

    with jax.named_scope('load_w'):
        load_wk.wait()
        load_wv.wait()
        load_wq.wait()
    lane_rb = lax.broadcasted_iota(jnp.int32, (TALL, 128), 1)
    low_half = lane_rb < 64
    first_rot = (lane_rb % 64) < 16

    def rotate(u, cos_b, sin_b):
        partner = jnp.where(first_rot, pltpu.roll(u, 112, 1), pltpu.roll(u, 16, 1))
        return (u * cos_b + partner * sin_b).astype(BF16).astype(F32)

    def project(i, _):
        start = pl.multiple_of(i * TALL, TALL)
        at = pl.ds(start, TALL)
        normed = stage[at, :]
        cos_b, sin_b = cos_t[at, :], sin_t[at, :]
        for head in range(4):
            q = jnp.dot(normed, wq[:, head * 256:head * 256 + 256], preferred_element_type=F32)
            for j in range(2):
                u = rotate(q[:, j * 128:j * 128 + 128], cos_b, sin_b) * 0.125
                swap = pltpu.roll(u, 64, 1)
                if head % 2 == 0:
                    a, b = jnp.where(low_half, u, 0.0), jnp.where(low_half, swap, 0.0)
                else:
                    a, b = jnp.where(low_half, 0.0, swap), jnp.where(low_half, 0.0, u)
                r = head * 4 + 2 * j
                qx[pl.ds(pl.multiple_of(r * PITCH + start, 8), TALL), :] = a
                qx[pl.ds(pl.multiple_of((r + 1) * PITCH + start, 8), TALL), :] = b
        kp = jnp.dot(normed, wk[...], preferred_element_type=F32)
        vp = jnp.dot(normed, wv[...], preferred_element_type=F32)
        for j in range(2):
            cut = slice(j * 128, j * 128 + 128)
            ku = rotate(kp[:, cut], cos_b, sin_b)
            vu = vp[:, cut].astype(BF16).astype(F32)
            kn[at, cut] = ku
            vn[at, cut] = vu
            knt_ref[cut, at] = ku.T.astype(BF16)
            vnt_ref[cut, at] = vu.T.astype(BF16)
        return 0

    with jax.named_scope('project'):
        lax.fori_loop(0, rows // TALL, project, 0)
    with jax.named_scope('barrier'):
        pl.semaphore_wait(barrier, 4)

    lane = lax.broadcasted_iota(jnp.int32, (8, 128), 1)
    row = lax.broadcasted_iota(jnp.int32, (8, 128), 0)
    low = lane < 64
    keep_w = (row < 4) == low
    stat = lane % 8
    even = (lane % 2) == 0
    keep_s = (row < 4) == even
    pair_of = lane // 8
    pos = lax.broadcasted_iota(jnp.int32, (16, span), 1)
    zero8 = jnp.zeros((8, 128), F32)
    first_pos = sp * span

    def pack(a, b, pick, keep):
        same = jnp.where(pick, a, b)
        other = pltpu.roll(jnp.where(pick, b, a), 4, 0)
        return jnp.where(keep, same, other)

    def queries(b):
        qa = qx[pl.ds(b, 8, stride=PITCH), :]
        qb = qx[pl.ds(b + 8 * PITCH, 8, stride=PITCH), :]
        return qa, qb

    def score(g, j):
        qa, qb = queries(g * GROUP + j)
        q = jnp.concatenate([jnp.concatenate([qa, zero8], 1), jnp.concatenate([zero8, qb], 1)], 0).astype(BF16)
        return jnp.dot(q, kring[lax.rem(g, SLOTS), j], preferred_element_type=F32)

    def weigh(g, side, j, s):
        b = g * GROUP + j
        qa, qb = queries(b)
        left = len_sm[b] - first_pos
        s = jnp.where(pos < left, s, -jnp.inf)
        k_self = kn[pl.ds(b, 1), :]
        s_self = jnp.sum(jnp.concatenate([qa * k_self[:, :128], qb * k_self[:, 128:]], 0), axis=1, keepdims=True)
        owner = jnp.logical_and(left >= 0, left < span)
        s_self = s_self + jnp.where(owner, 0.0, -jnp.inf)
        top = jnp.maximum(jnp.maximum(jnp.max(s, axis=1, keepdims=True), s_self), LOWEST)
        w = jnp.exp(s - top)
        w_self = jnp.exp(s_self - top)
        denom = jnp.sum(w, axis=1, keepdims=True) + w_self
        prob[side, 16 * j:16 * j + 16, :] = w.astype(BF16)
        self_w[side, 16 * j:16 * j + 16, :] = jnp.broadcast_to(w_self, (16, 128))
        return jnp.where(stat < 2, top[:8], jnp.where(stat < 4, top[8:], jnp.where(stat < 6, denom[:8], denom[8:])))

    def value(g, side, j):
        v_self = vn[pl.ds(g * GROUP + j, 1), :]
        part_b = lax.dot_general(prob[side, 16 * j:16 * j + 16, :], vring[lax.rem(g, SLOTS), j],
                                 (((1,), (1,)), ((), ())), preferred_element_type=F32)
        ca = part_b[:8, :128] + self_w[side, 16 * j:16 * j + 8, :] * v_self[:, :128]
        cb = part_b[8:, 128:] + self_w[side, 16 * j + 8:16 * j + 16, :] * v_self[:, 128:]
        return ca, cb

    def attend(score_g, value_g):
        if score_g is not None:
            g, side = score_g
            scores = [score(g, j) for j in range(GROUP)]
            tile = zero8
        for p in range(GROUP // 2):
            if value_g is not None:
                v, vside = value_g
                e, o = value(v, vside, 2 * p), value(v, vside, 2 * p + 1)
                own[v, 8 * p:8 * p + 8, 0:128] = pack(e[0], o[0], low, keep_w)
                own[v, 8 * p:8 * p + 8, 128:256] = pack(e[1], o[1], low, keep_w)
            if score_g is not None:
                e = weigh(g, side, 2 * p, scores[2 * p])
                o = weigh(g, side, 2 * p + 1, scores[2 * p + 1])
                tile = jnp.where(pair_of == p, pack(e, o, even, keep_s), tile)
        if score_g is not None:
            own[g, 4 * GROUP:BLOCK, 0:128] = tile
            own[g, 4 * GROUP:BLOCK, 128:256] = zero8

    is_top = stat < 4

    def spread(f, p, t):
        c = p * 8 + 2 * t
        return jnp.where(low, jnp.broadcast_to(f[:, c:c + 1], (8, 128)), jnp.broadcast_to(f[:, c + 1:c + 2], (8, 128)))

    def merge(a_ref, a, b_ref, b, emit):
        sa, sb = a_ref[a, 4 * GROUP:BLOCK, 0:128], b_ref[b, 4 * GROUP:BLOCK, 0:128]
        top = jnp.maximum(sa, sb)
        fa, fb = jnp.exp(sa - top), jnp.exp(sb - top)
        denom = sa * pltpu.roll(fa, 4, 1) + sb * pltpu.roll(fb, 4, 1)
        emit(None, None, jnp.where(is_top, top, denom))
        for p in range(GROUP // 2):
            r = slice(8 * p, 8 * p + 8)
            for t in range(2):
                c = slice(t * 128, t * 128 + 128)
                w = a_ref[a, r, c] * spread(fa, p, t) + b_ref[b, r, c] * spread(fb, p, t)
                emit(r, c, w / spread(denom, p, 2 + t) if emit.final else w)

    def store_to(ref, index, final):
        def emit(r, c, value):
            if r is None:
                if not final:
                    ref[index, 4 * GROUP:BLOCK, 0:128] = value
                    ref[index, 4 * GROUP:BLOCK, 128:256] = zero8
            elif final:
                base = c.start // 128 * (ref.shape[0] // 2)
                ref[pl.ds(pl.multiple_of(base + index * 4 * GROUP + r.start, 8), 8), :] = value
            else:
                ref[index, r, c] = value
        emit.final = final
        return emit

    starts = [sum(CHUNKS[:c]) for c in range(len(CHUNKS))]

    def remote(c, kind, src, dst, peer):
        return pltpu.make_async_remote_copy(
            src_ref=src, dst_ref=dst, send_sem=send_sem.at[c, kind], recv_sem=recv_sem.at[c, kind],
            device_id=device(*peer), device_id_type=MESH)

    def quarter(c):
        return CHUNKS[c] // 4

    def to_partner(c):
        n = quarter(c)
        src = own.at[pl.ds(starts[c] + (1 - core) * 2 * n, 2 * n)]
        return remote(c, 0, src, part.at[pl.ds(starts[c] // 2, 2 * n)], (0, 1, 0))

    def over_x(c):
        at = pl.ds(starts[c] // 4, quarter(c))
        return remote(c, 1, send2.at[at], recv2.at[at], (1, 0, 0))

    def over_y(c):
        half = quarter(c) * GROUP // 2
        src = proj.at[pl.ds(pl.multiple_of(starts[c] // 4 * GROUP + (1 - tp) * half, 8), half)]
        return remote(c, 2, src, recv3.at[pl.ds(starts[c] // 4 * GROUP // 2, half)], (0, 0, 1))

    def home(c, dx, dcore, dtp):
        half = quarter(c) * GROUP // 2
        index = ((core ^ dcore) * 2 + (x ^ dx)) * 2 + (tp ^ dtp)
        return total.at[pl.ds(pl.multiple_of(starts[c] * GROUP + index * half, 8), half)]

    def spread_own(c, kind, peer):
        return remote(c, kind, home(c, 0, 0, 0), home(c, 0, 0, 0), peer)

    def forward(c, kind, origin):
        return remote(c, kind, home(c, *origin), home(c, *origin), (0, 1, 0))

    passed = ((7, (1, 0, 0)), (8, (0, 0, 1)), (9, (1, 0, 1)))
    first_peer, other_peer = (1 - core, 0, core), (core, 0, 1 - core)

    def sent(c):
        copies = [spread_own(c, 4, (1, 0, 0)), spread_own(c, 5, (0, 0, 1)), spread_own(c, 3, (0, 1, 0))]
        if c in DIRECT:
            copies.append(spread_own(c, 6, (1, 0, 1)))
        return copies

    def relay(c):
        return remote(c, 6, home(c, *first_peer), home(c, *first_peer), other_peer)

    def step1(c):
        to_partner(c).start()

    def step2(c):
        n = quarter(c)
        with jax.named_scope(f'wait2_{c}'):
            to_partner(c).wait_recv()
        for dx in (1, 0):
            side = x ^ dx

            out = (send2, mine)[1 - dx]
            for i in range(n):
                merge(own, starts[c] + (core * 2 + side) * n + i, part, starts[c] // 2 + side * n + i,
                      store_to(out, starts[c] // 4 + i, False))
            if dx == 1:
                over_x(c).start()

    def step3(c):
        n = quarter(c)
        if c == 0:
            load_wo.wait()
        with jax.named_scope(f'wait3_{c}'):
            over_x(c).wait_recv()

        for i in range(n):
            at = starts[c] // 4 + i
            merge(mine, at, recv2, at, store_to(ctx, i, True))
        m = n * GROUP
        side = ctx.shape[0] // 2
        lhs = [jnp.concatenate([ctx[pl.ds(t * side + g, m, stride=4), :] for t in range(2)], 1).astype(BF16) for g in range(4)]
        for col in range(width // 256):
            cut = slice(col * 256, col * 256 + 256)
            acc = None
            for g in range(4):
                rhs = jnp.concatenate([wo[h * 256 + g * 64:h * 256 + g * 64 + 64, cut] for h in range(4)], 0)
                term = jnp.dot(lhs[g], rhs, preferred_element_type=F32)
                acc = term if acc is None else acc + term
            proj[starts[c] // 4 * GROUP:starts[c] // 4 * GROUP + m, cut] = acc
        over_y(c).start()

    def step4(c):
        half = quarter(c) * GROUP // 2
        with jax.named_scope(f'wait4_{c}'):
            over_y(c).wait_recv()
        src = pl.ds(pl.multiple_of(starts[c] // 4 * GROUP + tp * half, 8), half)
        other = starts[c] // 4 * GROUP // 2
        home(c, 0, 0, 0)[...] = proj[src, :] + recv3[other:other + half, :]
        for copy in sent(c):
            copy.start()

    def step5(c):
        with jax.named_scope(f'wait5_{c}'):
            spread_own(c, 4 + core, (0, 1, 0)).wait_recv()
        if c not in DIRECT:
            relay(c).start()
        forward(c, 7 + core, first_peer).start()

    def step6(c):
        with jax.named_scope(f'wait6a_{c}'):
            spread_own(c, 5 - core, (0, 1, 0)).wait_recv()
        forward(c, 8 - core, other_peer).start()
        with jax.named_scope(f'wait6b_{c}'):
            spread_own(c, 6, (0, 1, 0)).wait_recv()
        forward(c, 9, (1, 0, 1)).start()

    def out_copy(c):
        at = pl.ds(starts[c] * GROUP, CHUNKS[c] * GROUP)
        return pltpu.make_async_copy(stage.at[at], out_hbm.at[at], out_sem.at[c])

    def step7(c):
        with jax.named_scope(f'wait7_{c}'):
            spread_own(c, 3, (0, 1, 0)).wait_recv()
            for kind, origin in passed:
                forward(c, kind, origin).wait_recv()

        def body(i, _):
            at = pl.ds(pl.multiple_of((starts[c] + i) * GROUP, GROUP), GROUP)
            stage[at, :] = (hid[at, :].astype(F32) + total[at, :]).astype(BF16)
            return 0

        lax.fori_loop(0, CHUNKS[c], body, 0)
        out_copy(c).start()

    def scoped(i, c):
        with jax.named_scope(f'step{i + 1}_{c}'):
            steps[i](c)

    steps = (step1, step2, step3, step4, step5, step6, step7)
    def wait_for(keys, values):
        for g in keys:
            ring_copy(0, g).wait()
        for g in values:
            ring_copy(1, g).wait()

    def refill(which, g):
        @pl.when(g + SLOTS < groups)
        def _():
            ring_copy(which, g + SLOTS).start()

    wait_for((0,), ())
    with jax.named_scope('attend'):
        attend((0, 0), None)
    refill(0, 0)

    def loop(i, _):
        g = 2 * i
        with jax.named_scope('ring_wait'):
            wait_for((g + 1, g + 2), (g, g + 1))
        with jax.named_scope('attend'):
            attend((g + 1, 1), (g, 0))
            attend((g + 2, 0), (g + 1, 1))
        refill(0, g + 1)
        refill(1, g)
        refill(0, g + 2)
        refill(1, g + 1)
        for when, c, k in INSIDE:
            pl.when(i == when)(functools.partial(scoped, k - 1, c))
        return 0

    trips = groups // 2 - 1
    lax.fori_loop(0, trips, loop, 0)
    last = groups - 2
    with jax.named_scope('ring_wait'):
        wait_for((last + 1,), (last, last + 1))
    with jax.named_scope('attend'):
        attend((last + 1, 1), (last, 0))
        attend(None, (last + 1, 1))
    for c, k in AFTER:
        scoped(k - 1, c)
    with jax.named_scope('finish'):
        for c in range(len(CHUNKS)):
            to_partner(c).wait_send()
            over_x(c).wait_send()
            over_y(c).wait_send()
            for copy in sent(c):
                copy.wait_send()
            if c not in DIRECT:
                relay(c).wait_send()
            for kind, origin in passed:
                forward(c, kind, origin).wait_send()
            out_copy(c).wait()


def copy_kernel(*refs):
    n = len(refs) // 4
    sources, results, staged = refs[:n], refs[n:2 * n], refs[2 * n:3 * n]
    sems = refs[3 * n:]
    pieces = []
    for src, dst, mid, sem in zip(sources, results, staged, sems):
        count = src.shape[0] // 64
        for i in range(count):
            at = pl.ds(i * 64, 64)
            pieces.append((pltpu.make_async_copy(src.at[at], mid.at[at], sem.at[i, 0]),
                           pltpu.make_async_copy(mid.at[at], dst.at[at], sem.at[i, 1])))
    for load, _ in pieces:
        load.start()
    for load, save in pieces:
        load.wait()
        save.start()
    for _, save in pieces:
        save.wait()


def solution(mesh):
    def local_step(hidden, ln_gain, ln_bias, w_q, w_k, w_v, w_o, k_cache, v_cache, lengths):
        rows, span, kv_local, head_dim = k_cache.shape
        width = hidden.shape[1]
        kv_width = kv_local * head_dim
        q_width = w_q.shape[1]
        groups = rows // GROUP
        keys = jnp.transpose(k_cache, (0, 2, 3, 1)).reshape(rows, kv_width, span)
        values = jnp.transpose(v_cache, (0, 2, 3, 1)).reshape(rows, kv_width, span)
        half_rot = head_dim // 4
        inv_freq = np.power(10000.0, -2.0 * np.arange(half_rot) / (2 * half_rot)).astype(np.float32)
        inv_freq = jnp.asarray(np.broadcast_to(inv_freq[:, None], (half_rot, 128)).copy())
        vmem = pl.BlockSpec(memory_space=pltpu.VMEM)
        smem = pl.BlockSpec(memory_space=pltpu.SMEM)
        hbm = pl.BlockSpec(memory_space=pl.ANY)
        n = len(CHUNKS)
        out, k_new, v_new = pl.pallas_call(
            attention_kernel,
            out_shape=(jax.ShapeDtypeStruct((rows, width), BF16),
                       jax.ShapeDtypeStruct((kv_width, rows), BF16),
                       jax.ShapeDtypeStruct((kv_width, rows), BF16)),
            in_specs=[smem, vmem, vmem, vmem, vmem] + [hbm] * 7,
            out_specs=(hbm, vmem, vmem),
            scratch_shapes=[
                pltpu.VMEM((rows, width), BF16),
                pltpu.VMEM((width, q_width), BF16),
                pltpu.VMEM((width, kv_width), BF16),
                pltpu.VMEM((width, kv_width), BF16),
                pltpu.VMEM((q_width, width), BF16),
                pltpu.VMEM((SLOTS, GROUP, kv_width, span), BF16),
                pltpu.VMEM((SLOTS, GROUP, kv_width, span), BF16),
                pltpu.VMEM((rows, width), BF16),
                pltpu.VMEM((rows, 128), F32),
                pltpu.VMEM((rows, 128), F32),
                pltpu.VMEM((16 * PITCH, 128), F32),
                pltpu.VMEM((rows, kv_width), F32),
                pltpu.VMEM((rows, kv_width), F32),
                pltpu.VMEM((2, 16 * GROUP, span), BF16),
                pltpu.VMEM((2, 16 * GROUP, 128), F32),
                pltpu.VMEM((groups, BLOCK, 256), F32),
                pltpu.VMEM((groups // 2, BLOCK, 256), F32),
                pltpu.VMEM((groups // 4, BLOCK, 256), F32),
                pltpu.VMEM((groups // 4, BLOCK, 256), F32),
                pltpu.VMEM((groups // 4, BLOCK, 256), F32),
                pltpu.VMEM((2 * (max(CHUNKS) // 4) * GROUP * 4, 128), F32),
                pltpu.VMEM((rows // 4, width), F32),
                pltpu.VMEM((rows // 8, width), F32),
                pltpu.VMEM((rows, width), F32),
                pltpu.SemaphoreType.DMA((SLOTS, 2)),
                pltpu.SemaphoreType.DMA((4 + rows // 128,)),
                pltpu.SemaphoreType.DMA((n,)),
                pltpu.SemaphoreType.DMA((n, 10)),
                pltpu.SemaphoreType.DMA((n, 10)),
            ],
            compiler_params=pltpu.CompilerParams(
                collective_id=0, has_side_effects=True, vmem_limit_bytes=67043328),
        )(lengths, lengths.reshape(1, rows), inv_freq, ln_gain.reshape(width // 128, 128), ln_bias.reshape(width // 128, 128),
          hidden, w_q, w_k, w_v, w_o, keys, values)
        arrays = (out, k_new, v_new)
        out, k_new, v_new = pl.pallas_call(
            copy_kernel,
            out_shape=[jax.ShapeDtypeStruct(a.shape, a.dtype) for a in arrays],
            in_specs=[hbm] * 3,
            out_specs=[hbm] * 3,
            scratch_shapes=[pltpu.VMEM(a.shape, a.dtype) for a in arrays]
            + [pltpu.SemaphoreType.DMA((a.shape[0] // 64, 2)) for a in arrays],
            compiler_params=pltpu.CompilerParams(vmem_limit_bytes=67043328),
        )(*arrays)
        k_new = jnp.transpose(k_new.reshape(kv_local, head_dim, rows), (2, 0, 1))
        v_new = jnp.transpose(v_new.reshape(kv_local, head_dim, rows), (2, 0, 1))
        return out, k_new, v_new

    row_spec = P('dp', None)
    cache_spec = P('dp', 'sp', 'tp', None)
    head_spec = P('dp', 'tp', None)
    return jax.shard_map(local_step, mesh=mesh, in_specs=(row_spec, P(None), P(None), P(None, 'tp'), P(None, 'tp'), P(None, 'tp'), P('tp', None), cache_spec, cache_spec, P('dp')), out_specs=(row_spec, head_spec, head_spec), check_vma=False)
```

```python
import functools

import jax
import jax.numpy as jnp
import numpy as np
from jax import lax
from jax.experimental import pallas as pl
from jax.experimental.pallas import tpu as pltpu
from jax.sharding import PartitionSpec as P

MESH = pl.DeviceIdType.MESH
F32 = jnp.float32
BF16 = jnp.bfloat16
LOWEST = float(jnp.finfo(jnp.float32).min)

GROUP = 16
BLOCK = 4 * GROUP + 8

CHUNKS = (4, 4, 4, 4, 4, 4, 4, 2, 2)
DIRECT = (7, 8)
INSIDE = ((1, 0, 1), (2, 0, 2), (3, 1, 1), (4, 0, 3), (4, 1, 2), (5, 2, 1), (6, 2, 2), (6, 1, 3), (7, 0, 4), (7, 3, 1),
          (8, 3, 2), (8, 2, 3), (9, 1, 4), (9, 4, 1), (10, 4, 2), (10, 0, 5), (10, 3, 3), (11, 2, 4), (11, 5, 1), (12, 4,
          3), (12, 5, 2), (13, 2, 5), (13, 3, 4), (13, 6, 1), (14, 6, 2), (14, 4, 4), (14, 5, 3), (14, 7, 1))
AFTER = ((8, 1), (7, 2), (3, 5), (0, 6), (6, 3), (8, 2), (1, 5), (4, 5), (7, 3), (6, 4), (0, 7), (8, 3), (5, 4), (2, 6),
         (7, 4), (2, 7), (8, 4), (5, 5), (4, 6), (6, 5), (1, 6), (8, 5), (3, 6), (8, 6), (7, 5), (5, 6), (3, 7), (6, 6),
         (7, 6), (4, 7), (1, 7), (8, 7), (5, 7), (6, 7), (7, 7))
SLOTS = 7
TALL = 256
STATS = 32
PITCH = 520


def attention_kernel(len_sm, len_row, inv_freq, gain, bias, hid_hbm, wq_hbm, wk_hbm, wv_hbm, wo_hbm, k_hbm, v_hbm,
                     out_hbm, knt_ref, vnt_ref,
                     hid, wq, wk, wv, wo, kring, vring, stage, cos_t, sin_t, qx, kn, vn,
                     prob, self_w, own, part, send2, mine, recv2, ctx, away, keep, recv3, total,
                     ring_sem, load_sem, out_sem, send_sem, recv_sem):
    rows, width = hid.shape
    groups = rows // GROUP
    span = k_hbm.shape[2]
    tp = lax.axis_index('tp')
    sp = lax.axis_index('sp')
    x, core = sp // 2, sp % 2

    def ring_copy(which, g):
        slot = lax.rem(g, SLOTS)
        src, ring = ((k_hbm, kring), (v_hbm, vring))[which]
        return pltpu.make_async_copy(src.at[pl.ds(g * GROUP, GROUP)], ring.at[slot], ring_sem.at[slot, which])

    blocks = rows // 128

    def load_hid(i):
        at = pl.ds(i * 128, 128)
        return pltpu.make_async_copy(hid_hbm.at[at], hid.at[at], load_sem.at[4 + i])

    load_wk = pltpu.make_async_copy(wk_hbm, wk, load_sem.at[0])
    load_wv = pltpu.make_async_copy(wv_hbm, wv, load_sem.at[1])
    load_wq = pltpu.make_async_copy(wq_hbm, wq, load_sem.at[2])
    load_wo = pltpu.make_async_copy(wo_hbm, wo, load_sem.at[3])
    for i in range(blocks):
        load_hid(i).start()
    load_wq.start()
    load_wk.start()
    load_wv.start()
    for which in range(2):
        ring_copy(which, 0).start()

    def device(dx, dcore, dtp):
        return {'sp': (x ^ dx) * 2 + (core ^ dcore), 'tp': tp ^ dtp}

    barrier = pltpu.get_barrier_semaphore()
    for peer in ((0, 1, 0), (1, 0, 0), (0, 0, 1), (1, 0, 1)):
        pl.semaphore_signal(barrier, inc=1, device_id=device(*peer), device_id_type=MESH)

    angle = inv_freq[:, 0:1] * len_row[0:1, :].astype(F32)
    cos_a, sin_a = jnp.cos(angle), jnp.sin(angle)
    one, zero = jnp.ones((32, rows), F32), jnp.zeros((32, rows), F32)
    cos_full = jnp.concatenate([cos_a, cos_a, one] * 2, axis=0)
    sin_full = jnp.concatenate([-sin_a, sin_a, zero] * 2, axis=0)
    for blk in range(rows // 128):
        cut = slice(blk * 128, blk * 128 + 128)
        cos_t[cut, :] = cos_full[:, cut].T
        sin_t[cut, :] = sin_full[:, cut].T

    with jax.named_scope('load_hid'):
        for i in range(blocks):
            load_hid(i).wait()
    for g in range(1, SLOTS):
        for which in range(2):
            ring_copy(which, g).start()
    load_wo.start()
    gain_f, bias_f = gain[...].astype(F32), bias[...].astype(F32)
    gain_f = 1.0 + jnp.concatenate([gain_f[i:i + 1] for i in range(width // 128)], 1)
    bias_f = jnp.concatenate([bias_f[i:i + 1] for i in range(width // 128)], 1)

    def norm(i, _):
        for j in range(4):
            at = pl.ds(pl.multiple_of(i * 64 + j * 16, 16), 16)
            wide = hid[at, :].astype(F32)
            centred = wide - jnp.mean(wide, axis=-1, keepdims=True)
            var = jnp.mean(centred * centred, axis=-1, keepdims=True)
            stage[at, :] = (centred * lax.rsqrt(var + 1e-5) * gain_f + bias_f).astype(BF16)
        return 0

    with jax.named_scope('norm'):
        lax.fori_loop(0, rows // 64, norm, 0)

    with jax.named_scope('load_w'):
        load_wk.wait()
        load_wv.wait()
        load_wq.wait()
    lane_rb = lax.broadcasted_iota(jnp.int32, (TALL, 128), 1)
    low_half = lane_rb < 64
    first_rot = (lane_rb % 64) < 16

    def rotate(u, cos_b, sin_b):
        partner = jnp.where(first_rot, pltpu.roll(u, 112, 1), pltpu.roll(u, 16, 1))
        return (u * cos_b + partner * sin_b).astype(BF16).astype(F32)

    def project(i, _):
        start = pl.multiple_of(i * TALL, TALL)
        at = pl.ds(start, TALL)
        normed = stage[at, :]
        cos_b, sin_b = cos_t[at, :], sin_t[at, :]
        for head in range(4):
            q = jnp.dot(normed, wq[:, head * 256:head * 256 + 256], preferred_element_type=F32)
            for j in range(2):
                u = rotate(q[:, j * 128:j * 128 + 128], cos_b, sin_b) * 0.125
                swap = pltpu.roll(u, 64, 1)
                if head % 2 == 0:
                    a, b = jnp.where(low_half, u, 0.0), jnp.where(low_half, swap, 0.0)
                else:
                    a, b = jnp.where(low_half, 0.0, swap), jnp.where(low_half, 0.0, u)
                r = head * 4 + 2 * j
                qx[pl.ds(pl.multiple_of(r * PITCH + start, 8), TALL), :] = a
                qx[pl.ds(pl.multiple_of((r + 1) * PITCH + start, 8), TALL), :] = b
        kp = jnp.dot(normed, wk[...], preferred_element_type=F32)
        vp = jnp.dot(normed, wv[...], preferred_element_type=F32)
        for j in range(2):
            cut = slice(j * 128, j * 128 + 128)
            ku = rotate(kp[:, cut], cos_b, sin_b)
            vu = vp[:, cut].astype(BF16).astype(F32)
            kn[at, cut] = ku
            vn[at, cut] = vu
            knt_ref[cut, at] = ku.T.astype(BF16)
            vnt_ref[cut, at] = vu.T.astype(BF16)
        return 0

    with jax.named_scope('project'):
        lax.fori_loop(0, rows // TALL, project, 0)
    with jax.named_scope('barrier'):
        pl.semaphore_wait(barrier, 4)

    lane = lax.broadcasted_iota(jnp.int32, (8, 128), 1)
    row = lax.broadcasted_iota(jnp.int32, (8, 128), 0)
    low = lane < 64
    keep_w = (row < 4) == low
    stat = lane % 8
    even = (lane % 2) == 0
    keep_s = (row < 4) == even
    pair_of = lane // 8
    pos = lax.broadcasted_iota(jnp.int32, (16, span), 1)
    zero8 = jnp.zeros((8, 128), F32)
    first_pos = sp * span

    def pack(a, b, pick, keep):
        same = jnp.where(pick, a, b)
        other = pltpu.roll(jnp.where(pick, b, a), 4, 0)
        return jnp.where(keep, same, other)

    def queries(b):
        qa = qx[pl.ds(b, 8, stride=PITCH), :]
        qb = qx[pl.ds(b + 8 * PITCH, 8, stride=PITCH), :]
        return qa, qb

    def score(g, j):
        qa, qb = queries(g * GROUP + j)
        q = jnp.concatenate([jnp.concatenate([qa, zero8], 1), jnp.concatenate([zero8, qb], 1)], 0).astype(BF16)
        return jnp.dot(q, kring[lax.rem(g, SLOTS), j], preferred_element_type=F32)

    def weigh(g, side, j, s):
        b = g * GROUP + j
        qa, qb = queries(b)
        left = len_sm[b] - first_pos
        s = jnp.where(pos < left, s, -jnp.inf)
        k_self = kn[pl.ds(b, 1), :]
        s_self = jnp.sum(jnp.concatenate([qa * k_self[:, :128], qb * k_self[:, 128:]], 0), axis=1, keepdims=True)
        owner = jnp.logical_and(left >= 0, left < span)
        s_self = s_self + jnp.where(owner, 0.0, -jnp.inf)
        top = jnp.maximum(jnp.maximum(jnp.max(s, axis=1, keepdims=True), s_self), LOWEST)
        w = jnp.exp(s - top)
        w_self = jnp.exp(s_self - top)
        denom = jnp.sum(w, axis=1, keepdims=True) + w_self
        prob[side, 16 * j:16 * j + 16, :] = w.astype(BF16)
        self_w[side, 16 * j:16 * j + 16, :] = jnp.broadcast_to(w_self, (16, 128))
        return jnp.where(stat < 2, top[:8], jnp.where(stat < 4, top[8:], jnp.where(stat < 6, denom[:8], denom[8:])))

    def value(g, side, j):
        v_self = vn[pl.ds(g * GROUP + j, 1), :]
        part_b = lax.dot_general(prob[side, 16 * j:16 * j + 16, :], vring[lax.rem(g, SLOTS), j],
                                 (((1,), (1,)), ((), ())), preferred_element_type=F32)
        ca = part_b[:8, :128] + self_w[side, 16 * j:16 * j + 8, :] * v_self[:, :128]
        cb = part_b[8:, 128:] + self_w[side, 16 * j + 8:16 * j + 16, :] * v_self[:, 128:]
        return ca, cb

    def pair_row(p):
        return 8 * p if 8 * p < STATS else 8 * p + 8

    def attend(score_g, value_g):
        if score_g is not None:
            g, side = score_g
            scores = [score(g, j) for j in range(GROUP)]
            tile = zero8
        for p in range(GROUP // 2):
            if value_g is not None:
                v, vside = value_g
                e, o = value(v, vside, 2 * p), value(v, vside, 2 * p + 1)
                r = pair_row(p)
                own[v, r:r + 8, 0:128] = pack(e[0], o[0], low, keep_w)
                own[v, r:r + 8, 128:256] = pack(e[1], o[1], low, keep_w)
            if score_g is not None:
                e = weigh(g, side, 2 * p, scores[2 * p])
                o = weigh(g, side, 2 * p + 1, scores[2 * p + 1])
                tile = jnp.where(pair_of == p, pack(e, o, even, keep_s), tile)
        if score_g is not None:
            own[g, STATS:STATS + 8, 0:128] = tile
            own[g, STATS:STATS + 8, 128:256] = zero8

    is_top = stat < 4

    def spread(f, p, t):
        c = p * 8 + 2 * t
        return jnp.where(low, jnp.broadcast_to(f[:, c:c + 1], (8, 128)), jnp.broadcast_to(f[:, c + 1:c + 2], (8, 128)))

    def factors(a_ref, a, b_ref, b):
        sa, sb = a_ref[a, STATS:STATS + 8, 0:128], b_ref[b, STATS:STATS + 8, 0:128]
        top = jnp.maximum(sa, sb)
        fa, fb = jnp.exp(sa - top), jnp.exp(sb - top)
        denom = sa * pltpu.roll(fa, 4, 1) + sb * pltpu.roll(fb, 4, 1)
        return fa, fb, denom, jnp.where(is_top, top, denom)

    def pairs(side, values):
        if side is None:
            return [pair_row(p) for p in range(GROUP // 2)], values
        rows_of = [pl.multiple_of((STATS + 8) * side + 8 * p, 8) for p in range(GROUP // 4)]
        return rows_of, tuple(jnp.where(side == 1, pltpu.roll(f, 96, 1), f) for f in values)

    def blend(a_ref, a, b_ref, b, found, side, out_ref, out):
        at, (fa, fb) = pairs(side, found[:2])
        for p, r in enumerate(at):
            for t in range(2):
                c = slice(t * 128, t * 128 + 128)
                r8 = pl.ds(r, 8)
                out_ref[out, r8, c] = a_ref[a, r8, c] * spread(fa, p, t) + b_ref[b, r8, c] * spread(fb, p, t)
        out_ref[out, STATS:STATS + 8, 0:128] = found[3]
        out_ref[out, STATS:STATS + 8, 128:256] = zero8

    def finish(a_ref, a, b_ref, b, side, unit):
        found = factors(a_ref, a, b_ref, b)
        at, (fa, fb, denom) = pairs(side, found[:3])
        for p, r in enumerate(at):
            for t in range(2):
                c = slice(t * 128, t * 128 + 128)
                r8 = pl.ds(r, 8)
                w = a_ref[a, r8, c] * spread(fa, p, t) + b_ref[b, r8, c] * spread(fb, p, t)
                base = t * (ctx.shape[0] // 2) + unit * 4 * GROUP + 8 * p
                ctx[base:base + 8, :] = w / spread(denom, p, 2 + t)

    starts = [sum(CHUNKS[:c]) for c in range(len(CHUNKS))]

    def remote(c, kind, src, dst, peer):
        return pltpu.make_async_remote_copy(
            src_ref=src, dst_ref=dst, send_sem=send_sem.at[c, kind], recv_sem=recv_sem.at[c, kind],
            device_id=device(*peer), device_id_type=MESH)

    units = [max(n // 4, 1) for n in CHUNKS]
    blocks_at = [sum(units[:c]) for c in range(len(CHUNKS))]
    columns = width // 2

    def quarter_rows(c):
        return CHUNKS[c] * GROUP // 4

    def quarters(c):
        return pl.ds(starts[c] * GROUP // 4, quarter_rows(c))

    def to_partner(c):
        n = CHUNKS[c] // 2
        src = own.at[pl.ds(starts[c] + (1 - core) * n, n)]
        return remote(c, 0, src, part.at[pl.ds(starts[c] // 2, n)], (0, 1, 0))

    def over_x(c):
        if CHUNKS[c] < 4:
            at = blocks_at[c], pl.ds(pl.multiple_of(STATS * (1 - x), 8), STATS + 8)
        else:
            at = pl.ds(blocks_at[c], units[c])
        return remote(c, 1, send2.at[at], recv2.at[at], (1, 0, 0))

    def over_y(c):
        return remote(c, 2, away.at[quarters(c)], recv3.at[quarters(c)], (0, 0, 1))

    def home(c, dx, dcore, dtp):
        n = quarter_rows(c)
        at = pl.ds(pl.multiple_of(starts[c] * GROUP + ((core ^ dcore) * 2 + (x ^ dx)) * n, 8), n)
        return total.at[at, pl.ds(pl.multiple_of((tp ^ dtp) * columns, columns), columns)]

    def spread_own(c, kind, peer):
        return remote(c, kind, home(c, 0, 0, 0), home(c, 0, 0, 0), peer)

    def forward(c, kind, origin):
        return remote(c, kind, home(c, *origin), home(c, *origin), (0, 1, 0))

    passed = ((7, (1, 0, 0)), (8, (0, 0, 1)), (9, (1, 0, 1)))
    first_peer, other_peer = (1 - core, 0, core), (core, 0, 1 - core)

    def sent(c):
        copies = [spread_own(c, 4, (1, 0, 0)), spread_own(c, 5, (0, 0, 1)), spread_own(c, 3, (0, 1, 0))]
        if c in DIRECT:
            copies.append(spread_own(c, 6, (1, 0, 1)))
        return copies

    def relay(c):
        return remote(c, 6, home(c, *first_peer), home(c, *first_peer), other_peer)

    def step1(c):
        to_partner(c).start()

    def step2(c):
        n = units[c]
        with jax.named_scope(f'wait2_{c}'):
            to_partner(c).wait_recv()
        work = []
        for dx in (1, 0):
            side = x ^ dx
            for i in range(n):
                if CHUNKS[c] < 4:
                    a, b, half = starts[c] + core, starts[c] // 2, side
                else:
                    a, b, half = starts[c] + (core * 2 + side) * n + i, starts[c] // 2 + side * n + i, None
                work.append((a, b, half, factors(own, a, part, b), (mine, send2)[dx], blocks_at[c] + i))
        for k, (a, b, half, found, out_ref, out) in enumerate(work):
            blend(own, a, part, b, found, half, out_ref, out)
            if k == n - 1:
                over_x(c).start()

    def step3(c):
        if c == 0:
            load_wo.wait()
        with jax.named_scope(f'wait3_{c}'):
            over_x(c).wait_recv()
        for i in range(units[c]):
            at = blocks_at[c] + i
            finish(mine, at, recv2, at, x if CHUNKS[c] < 4 else None, i)
        m = quarter_rows(c)
        side = ctx.shape[0] // 2
        lhs = [jnp.concatenate([ctx[pl.ds(t * side + g, m, stride=4), :] for t in range(2)], 1).astype(BF16) for g in range(4)]
        for out_ref, which in ((away, 1 - tp), (keep, tp)):
            for col in range(columns // 256):
                cut = pl.ds(pl.multiple_of(which * columns + col * 256, 256), 256)
                acc = None
                for g in range(4):
                    rhs = jnp.concatenate([wo[h * 256 + g * 64:h * 256 + g * 64 + 64, cut] for h in range(4)], 0)
                    term = jnp.dot(lhs[g], rhs, preferred_element_type=F32)
                    acc = term if acc is None else acc + term
                out_ref[quarters(c), col * 256:col * 256 + 256] = acc
            if out_ref is away:
                over_y(c).start()

    def step4(c):
        with jax.named_scope(f'wait4_{c}'):
            over_y(c).wait_recv()
        home(c, 0, 0, 0)[...] = keep[quarters(c), :] + recv3[quarters(c), :]
        for copy in sent(c):
            copy.start()

    def step5(c):
        with jax.named_scope(f'wait5_{c}'):
            spread_own(c, 4 + core, (0, 1, 0)).wait_recv()
        if c not in DIRECT:
            relay(c).start()
        forward(c, 7 + core, first_peer).start()

    def step6(c):
        with jax.named_scope(f'wait6a_{c}'):
            spread_own(c, 5 - core, (0, 1, 0)).wait_recv()
        forward(c, 8 - core, other_peer).start()
        with jax.named_scope(f'wait6b_{c}'):
            spread_own(c, 6, (0, 1, 0)).wait_recv()
        forward(c, 9, (1, 0, 1)).start()

    def out_copy(c):
        at = pl.ds(starts[c] * GROUP, CHUNKS[c] * GROUP)
        return pltpu.make_async_copy(stage.at[at], out_hbm.at[at], out_sem.at[c])

    def step7(c):
        with jax.named_scope(f'wait7_{c}'):
            spread_own(c, 3, (0, 1, 0)).wait_recv()
            for kind, origin in passed:
                forward(c, kind, origin).wait_recv()

        def body(i, _):
            at = pl.ds(pl.multiple_of((starts[c] + i) * GROUP, GROUP), GROUP)
            stage[at, :] = (hid[at, :].astype(F32) + total[at, :]).astype(BF16)
            return 0

        lax.fori_loop(0, CHUNKS[c], body, 0)
        out_copy(c).start()

    def scoped(i, c):
        with jax.named_scope(f'step{i + 1}_{c}'):
            steps[i](c)

    steps = (step1, step2, step3, step4, step5, step6, step7)
    def wait_for(keys, values):
        for g in keys:
            ring_copy(0, g).wait()
        for g in values:
            ring_copy(1, g).wait()

    def refill(which, g):
        @pl.when(g + SLOTS < groups)
        def _():
            ring_copy(which, g + SLOTS).start()

    wait_for((0,), ())
    with jax.named_scope('attend'):
        attend((0, 0), None)
    refill(0, 0)

    def loop(i, _):
        g = 2 * i
        with jax.named_scope('ring_wait'):
            wait_for((g + 1, g + 2), (g, g + 1))
        with jax.named_scope('attend'):
            attend((g + 1, 1), (g, 0))
            attend((g + 2, 0), (g + 1, 1))
        refill(0, g + 1)
        refill(1, g)
        refill(0, g + 2)
        refill(1, g + 1)
        for when, c, k in INSIDE:
            pl.when(i == when)(functools.partial(scoped, k - 1, c))
        return 0

    trips = groups // 2 - 1
    lax.fori_loop(0, trips, loop, 0)
    last = groups - 2
    with jax.named_scope('ring_wait'):
        wait_for((last + 1,), (last, last + 1))
    with jax.named_scope('attend'):
        attend((last + 1, 1), (last, 0))
        attend(None, (last + 1, 1))
    for c, k in AFTER:
        scoped(k - 1, c)
    with jax.named_scope('finish'):
        for c in range(len(CHUNKS)):
            to_partner(c).wait_send()
            over_x(c).wait_send()
            over_y(c).wait_send()
            for copy in sent(c):
                copy.wait_send()
            if c not in DIRECT:
                relay(c).wait_send()
            for kind, origin in passed:
                forward(c, kind, origin).wait_send()
            out_copy(c).wait()


def copy_kernel(*refs):
    n = len(refs) // 4
    sources, results, staged = refs[:n], refs[n:2 * n], refs[2 * n:3 * n]
    sems = refs[3 * n:]
    pieces = []
    for src, dst, mid, sem in zip(sources, results, staged, sems):
        count = src.shape[0] // 64
        for i in range(count):
            at = pl.ds(i * 64, 64)
            pieces.append((pltpu.make_async_copy(src.at[at], mid.at[at], sem.at[i, 0]),
                           pltpu.make_async_copy(mid.at[at], dst.at[at], sem.at[i, 1])))
    for load, _ in pieces:
        load.start()
    for load, save in pieces:
        load.wait()
        save.start()
    for _, save in pieces:
        save.wait()


def solution(mesh):
    def local_step(hidden, ln_gain, ln_bias, w_q, w_k, w_v, w_o, k_cache, v_cache, lengths):
        rows, span, kv_local, head_dim = k_cache.shape
        width = hidden.shape[1]
        kv_width = kv_local * head_dim
        q_width = w_q.shape[1]
        groups = rows // GROUP
        keys = jnp.transpose(k_cache, (0, 2, 3, 1)).reshape(rows, kv_width, span)
        values = jnp.transpose(v_cache, (0, 2, 3, 1)).reshape(rows, kv_width, span)
        half_rot = head_dim // 4
        inv_freq = np.power(10000.0, -2.0 * np.arange(half_rot) / (2 * half_rot)).astype(np.float32)
        inv_freq = jnp.asarray(np.broadcast_to(inv_freq[:, None], (half_rot, 128)).copy())
        vmem = pl.BlockSpec(memory_space=pltpu.VMEM)
        smem = pl.BlockSpec(memory_space=pltpu.SMEM)
        hbm = pl.BlockSpec(memory_space=pl.ANY)
        n = len(CHUNKS)
        out, k_new, v_new = pl.pallas_call(
            attention_kernel,
            out_shape=(jax.ShapeDtypeStruct((rows, width), BF16),
                       jax.ShapeDtypeStruct((kv_width, rows), BF16),
                       jax.ShapeDtypeStruct((kv_width, rows), BF16)),
            in_specs=[smem, vmem, vmem, vmem, vmem] + [hbm] * 7,
            out_specs=(hbm, vmem, vmem),
            scratch_shapes=[
                pltpu.VMEM((rows, width), BF16),
                pltpu.VMEM((width, q_width), BF16),
                pltpu.VMEM((width, kv_width), BF16),
                pltpu.VMEM((width, kv_width), BF16),
                pltpu.VMEM((q_width, width), BF16),
                pltpu.VMEM((SLOTS, GROUP, kv_width, span), BF16),
                pltpu.VMEM((SLOTS, GROUP, kv_width, span), BF16),
                pltpu.VMEM((rows, width), BF16),
                pltpu.VMEM((rows, 128), F32),
                pltpu.VMEM((rows, 128), F32),
                pltpu.VMEM((16 * PITCH, 128), F32),
                pltpu.VMEM((rows, kv_width), F32),
                pltpu.VMEM((rows, kv_width), F32),
                pltpu.VMEM((2, 16 * GROUP, span), BF16),
                pltpu.VMEM((2, 16 * GROUP, 128), F32),
                pltpu.VMEM((groups, BLOCK, 256), F32),
                pltpu.VMEM((groups // 2, BLOCK, 256), F32),
                pltpu.VMEM((sum(max(c // 4, 1) for c in CHUNKS), BLOCK, 256), F32),
                pltpu.VMEM((sum(max(c // 4, 1) for c in CHUNKS), BLOCK, 256), F32),
                pltpu.VMEM((sum(max(c // 4, 1) for c in CHUNKS), BLOCK, 256), F32),
                pltpu.VMEM((2 * (max(CHUNKS) // 4) * GROUP * 4, 128), F32),
                pltpu.VMEM((rows // 4, width // 2), F32),
                pltpu.VMEM((rows // 4, width // 2), F32),
                pltpu.VMEM((rows // 4, width // 2), F32),
                pltpu.VMEM((rows, width), F32),
                pltpu.SemaphoreType.DMA((SLOTS, 2)),
                pltpu.SemaphoreType.DMA((4 + rows // 128,)),
                pltpu.SemaphoreType.DMA((n,)),
                pltpu.SemaphoreType.DMA((n, 10)),
                pltpu.SemaphoreType.DMA((n, 10)),
            ],
            compiler_params=pltpu.CompilerParams(
                collective_id=0, has_side_effects=True, vmem_limit_bytes=67043328),
        )(lengths, lengths.reshape(1, rows), inv_freq, ln_gain.reshape(width // 128, 128), ln_bias.reshape(width // 128, 128),
          hidden, w_q, w_k, w_v, w_o, keys, values)
        arrays = (out, k_new, v_new)
        out, k_new, v_new = pl.pallas_call(
            copy_kernel,
            out_shape=[jax.ShapeDtypeStruct(a.shape, a.dtype) for a in arrays],
            in_specs=[hbm] * 3,
            out_specs=[hbm] * 3,
            scratch_shapes=[pltpu.VMEM(a.shape, a.dtype) for a in arrays]
            + [pltpu.SemaphoreType.DMA((a.shape[0] // 64, 2)) for a in arrays],
            compiler_params=pltpu.CompilerParams(vmem_limit_bytes=67043328),
        )(*arrays)
        k_new = jnp.transpose(k_new.reshape(kv_local, head_dim, rows), (2, 0, 1))
        v_new = jnp.transpose(v_new.reshape(kv_local, head_dim, rows), (2, 0, 1))
        return out, k_new, v_new

    row_spec = P('dp', None)
    cache_spec = P('dp', 'sp', 'tp', None)
    head_spec = P('dp', 'tp', None)
    return jax.shard_map(local_step, mesh=mesh, in_specs=(row_spec, P(None), P(None), P(None, 'tp'), P(None, 'tp'), P(None, 'tp'), P('tp', None), cache_spec, cache_spec, P('dp')), out_specs=(row_spec, head_spec, head_spec), check_vma=False)
```

```python
import jax
import jax.numpy as jnp
import numpy as np
from jax import lax
from jax.experimental import pallas as pl
from jax.experimental.pallas import tpu as pltpu
from jax.sharding import PartitionSpec as P

MESH = pl.DeviceIdType.MESH
F32 = jnp.float32
BF16 = jnp.bfloat16
LOWEST = float(jnp.finfo(jnp.float32).min)

GROUP = 16
BLOCK = 4 * GROUP + 8

CHUNKS = (8, 4, 4, 4, 4, 4, 2, 2)
DIRECT = (7,)
INSIDE = ((3, 0, 1), (4, 0, 2), (5, 1, 1), (6, 1, 2), (7, 0, 3), (7, 2, 1), (8, 2, 2), (8, 1, 3), (9, 0, 4), (9, 3, 1),
          (10, 2, 3), (10, 3, 2), (10, 1, 4), (11, 4, 1), (12, 0, 5), (12, 4, 2), (12, 3, 3), (13, 2, 4), (13, 1, 5), (13,
          5, 1), (14, 5, 2), (14, 3, 4), (14, 6, 1))
AFTER = ((2, 5), (7, 1), (4, 3), (6, 2), (7, 2), (5, 3), (3, 5), (4, 4), (6, 3), (7, 3), (3, 6), (5, 4), (2, 6), (0, 6),
         (4, 5), (3, 7), (6, 4), (2, 7), (7, 4), (1, 6), (5, 5), (6, 5), (4, 6), (1, 7), (4, 7), (0, 7), (7, 5), (7, 6),
         (5, 6), (6, 6), (7, 7), (5, 7), (6, 7))
SLOTS = 7
TALL = 256
STATS = 32
PITCH = 520


def attention_kernel(len_hbm, len_row_hbm, inv_freq_hbm, gain_hbm, bias_hbm, hid_hbm, wq_hbm, wk_hbm, wv_hbm, wo_hbm, k_hbm, v_hbm,
                     out_hbm, knt_ref, vnt_ref,
                     len_sm, len_row, inv_freq, gain, bias, hid, wq, wk, wv, wo, kring, vring, stage, cos_t, sin_t, qx, kn, vn,
                     prob, self_w, own, part, send2, mine, recv2, ctx, away, keep, recv3, total,
                     ring_sem, load_sem, out_sem, send_sem, recv_sem):
    rows, width = hid.shape
    groups = rows // GROUP
    span = k_hbm.shape[2]
    tp = lax.axis_index('tp')
    sp = lax.axis_index('sp')
    x, core = sp // 2, sp % 2

    def ring_copy(which, g):
        slot = lax.rem(g, SLOTS)
        src, ring = ((k_hbm, kring), (v_hbm, vring))[which]
        return pltpu.make_async_copy(src.at[pl.ds(g * GROUP, GROUP)], ring.at[slot], ring_sem.at[slot, which])

    blocks = rows // 128

    def load_hid(i):
        at = pl.ds(i * 128, 128)
        return pltpu.make_async_copy(hid_hbm.at[at], hid.at[at], load_sem.at[4 + i])

    load_wk = pltpu.make_async_copy(wk_hbm, wk, load_sem.at[0])
    load_wv = pltpu.make_async_copy(wv_hbm, wv, load_sem.at[1])
    load_wq = pltpu.make_async_copy(wq_hbm, wq, load_sem.at[2])
    load_wo = pltpu.make_async_copy(wo_hbm, wo, load_sem.at[3])
    small = [pltpu.make_async_copy(src, dst, load_sem.at[4 + blocks + i]) for i, (src, dst) in enumerate(
        ((len_row_hbm, len_row), (inv_freq_hbm, inv_freq), (gain_hbm, gain), (bias_hbm, bias), (len_hbm, len_sm)))]
    for copy in small:
        copy.start()
    for i in range(blocks):
        load_hid(i).start()
    load_wq.start()
    load_wk.start()
    load_wv.start()
    for which in range(2):
        ring_copy(which, 0).start()

    def device(dx, dcore, dtp):
        return {'sp': (x ^ dx) * 2 + (core ^ dcore), 'tp': tp ^ dtp}

    barrier = pltpu.get_barrier_semaphore()
    for peer in ((0, 1, 0), (1, 0, 0), (0, 0, 1), (1, 0, 1)):
        pl.semaphore_signal(barrier, inc=1, device_id=device(*peer), device_id_type=MESH)

    for copy in small:
        copy.wait()
    angle = inv_freq[:, 0:1] * len_row[0:1, :].astype(F32)
    cos_a, sin_a = jnp.cos(angle), jnp.sin(angle)
    one, zero = jnp.ones((32, rows), F32), jnp.zeros((32, rows), F32)
    cos_full = jnp.concatenate([cos_a, cos_a, one] * 2, axis=0)
    sin_full = jnp.concatenate([-sin_a, sin_a, zero] * 2, axis=0)
    for blk in range(rows // 128):
        cut = slice(blk * 128, blk * 128 + 128)
        cos_t[cut, :] = cos_full[:, cut].T
        sin_t[cut, :] = sin_full[:, cut].T

    gain_f, bias_f = gain[...].astype(F32), bias[...].astype(F32)
    gain_f = 1.0 + jnp.concatenate([gain_f[i:i + 1] for i in range(width // 128)], 1)
    bias_f = jnp.concatenate([bias_f[i:i + 1] for i in range(width // 128)], 1)

    def norm(i, _):
        for j in range(4):
            at = pl.ds(pl.multiple_of(i * 64 + j * 16, 16), 16)
            wide = hid[at, :].astype(F32)
            centred = wide - jnp.mean(wide, axis=-1, keepdims=True)
            var = jnp.mean(centred * centred, axis=-1, keepdims=True)
            stage[at, :] = (centred * lax.rsqrt(var + 1e-5) * gain_f + bias_f).astype(BF16)
        return 0

    for i in range(blocks):
        with jax.named_scope(f'load_hid{i}'):
            load_hid(i).wait()
        if i == 1:
            for g in range(1, SLOTS):
                for which in range(2):
                    ring_copy(which, g).start()
            load_wo.start()
        with jax.named_scope('norm'):
            lax.fori_loop(2 * i, 2 * i + 2, norm, 0)

    with jax.named_scope('load_w'):
        load_wk.wait()
        load_wv.wait()
        load_wq.wait()
    lane_rb = lax.broadcasted_iota(jnp.int32, (TALL, 128), 1)
    low_half = lane_rb < 64
    first_rot = (lane_rb % 64) < 16

    def rotate(u, cos_b, sin_b):
        partner = jnp.where(first_rot, pltpu.roll(u, 112, 1), pltpu.roll(u, 16, 1))
        return (u * cos_b + partner * sin_b).astype(BF16).astype(F32)

    def project(i, _):
        start = pl.multiple_of(i * TALL, TALL)
        at = pl.ds(start, TALL)
        normed = stage[at, :]
        cos_b, sin_b = cos_t[at, :], sin_t[at, :]
        for head in range(4):
            q = jnp.dot(normed, wq[:, head * 256:head * 256 + 256], preferred_element_type=F32)
            for j in range(2):
                u = rotate(q[:, j * 128:j * 128 + 128], cos_b, sin_b) * 0.125
                swap = pltpu.roll(u, 64, 1)
                if head % 2 == 0:
                    a, b = jnp.where(low_half, u, 0.0), jnp.where(low_half, swap, 0.0)
                else:
                    a, b = jnp.where(low_half, 0.0, swap), jnp.where(low_half, 0.0, u)
                r = head * 4 + 2 * j
                qx[pl.ds(pl.multiple_of(r * PITCH + start, 8), TALL), :] = a
                qx[pl.ds(pl.multiple_of((r + 1) * PITCH + start, 8), TALL), :] = b
        kp = jnp.dot(normed, wk[...], preferred_element_type=F32)
        vp = jnp.dot(normed, wv[...], preferred_element_type=F32)
        for j in range(2):
            cut = slice(j * 128, j * 128 + 128)
            ku = rotate(kp[:, cut], cos_b, sin_b)
            vu = vp[:, cut].astype(BF16).astype(F32)
            kn[at, cut] = ku
            vn[at, cut] = vu
            knt_ref[cut, at] = ku.T.astype(BF16)
            vnt_ref[cut, at] = vu.T.astype(BF16)
        return 0

    with jax.named_scope('project'):
        lax.fori_loop(0, rows // TALL, project, 0)
    with jax.named_scope('barrier'):
        pl.semaphore_wait(barrier, 4)

    lane = lax.broadcasted_iota(jnp.int32, (8, 128), 1)
    row = lax.broadcasted_iota(jnp.int32, (8, 128), 0)
    low = lane < 64
    keep_w = (row < 4) == low
    stat = lane % 8
    even = (lane % 2) == 0
    keep_s = (row < 4) == even
    pair_of = lane // 8
    pos = lax.broadcasted_iota(jnp.int32, (16, span), 1)
    zero8 = jnp.zeros((8, 128), F32)
    first_pos = sp * span

    def pack(a, b, pick, keep):
        same = jnp.where(pick, a, b)
        other = pltpu.roll(jnp.where(pick, b, a), 4, 0)
        return jnp.where(keep, same, other)

    def queries(b):
        qa = qx[pl.ds(b, 8, stride=PITCH), :]
        qb = qx[pl.ds(b + 8 * PITCH, 8, stride=PITCH), :]
        return qa, qb

    def score(g, j):
        qa, qb = queries(g * GROUP + j)
        q = jnp.concatenate([jnp.concatenate([qa, zero8], 1), jnp.concatenate([zero8, qb], 1)], 0).astype(BF16)
        return jnp.dot(q, kring[lax.rem(g, SLOTS), j], preferred_element_type=F32)

    def weigh(g, side, j, s):
        b = g * GROUP + j
        qa, qb = queries(b)
        left = len_sm[b] - first_pos
        s = jnp.where(pos < left, s, -jnp.inf)
        k_self = kn[pl.ds(b, 1), :]
        s_self = jnp.sum(jnp.concatenate([qa * k_self[:, :128], qb * k_self[:, 128:]], 0), axis=1, keepdims=True)
        owner = jnp.logical_and(left >= 0, left < span)
        s_self = s_self + jnp.where(owner, 0.0, -jnp.inf)
        top = jnp.maximum(jnp.maximum(jnp.max(s, axis=1, keepdims=True), s_self), LOWEST)
        w = jnp.exp(s - top)
        w_self = jnp.exp(s_self - top)
        denom = jnp.sum(w, axis=1, keepdims=True) + w_self
        prob[side, 16 * j:16 * j + 16, :] = w.astype(BF16)
        self_w[side, 16 * j:16 * j + 16, :] = jnp.broadcast_to(w_self, (16, 128))
        return jnp.where(stat < 2, top[:8], jnp.where(stat < 4, top[8:], jnp.where(stat < 6, denom[:8], denom[8:])))

    def value(g, side, j):
        v_self = vn[pl.ds(g * GROUP + j, 1), :]
        part_b = lax.dot_general(prob[side, 16 * j:16 * j + 16, :], vring[lax.rem(g, SLOTS), j],
                                 (((1,), (1,)), ((), ())), preferred_element_type=F32)
        ca = part_b[:8, :128] + self_w[side, 16 * j:16 * j + 8, :] * v_self[:, :128]
        cb = part_b[8:, 128:] + self_w[side, 16 * j + 8:16 * j + 16, :] * v_self[:, 128:]
        return ca, cb

    def pair_row(p):
        return 8 * p if 8 * p < STATS else 8 * p + 8

    def attend(score_g, value_g):
        if score_g is not None:
            g, side = score_g
            scores = [score(g, j) for j in range(GROUP)]
            tile = zero8
        for p in range(GROUP // 2):
            if value_g is not None:
                v, vside = value_g
                e, o = value(v, vside, 2 * p), value(v, vside, 2 * p + 1)
                r = pair_row(p)
                own[v, r:r + 8, 0:128] = pack(e[0], o[0], low, keep_w)
                own[v, r:r + 8, 128:256] = pack(e[1], o[1], low, keep_w)
            if score_g is not None:
                e = weigh(g, side, 2 * p, scores[2 * p])
                o = weigh(g, side, 2 * p + 1, scores[2 * p + 1])
                tile = jnp.where(pair_of == p, pack(e, o, even, keep_s), tile)
        if score_g is not None:
            own[g, STATS:STATS + 8, 0:128] = tile
            own[g, STATS:STATS + 8, 128:256] = zero8

    is_top = stat < 4

    def spread(f, p, t):
        c = p * 8 + 2 * t
        return jnp.where(low, jnp.broadcast_to(f[:, c:c + 1], (8, 128)), jnp.broadcast_to(f[:, c + 1:c + 2], (8, 128)))

    def factors(a_ref, a, b_ref, b):
        sa, sb = a_ref[a, STATS:STATS + 8, 0:128], b_ref[b, STATS:STATS + 8, 0:128]
        top = jnp.maximum(sa, sb)
        fa, fb = jnp.exp(sa - top), jnp.exp(sb - top)
        denom = sa * pltpu.roll(fa, 4, 1) + sb * pltpu.roll(fb, 4, 1)
        return fa, fb, denom, jnp.where(is_top, top, denom)

    def pairs(side, values):
        if side is None:
            return [pair_row(p) for p in range(GROUP // 2)], values
        rows_of = [pl.multiple_of((STATS + 8) * side + 8 * p, 8) for p in range(GROUP // 4)]
        return rows_of, tuple(jnp.where(side == 1, pltpu.roll(f, 96, 1), f) for f in values)

    def blend(a_ref, a, b_ref, b, found, side, out_ref, out):
        at, (fa, fb) = pairs(side, found[:2])
        for p, r in enumerate(at):
            for t in range(2):
                c = slice(t * 128, t * 128 + 128)
                r8 = pl.ds(r, 8)
                out_ref[out, r8, c] = a_ref[a, r8, c] * spread(fa, p, t) + b_ref[b, r8, c] * spread(fb, p, t)
        out_ref[out, STATS:STATS + 8, 0:128] = found[3]
        out_ref[out, STATS:STATS + 8, 128:256] = zero8

    def finish(a_ref, a, b_ref, b, side, unit):
        found = factors(a_ref, a, b_ref, b)
        at, (fa, fb, denom) = pairs(side, found[:3])
        for p, r in enumerate(at):
            for t in range(2):
                c = slice(t * 128, t * 128 + 128)
                r8 = pl.ds(r, 8)
                w = a_ref[a, r8, c] * spread(fa, p, t) + b_ref[b, r8, c] * spread(fb, p, t)
                base = t * (ctx.shape[0] // 2) + unit * 4 * GROUP + 8 * p
                ctx[base:base + 8, :] = w / spread(denom, p, 2 + t)

    starts = [sum(CHUNKS[:c]) for c in range(len(CHUNKS))]

    def remote(c, kind, src, dst, peer):
        return pltpu.make_async_remote_copy(
            src_ref=src, dst_ref=dst, send_sem=send_sem.at[c, kind], recv_sem=recv_sem.at[c, kind],
            device_id=device(*peer), device_id_type=MESH)

    units = [max(n // 4, 1) for n in CHUNKS]
    blocks_at = [sum(units[:c]) for c in range(len(CHUNKS))]
    columns = width // 2

    def quarter_rows(c):
        return CHUNKS[c] * GROUP // 4

    def quarters(c):
        return pl.ds(starts[c] * GROUP // 4, quarter_rows(c))

    def to_partner(c):
        n = CHUNKS[c] // 2
        src = own.at[pl.ds(starts[c] + (1 - core) * n, n)]
        return remote(c, 0, src, part.at[pl.ds(starts[c] // 2, n)], (0, 1, 0))

    def over_x(c):
        if CHUNKS[c] < 4:
            at = blocks_at[c], pl.ds(pl.multiple_of(STATS * (1 - x), 8), STATS + 8)
        else:
            at = pl.ds(blocks_at[c], units[c])
        return remote(c, 1, send2.at[at], recv2.at[at], (1, 0, 0))

    def over_y(c):
        return remote(c, 2, away.at[quarters(c)], recv3.at[quarters(c)], (0, 0, 1))

    def home(c, dx, dcore, dtp):
        n = quarter_rows(c)
        at = pl.ds(pl.multiple_of(starts[c] * GROUP + ((core ^ dcore) * 2 + (x ^ dx)) * n, 8), n)
        return total.at[at, pl.ds(pl.multiple_of((tp ^ dtp) * columns, columns), columns)]

    def spread_own(c, kind, peer):
        return remote(c, kind, home(c, 0, 0, 0), home(c, 0, 0, 0), peer)

    def forward(c, kind, origin):
        return remote(c, kind, home(c, *origin), home(c, *origin), (0, 1, 0))

    passed = ((7, (1, 0, 0)), (8, (0, 0, 1)), (9, (1, 0, 1)))
    first_peer, other_peer = (1 - core, 0, core), (core, 0, 1 - core)

    def sent(c):
        copies = [spread_own(c, 4, (1, 0, 0)), spread_own(c, 5, (0, 0, 1)), spread_own(c, 3, (0, 1, 0))]
        if c in DIRECT:
            copies.append(spread_own(c, 6, (1, 0, 1)))
        return copies

    def relay(c):
        return remote(c, 6, home(c, *first_peer), home(c, *first_peer), other_peer)

    def step1(c):
        to_partner(c).start()

    def step2(c):
        n = units[c]
        with jax.named_scope(f'wait2_{c}'):
            to_partner(c).wait_recv()
        work = []
        for dx in (1, 0):
            side = x ^ dx
            for i in range(n):
                if CHUNKS[c] < 4:
                    a, b, half = starts[c] + core, starts[c] // 2, side
                else:
                    a, b, half = starts[c] + (core * 2 + side) * n + i, starts[c] // 2 + side * n + i, None
                work.append((a, b, half, factors(own, a, part, b), (mine, send2)[dx], blocks_at[c] + i))
        for k, (a, b, half, found, out_ref, out) in enumerate(work):
            blend(own, a, part, b, found, half, out_ref, out)
            if k == n - 1:
                over_x(c).start()

    def step3(c):
        if c == 0:
            load_wo.wait()
        with jax.named_scope(f'wait3_{c}'):
            over_x(c).wait_recv()
        for i in range(units[c]):
            at = blocks_at[c] + i
            finish(mine, at, recv2, at, x if CHUNKS[c] < 4 else None, i)
        m = quarter_rows(c)
        side = ctx.shape[0] // 2
        lhs = [jnp.concatenate([ctx[pl.ds(t * side + g, m, stride=4), :] for t in range(2)], 1).astype(BF16) for g in range(4)]
        for out_ref, which in ((away, 1 - tp), (keep, tp)):
            for col in range(columns // 256):
                cut = pl.ds(pl.multiple_of(which * columns + col * 256, 256), 256)
                acc = None
                for g in range(4):
                    rhs = jnp.concatenate([wo[h * 256 + g * 64:h * 256 + g * 64 + 64, cut] for h in range(4)], 0)
                    term = jnp.dot(lhs[g], rhs, preferred_element_type=F32)
                    acc = term if acc is None else acc + term
                out_ref[quarters(c), col * 256:col * 256 + 256] = acc
            if out_ref is away:
                over_y(c).start()

    def step4(c):
        with jax.named_scope(f'wait4_{c}'):
            over_y(c).wait_recv()
        home(c, 0, 0, 0)[...] = keep[quarters(c), :] + recv3[quarters(c), :]
        for copy in sent(c):
            copy.start()

    def step5(c):
        with jax.named_scope(f'wait5_{c}'):
            spread_own(c, 4 + core, (0, 1, 0)).wait_recv()
        if c not in DIRECT:
            relay(c).start()
        forward(c, 7 + core, first_peer).start()

    def step6(c):
        with jax.named_scope(f'wait6a_{c}'):
            spread_own(c, 5 - core, (0, 1, 0)).wait_recv()
        forward(c, 8 - core, other_peer).start()
        with jax.named_scope(f'wait6b_{c}'):
            spread_own(c, 6, (0, 1, 0)).wait_recv()
        forward(c, 9, (1, 0, 1)).start()

    def out_copy(c):
        at = pl.ds(starts[c] * GROUP, CHUNKS[c] * GROUP)
        return pltpu.make_async_copy(stage.at[at], out_hbm.at[at], out_sem.at[c])

    def step7(c):
        with jax.named_scope(f'wait7_{c}'):
            spread_own(c, 3, (0, 1, 0)).wait_recv()
            for kind, origin in passed:
                forward(c, kind, origin).wait_recv()

        def body(i, _):
            at = pl.ds(pl.multiple_of((starts[c] + i) * GROUP, GROUP), GROUP)
            stage[at, :] = (hid[at, :].astype(F32) + total[at, :]).astype(BF16)
            return 0

        lax.fori_loop(0, CHUNKS[c], body, 0)
        out_copy(c).start()

    def scoped(i, c):
        with jax.named_scope(f'step{i + 1}_{c}'):
            steps[i](c)

    steps = (step1, step2, step3, step4, step5, step6, step7)
    def wait_for(keys, values):
        for g in keys:
            ring_copy(0, g).wait()
        for g in values:
            ring_copy(1, g).wait()

    def refill(which, g):
        @pl.when(g + SLOTS < groups)
        def _():
            ring_copy(which, g + SLOTS).start()

    wait_for((0,), ())
    with jax.named_scope('attend'):
        attend((0, 0), None)
    refill(0, 0)

    def loop(i, _):
        g = 2 * i
        with jax.named_scope('ring_wait'):
            wait_for((g + 1, g + 2), (g, g + 1))
        with jax.named_scope('attend'):
            attend((g + 1, 1), (g, 0))
            attend((g + 2, 0), (g + 1, 1))
        refill(0, g + 1)
        refill(1, g)
        refill(0, g + 2)
        refill(1, g + 1)
        for when in sorted({e[0] for e in INSIDE}):
            @pl.when(i == when)
            def _():
                for at, c, k in INSIDE:
                    if at == when:
                        scoped(k - 1, c)
        return 0

    trips = groups // 2 - 1
    lax.fori_loop(0, trips, loop, 0)
    last = groups - 2
    with jax.named_scope('ring_wait'):
        wait_for((last + 1,), (last, last + 1))
    with jax.named_scope('attend'):
        attend((last + 1, 1), (last, 0))
        attend(None, (last + 1, 1))
    for c, k in AFTER:
        scoped(k - 1, c)
    with jax.named_scope('finish'):
        for c in range(len(CHUNKS)):
            to_partner(c).wait_send()
            over_x(c).wait_send()
            over_y(c).wait_send()
            for copy in sent(c):
                copy.wait_send()
            if c not in DIRECT:
                relay(c).wait_send()
            for kind, origin in passed:
                forward(c, kind, origin).wait_send()
            out_copy(c).wait()


def copy_kernel(*refs):
    n = len(refs) // 4
    sources, results, staged = refs[:n], refs[n:2 * n], refs[2 * n:3 * n]
    sems = refs[3 * n:]
    pieces = []
    for src, dst, mid, sem in zip(sources, results, staged, sems):
        count = src.shape[0] // 64
        for i in range(count):
            at = pl.ds(i * 64, 64)
            pieces.append((pltpu.make_async_copy(src.at[at], mid.at[at], sem.at[i, 0]),
                           pltpu.make_async_copy(mid.at[at], dst.at[at], sem.at[i, 1])))
    for load, _ in pieces:
        load.start()
    for load, save in pieces:
        load.wait()
        save.start()
    for _, save in pieces:
        save.wait()


def solution(mesh):
    def local_step(hidden, ln_gain, ln_bias, w_q, w_k, w_v, w_o, k_cache, v_cache, lengths):
        rows, span, kv_local, head_dim = k_cache.shape
        width = hidden.shape[1]
        kv_width = kv_local * head_dim
        q_width = w_q.shape[1]
        groups = rows // GROUP
        keys = jnp.transpose(k_cache, (0, 2, 3, 1)).reshape(rows, kv_width, span)
        values = jnp.transpose(v_cache, (0, 2, 3, 1)).reshape(rows, kv_width, span)
        half_rot = head_dim // 4
        inv_freq = np.power(10000.0, -2.0 * np.arange(half_rot) / (2 * half_rot)).astype(np.float32)
        inv_freq = jnp.asarray(np.broadcast_to(inv_freq[:, None], (half_rot, 128)).copy())
        vmem = pl.BlockSpec(memory_space=pltpu.VMEM)
        hbm = pl.BlockSpec(memory_space=pl.ANY)
        n = len(CHUNKS)
        out, k_new, v_new = pl.pallas_call(
            attention_kernel,
            out_shape=(jax.ShapeDtypeStruct((rows, width), BF16),
                       jax.ShapeDtypeStruct((kv_width, rows), BF16),
                       jax.ShapeDtypeStruct((kv_width, rows), BF16)),
            in_specs=[hbm] * 12,
            out_specs=(hbm, vmem, vmem),
            scratch_shapes=[
                pltpu.SMEM((rows,), jnp.int32),
                pltpu.VMEM((1, rows), jnp.int32),
                pltpu.VMEM((half_rot, 128), F32),
                pltpu.VMEM((width // 128, 128), BF16),
                pltpu.VMEM((width // 128, 128), BF16),
                pltpu.VMEM((rows, width), BF16),
                pltpu.VMEM((width, q_width), BF16),
                pltpu.VMEM((width, kv_width), BF16),
                pltpu.VMEM((width, kv_width), BF16),
                pltpu.VMEM((q_width, width), BF16),
                pltpu.VMEM((SLOTS, GROUP, kv_width, span), BF16),
                pltpu.VMEM((SLOTS, GROUP, kv_width, span), BF16),
                pltpu.VMEM((rows, width), BF16),
                pltpu.VMEM((rows, 128), F32),
                pltpu.VMEM((rows, 128), F32),
                pltpu.VMEM((16 * PITCH, 128), F32),
                pltpu.VMEM((rows, kv_width), F32),
                pltpu.VMEM((rows, kv_width), F32),
                pltpu.VMEM((2, 16 * GROUP, span), BF16),
                pltpu.VMEM((2, 16 * GROUP, 128), F32),
                pltpu.VMEM((groups, BLOCK, 256), F32),
                pltpu.VMEM((groups // 2, BLOCK, 256), F32),
                pltpu.VMEM((sum(max(c // 4, 1) for c in CHUNKS), BLOCK, 256), F32),
                pltpu.VMEM((sum(max(c // 4, 1) for c in CHUNKS), BLOCK, 256), F32),
                pltpu.VMEM((sum(max(c // 4, 1) for c in CHUNKS), BLOCK, 256), F32),
                pltpu.VMEM((2 * (max(CHUNKS) // 4) * GROUP * 4, 128), F32),
                pltpu.VMEM((rows // 4, width // 2), F32),
                pltpu.VMEM((rows // 4, width // 2), F32),
                pltpu.VMEM((rows // 4, width // 2), F32),
                pltpu.VMEM((rows, width), F32),
                pltpu.SemaphoreType.DMA((SLOTS, 2)),
                pltpu.SemaphoreType.DMA((9 + rows // 128,)),
                pltpu.SemaphoreType.DMA((n,)),
                pltpu.SemaphoreType.DMA((n, 10)),
                pltpu.SemaphoreType.DMA((n, 10)),
            ],
            compiler_params=pltpu.CompilerParams(
                collective_id=0, has_side_effects=True, vmem_limit_bytes=67043328),
        )(lengths, lengths.reshape(1, rows), inv_freq, ln_gain.reshape(width // 128, 128), ln_bias.reshape(width // 128, 128),
          hidden, w_q, w_k, w_v, w_o, keys, values)
        arrays = (out, k_new, v_new)
        out, k_new, v_new = pl.pallas_call(
            copy_kernel,
            out_shape=[jax.ShapeDtypeStruct(a.shape, a.dtype) for a in arrays],
            in_specs=[hbm] * 3,
            out_specs=[hbm] * 3,
            scratch_shapes=[pltpu.VMEM(a.shape, a.dtype) for a in arrays]
            + [pltpu.SemaphoreType.DMA((a.shape[0] // 64, 2)) for a in arrays],
            compiler_params=pltpu.CompilerParams(vmem_limit_bytes=67043328),
        )(*arrays)
        k_new = jnp.transpose(k_new.reshape(kv_local, head_dim, rows), (2, 0, 1))
        v_new = jnp.transpose(v_new.reshape(kv_local, head_dim, rows), (2, 0, 1))
        return out, k_new, v_new

    row_spec = P('dp', None)
    cache_spec = P('dp', 'sp', 'tp', None)
    head_spec = P('dp', 'tp', None)
    return jax.shard_map(local_step, mesh=mesh, in_specs=(row_spec, P(None), P(None), P(None, 'tp'), P(None, 'tp'), P(None, 'tp'), P('tp', None), cache_spec, cache_spec, P('dp')), out_specs=(row_spec, head_spec, head_spec), check_vma=False)
```

```python
import jax
import jax.numpy as jnp
import numpy as np
from jax import lax
from jax.experimental import pallas as pl
from jax.experimental.pallas import tpu as pltpu
from jax.sharding import PartitionSpec as P

MESH = pl.DeviceIdType.MESH
F32 = jnp.float32
BF16 = jnp.bfloat16
LOWEST = float(jnp.finfo(jnp.float32).min)

GROUP = 16
BLOCK = 4 * GROUP + 8

CHUNKS = (8, 4, 4, 4, 4, 4, 2, 2)
DIRECT = (7,)
INSIDE = ((3, 0, 1), (4, 0, 2), (5, 1, 1), (6, 1, 2), (7, 0, 3), (7, 2, 1), (8, 2, 2), (8, 1, 3), (9, 0, 4), (9, 3, 1),
          (10, 2, 3), (10, 3, 2), (10, 1, 4), (11, 4, 1), (12, 0, 5), (12, 4, 2), (12, 3, 3), (13, 2, 4), (13, 1, 5), (13,
          5, 1), (14, 5, 2), (14, 3, 4), (14, 6, 1))
AFTER = ((2, 5), (7, 1), (4, 3), (6, 2), (7, 2), (5, 3), (3, 5), (4, 4), (6, 3), (7, 3), (3, 6), (5, 4), (2, 6), (0, 6),
         (4, 5), (3, 7), (6, 4), (2, 7), (7, 4), (1, 6), (5, 5), (6, 5), (4, 6), (1, 7), (4, 7), (0, 7), (7, 5), (7, 6),
         (5, 6), (6, 6), (7, 7), (5, 7), (6, 7))
SLOTS = 7
TALL = 256
STATS = 32
PITCH = 520


def attention_kernel(len_hbm, len_row_hbm, inv_freq_hbm, gain_hbm, bias_hbm, hid_hbm, wq_hbm, wk_hbm, wv_hbm, wo_hbm, k_hbm, v_hbm,
                     out_hbm, knt_hbm, vnt_hbm,
                     knt_ref, vnt_ref, len_sm, len_row, inv_freq, gain, bias, hid, wq, wk, wv, wo, kring, vring, stage, cos_t, sin_t, qx, kn, vn,
                     prob, self_w, own, part, send2, mine, recv2, ctx, away, keep, recv3, total,
                     ring_sem, load_sem, out_sem, send_sem, recv_sem):
    rows, width = hid.shape
    groups = rows // GROUP
    span = k_hbm.shape[2]
    tp = lax.axis_index('tp')
    sp = lax.axis_index('sp')
    x, core = sp // 2, sp % 2

    def ring_copy(which, g):
        slot = lax.rem(g, SLOTS)
        src, ring = ((k_hbm, kring), (v_hbm, vring))[which]
        return pltpu.make_async_copy(src.at[pl.ds(g * GROUP, GROUP)], ring.at[slot], ring_sem.at[slot, which])

    blocks = rows // 128

    def load_hid(i):
        at = pl.ds(i * 128, 128)
        return pltpu.make_async_copy(hid_hbm.at[at], hid.at[at], load_sem.at[4 + i])

    load_wk = pltpu.make_async_copy(wk_hbm, wk, load_sem.at[0])
    load_wv = pltpu.make_async_copy(wv_hbm, wv, load_sem.at[1])
    load_wq = pltpu.make_async_copy(wq_hbm, wq, load_sem.at[2])
    load_wo = pltpu.make_async_copy(wo_hbm, wo, load_sem.at[3])
    small = [pltpu.make_async_copy(src, dst, load_sem.at[4 + blocks + i]) for i, (src, dst) in enumerate(
        ((len_row_hbm, len_row), (inv_freq_hbm, inv_freq), (gain_hbm, gain), (bias_hbm, bias), (len_hbm, len_sm)))]
    for copy in small:
        copy.start()
    for i in range(blocks):
        load_hid(i).start()
    load_wq.start()
    load_wk.start()
    load_wv.start()
    for which in range(2):
        ring_copy(which, 0).start()

    def device(dx, dcore, dtp):
        return {'sp': (x ^ dx) * 2 + (core ^ dcore), 'tp': tp ^ dtp}

    barrier = pltpu.get_barrier_semaphore()
    for peer in ((0, 1, 0), (1, 0, 0), (0, 0, 1), (1, 0, 1)):
        pl.semaphore_signal(barrier, inc=1, device_id=device(*peer), device_id_type=MESH)

    for copy in small:
        copy.wait()
    angle = inv_freq[:, 0:1] * len_row[0:1, :].astype(F32)
    cos_a, sin_a = jnp.cos(angle), jnp.sin(angle)
    one, zero = jnp.ones((32, rows), F32), jnp.zeros((32, rows), F32)
    cos_full = jnp.concatenate([cos_a, cos_a, one] * 2, axis=0)
    sin_full = jnp.concatenate([-sin_a, sin_a, zero] * 2, axis=0)
    for blk in range(rows // 128):
        cut = slice(blk * 128, blk * 128 + 128)
        cos_t[cut, :] = cos_full[:, cut].T
        sin_t[cut, :] = sin_full[:, cut].T

    gain_f, bias_f = gain[...].astype(F32), bias[...].astype(F32)
    gain_f = 1.0 + jnp.concatenate([gain_f[i:i + 1] for i in range(width // 128)], 1)
    bias_f = jnp.concatenate([bias_f[i:i + 1] for i in range(width // 128)], 1)

    def norm(i, _):
        for j in range(4):
            at = pl.ds(pl.multiple_of(i * 64 + j * 16, 16), 16)
            wide = hid[at, :].astype(F32)
            centred = wide - jnp.mean(wide, axis=-1, keepdims=True)
            var = jnp.mean(centred * centred, axis=-1, keepdims=True)
            stage[at, :] = (centred * lax.rsqrt(var + 1e-5) * gain_f + bias_f).astype(BF16)
        return 0

    for i in range(blocks):
        with jax.named_scope(f'load_hid{i}'):
            load_hid(i).wait()
        if i == 1:
            for g in range(1, SLOTS):
                for which in range(2):
                    ring_copy(which, g).start()
            load_wo.start()
        with jax.named_scope('norm'):
            lax.fori_loop(2 * i, 2 * i + 2, norm, 0)

    with jax.named_scope('load_w'):
        load_wk.wait()
        load_wv.wait()
        load_wq.wait()
    lane_rb = lax.broadcasted_iota(jnp.int32, (TALL, 128), 1)
    low_half = lane_rb < 64
    first_rot = (lane_rb % 64) < 16

    def rotate(u, cos_b, sin_b):
        partner = jnp.where(first_rot, pltpu.roll(u, 112, 1), pltpu.roll(u, 16, 1))
        return (u * cos_b + partner * sin_b).astype(BF16).astype(F32)

    def project(i, _):
        start = pl.multiple_of(i * TALL, TALL)
        at = pl.ds(start, TALL)
        normed = stage[at, :]
        cos_b, sin_b = cos_t[at, :], sin_t[at, :]
        for head in range(4):
            q = jnp.dot(normed, wq[:, head * 256:head * 256 + 256], preferred_element_type=F32)
            for j in range(2):
                u = rotate(q[:, j * 128:j * 128 + 128], cos_b, sin_b) * 0.125
                swap = pltpu.roll(u, 64, 1)
                if head % 2 == 0:
                    a, b = jnp.where(low_half, u, 0.0), jnp.where(low_half, swap, 0.0)
                else:
                    a, b = jnp.where(low_half, 0.0, swap), jnp.where(low_half, 0.0, u)
                r = head * 4 + 2 * j
                qx[pl.ds(pl.multiple_of(r * PITCH + start, 8), TALL), :] = a
                qx[pl.ds(pl.multiple_of((r + 1) * PITCH + start, 8), TALL), :] = b
        kp = jnp.dot(normed, wk[...], preferred_element_type=F32)
        vp = jnp.dot(normed, wv[...], preferred_element_type=F32)
        for j in range(2):
            cut = slice(j * 128, j * 128 + 128)
            ku = rotate(kp[:, cut], cos_b, sin_b)
            vu = vp[:, cut].astype(BF16).astype(F32)
            kn[at, cut] = ku
            vn[at, cut] = vu
            knt_ref[cut, at] = ku.T.astype(BF16)
            vnt_ref[cut, at] = vu.T.astype(BF16)
        return 0

    with jax.named_scope('project'):
        lax.fori_loop(0, rows // TALL, project, 0)
    new_copies = [pltpu.make_async_copy(src, dst, load_sem.at[4 + blocks + i]) for i, (src, dst) in enumerate(
        ((knt_ref, knt_hbm), (vnt_ref, vnt_hbm)))]
    for copy in new_copies:
        copy.start()
    with jax.named_scope('barrier'):
        pl.semaphore_wait(barrier, 4)

    lane = lax.broadcasted_iota(jnp.int32, (8, 128), 1)
    row = lax.broadcasted_iota(jnp.int32, (8, 128), 0)
    low = lane < 64
    keep_w = (row < 4) == low
    stat = lane % 8
    even = (lane % 2) == 0
    keep_s = (row < 4) == even
    pair_of = lane // 8
    pos = lax.broadcasted_iota(jnp.int32, (16, span), 1)
    zero8 = jnp.zeros((8, 128), F32)
    first_pos = sp * span

    def pack(a, b, pick, keep):
        same = jnp.where(pick, a, b)
        other = pltpu.roll(jnp.where(pick, b, a), 4, 0)
        return jnp.where(keep, same, other)

    def queries(b):
        qa = qx[pl.ds(b, 8, stride=PITCH), :]
        qb = qx[pl.ds(b + 8 * PITCH, 8, stride=PITCH), :]
        return qa, qb

    def score(g, j):
        qa, qb = queries(g * GROUP + j)
        q = jnp.concatenate([jnp.concatenate([qa, zero8], 1), jnp.concatenate([zero8, qb], 1)], 0).astype(BF16)
        return jnp.dot(q, kring[lax.rem(g, SLOTS), j], preferred_element_type=F32)

    def weigh(g, side, j, s):
        b = g * GROUP + j
        qa, qb = queries(b)
        left = len_sm[b] - first_pos
        s = jnp.where(pos < left, s, -jnp.inf)
        k_self = kn[pl.ds(b, 1), :]
        s_self = jnp.sum(jnp.concatenate([qa * k_self[:, :128], qb * k_self[:, 128:]], 0), axis=1, keepdims=True)
        owner = jnp.logical_and(left >= 0, left < span)
        s_self = s_self + jnp.where(owner, 0.0, -jnp.inf)
        top = jnp.maximum(jnp.maximum(jnp.max(s, axis=1, keepdims=True), s_self), LOWEST)
        w = jnp.exp(s - top)
        w_self = jnp.exp(s_self - top)
        denom = jnp.sum(w, axis=1, keepdims=True) + w_self
        prob[side, 16 * j:16 * j + 16, :] = w.astype(BF16)
        self_w[side, 16 * j:16 * j + 16, :] = jnp.broadcast_to(w_self, (16, 128))
        return jnp.where(stat < 2, top[:8], jnp.where(stat < 4, top[8:], jnp.where(stat < 6, denom[:8], denom[8:])))

    def value(g, side, j):
        v_self = vn[pl.ds(g * GROUP + j, 1), :]
        part_b = lax.dot_general(prob[side, 16 * j:16 * j + 16, :], vring[lax.rem(g, SLOTS), j],
                                 (((1,), (1,)), ((), ())), preferred_element_type=F32)
        ca = part_b[:8, :128] + self_w[side, 16 * j:16 * j + 8, :] * v_self[:, :128]
        cb = part_b[8:, 128:] + self_w[side, 16 * j + 8:16 * j + 16, :] * v_self[:, 128:]
        return ca, cb

    def pair_row(p):
        return 8 * p if 8 * p < STATS else 8 * p + 8

    def attend(score_g, value_g):
        if score_g is not None:
            g, side = score_g
            scores = [score(g, j) for j in range(GROUP)]
            tile = zero8
        for p in range(GROUP // 2):
            if value_g is not None:
                v, vside = value_g
                e, o = value(v, vside, 2 * p), value(v, vside, 2 * p + 1)
                r = pair_row(p)
                own[v, r:r + 8, 0:128] = pack(e[0], o[0], low, keep_w)
                own[v, r:r + 8, 128:256] = pack(e[1], o[1], low, keep_w)
            if score_g is not None:
                e = weigh(g, side, 2 * p, scores[2 * p])
                o = weigh(g, side, 2 * p + 1, scores[2 * p + 1])
                tile = jnp.where(pair_of == p, pack(e, o, even, keep_s), tile)
        if score_g is not None:
            own[g, STATS:STATS + 8, 0:128] = tile
            own[g, STATS:STATS + 8, 128:256] = zero8

    is_top = stat < 4

    def spread(f, p, t):
        c = p * 8 + 2 * t
        return jnp.where(low, jnp.broadcast_to(f[:, c:c + 1], (8, 128)), jnp.broadcast_to(f[:, c + 1:c + 2], (8, 128)))

    def factors(a_ref, a, b_ref, b):
        sa, sb = a_ref[a, STATS:STATS + 8, 0:128], b_ref[b, STATS:STATS + 8, 0:128]
        top = jnp.maximum(sa, sb)
        fa, fb = jnp.exp(sa - top), jnp.exp(sb - top)
        denom = sa * pltpu.roll(fa, 4, 1) + sb * pltpu.roll(fb, 4, 1)
        return fa, fb, denom, jnp.where(is_top, top, denom)

    def pairs(side, values):
        if side is None:
            return [pair_row(p) for p in range(GROUP // 2)], values
        rows_of = [pl.multiple_of((STATS + 8) * side + 8 * p, 8) for p in range(GROUP // 4)]
        return rows_of, tuple(jnp.where(side == 1, pltpu.roll(f, 96, 1), f) for f in values)

    def blend(a_ref, a, b_ref, b, found, side, out_ref, out):
        at, (fa, fb) = pairs(side, found[:2])
        for p, r in enumerate(at):
            for t in range(2):
                c = slice(t * 128, t * 128 + 128)
                r8 = pl.ds(r, 8)
                out_ref[out, r8, c] = a_ref[a, r8, c] * spread(fa, p, t) + b_ref[b, r8, c] * spread(fb, p, t)
        out_ref[out, STATS:STATS + 8, 0:128] = found[3]
        out_ref[out, STATS:STATS + 8, 128:256] = zero8

    def finish(a_ref, a, b_ref, b, side, unit):
        found = factors(a_ref, a, b_ref, b)
        at, (fa, fb, denom) = pairs(side, found[:3])
        for p, r in enumerate(at):
            for t in range(2):
                c = slice(t * 128, t * 128 + 128)
                r8 = pl.ds(r, 8)
                w = a_ref[a, r8, c] * spread(fa, p, t) + b_ref[b, r8, c] * spread(fb, p, t)
                base = t * (ctx.shape[0] // 2) + unit * 4 * GROUP + 8 * p
                ctx[base:base + 8, :] = w / spread(denom, p, 2 + t)

    starts = [sum(CHUNKS[:c]) for c in range(len(CHUNKS))]

    def remote(c, kind, src, dst, peer, arrival=None):
        sem = {0: 0, 1: 9 + c}[kind] if isinstance(kind, int) and kind < 2 else kind - 1
        return pltpu.make_async_remote_copy(
            src_ref=src, dst_ref=dst, send_sem=send_sem.at[sem],
            recv_sem=recv_sem.at[c, kind if arrival is None else arrival],
            device_id=device(*peer), device_id_type=MESH)

    units = [max(n // 4, 1) for n in CHUNKS]
    blocks_at = [sum(units[:c]) for c in range(len(CHUNKS))]
    columns = width // 2

    def quarter_rows(c):
        return CHUNKS[c] * GROUP // 4

    def quarters(c):
        return pl.ds(starts[c] * GROUP // 4, quarter_rows(c))

    def to_partner(c):
        n = CHUNKS[c] // 2
        src = own.at[pl.ds(starts[c] + (1 - core) * n, n)]
        return remote(c, 0, src, part.at[pl.ds(starts[c] // 2, n)], (0, 1, 0))

    def over_x(c):
        if CHUNKS[c] < 4:
            at = blocks_at[c], pl.ds(pl.multiple_of(STATS * (1 - x), 8), STATS + 8)
        else:
            at = pl.ds(blocks_at[c], units[c])
        return remote(c, 1, send2.at[at], recv2.at[at], (1, 0, 0))

    def over_y(c):
        return remote(c, 2, away.at[quarters(c)], recv3.at[quarters(c)], (0, 0, 1))

    def home(c, dx, dcore, dtp):
        n = quarter_rows(c)
        at = pl.ds(pl.multiple_of(starts[c] * GROUP + ((core ^ dcore) * 2 + (x ^ dx)) * n, 8), n)
        return total.at[at, pl.ds(pl.multiple_of((tp ^ dtp) * columns, columns), columns)]

    def spread_own(c, kind, peer):
        return remote(c, kind, home(c, 0, 0, 0), home(c, 0, 0, 0), peer)

    def forward(c, kind, origin):
        return remote(c, kind, home(c, *origin), home(c, *origin), (0, 1, 0), 3)

    first_peer, other_peer = (1 - core, 0, core), (core, 0, 1 - core)

    def sent(c):
        copies = [spread_own(c, 4, (1, 0, 0)), spread_own(c, 5, (0, 0, 1)), spread_own(c, 3, (0, 1, 0))]
        if c in DIRECT:
            copies.append(spread_own(c, 6, (1, 0, 1)))
        return copies

    def relay(c):
        return remote(c, 6, home(c, *first_peer), home(c, *first_peer), other_peer)

    def step1(c):
        to_partner(c).start()

    def step2(c):
        n = units[c]
        with jax.named_scope(f'wait2_{c}'):
            to_partner(c).wait_recv()
        work = []
        for dx in (1, 0):
            side = x ^ dx
            for i in range(n):
                if CHUNKS[c] < 4:
                    a, b, half = starts[c] + core, starts[c] // 2, side
                else:
                    a, b, half = starts[c] + (core * 2 + side) * n + i, starts[c] // 2 + side * n + i, None
                work.append((a, b, half, factors(own, a, part, b), (mine, send2)[dx], blocks_at[c] + i))
        for k, (a, b, half, found, out_ref, out) in enumerate(work):
            blend(own, a, part, b, found, half, out_ref, out)
            if k == n - 1:
                over_x(c).start()

    def step3(c):
        if c == 0:
            load_wo.wait()
        with jax.named_scope(f'wait3_{c}'):
            over_x(c).wait_recv()
        for i in range(units[c]):
            at = blocks_at[c] + i
            finish(mine, at, recv2, at, x if CHUNKS[c] < 4 else None, i)
        m = quarter_rows(c)
        side = ctx.shape[0] // 2
        lhs = [jnp.concatenate([ctx[pl.ds(t * side + g, m, stride=4), :] for t in range(2)], 1).astype(BF16) for g in range(4)]
        for out_ref, which in ((away, 1 - tp), (keep, tp)):
            for col in range(columns // 256):
                cut = pl.ds(pl.multiple_of(which * columns + col * 256, 256), 256)
                acc = None
                for g in range(4):
                    rhs = jnp.concatenate([wo[h * 256 + g * 64:h * 256 + g * 64 + 64, cut] for h in range(4)], 0)
                    term = jnp.dot(lhs[g], rhs, preferred_element_type=F32)
                    acc = term if acc is None else acc + term
                out_ref[quarters(c), col * 256:col * 256 + 256] = acc
            if out_ref is away:
                over_y(c).start()

    def step4(c):
        with jax.named_scope(f'wait4_{c}'):
            over_y(c).wait_recv()
        home(c, 0, 0, 0)[...] = keep[quarters(c), :] + recv3[quarters(c), :]
        for copy in sent(c):
            copy.start()

    def step5(c):
        with jax.named_scope(f'wait5_{c}'):
            spread_own(c, 4 + core, (0, 1, 0)).wait_recv()
        if c not in DIRECT:
            relay(c).start()
        forward(c, 7 + core, first_peer).start()

    def step6(c):
        with jax.named_scope(f'wait6a_{c}'):
            spread_own(c, 5 - core, (0, 1, 0)).wait_recv()
        forward(c, 8 - core, other_peer).start()
        with jax.named_scope(f'wait6b_{c}'):
            spread_own(c, 6, (0, 1, 0)).wait_recv()
        forward(c, 9, (1, 0, 1)).start()

    def out_copy(c):
        at = pl.ds(starts[c] * GROUP, CHUNKS[c] * GROUP)
        return pltpu.make_async_copy(stage.at[at], out_hbm.at[at], out_sem.at[c])

    def step7(c):
        with jax.named_scope(f'wait7_{c}'):
            four = total.at[pl.ds(starts[c] * GROUP, CHUNKS[c] * GROUP), pl.ds(0, columns)]
            remote(c, 3, four, four, (0, 1, 0)).wait_recv()

        def body(i, _):
            at = pl.ds(pl.multiple_of((starts[c] + i) * GROUP, GROUP), GROUP)
            stage[at, :] = (hid[at, :].astype(F32) + total[at, :]).astype(BF16)
            return 0

        lax.fori_loop(0, CHUNKS[c], body, 0)
        out_copy(c).start()

    def scoped(i, c):
        with jax.named_scope(f'step{i + 1}_{c}'):
            steps[i](c)

    steps = (step1, step2, step3, step4, step5, step6, step7)
    def wait_for(keys, values):
        for g in keys:
            ring_copy(0, g).wait()
        for g in values:
            ring_copy(1, g).wait()

    def refill(which, g):
        @pl.when(g + SLOTS < groups)
        def _():
            ring_copy(which, g + SLOTS).start()

    wait_for((0,), ())
    with jax.named_scope('attend'):
        attend((0, 0), None)
    refill(0, 0)

    def loop(i, _):
        g = 2 * i
        with jax.named_scope('ring_wait'):
            wait_for((g + 1, g + 2), (g, g + 1))
        with jax.named_scope('attend'):
            attend((g + 1, 1), (g, 0))
            attend((g + 2, 0), (g + 1, 1))
        refill(0, g + 1)
        refill(1, g)
        refill(0, g + 2)
        refill(1, g + 1)
        for when in sorted({e[0] for e in INSIDE}):
            @pl.when(i == when)
            def _():
                for at, c, k in INSIDE:
                    if at == when:
                        scoped(k - 1, c)
        return 0

    trips = groups // 2 - 1
    lax.fori_loop(0, trips, loop, 0)
    last = groups - 2
    with jax.named_scope('ring_wait'):
        wait_for((last + 1,), (last, last + 1))
    with jax.named_scope('attend'):
        attend((last + 1, 1), (last, 0))
        attend(None, (last + 1, 1))
    for c, k in AFTER:
        scoped(k - 1, c)
    with jax.named_scope('finish'):
        remote(0, 0, part, part, (0, 1, 0)).wait_send()
        for kind in range(2, 10):
            remote(0, kind, away, away, (0, 1, 0), 3).wait_send()
        for c in range(len(CHUNKS)):
            over_x(c).wait_send()
            out_copy(c).wait()
        for copy in new_copies:
            copy.wait()


def copy_kernel(*refs):
    n = len(refs) // 4
    sources, results, staged = refs[:n], refs[n:2 * n], refs[2 * n:3 * n]
    sems = refs[3 * n:]
    pieces = []
    for src, dst, mid, sem in zip(sources, results, staged, sems):
        count = src.shape[0] // 64
        for i in range(count):
            at = pl.ds(i * 64, 64)
            pieces.append((pltpu.make_async_copy(src.at[at], mid.at[at], sem.at[i, 0]),
                           pltpu.make_async_copy(mid.at[at], dst.at[at], sem.at[i, 1])))
    for load, _ in pieces:
        load.start()
    for load, save in pieces:
        load.wait()
        save.start()
    for _, save in pieces:
        save.wait()


def solution(mesh):
    def local_step(hidden, ln_gain, ln_bias, w_q, w_k, w_v, w_o, k_cache, v_cache, lengths):
        rows, span, kv_local, head_dim = k_cache.shape
        width = hidden.shape[1]
        kv_width = kv_local * head_dim
        q_width = w_q.shape[1]
        groups = rows // GROUP
        keys = jnp.transpose(k_cache, (0, 2, 3, 1)).reshape(rows, kv_width, span)
        values = jnp.transpose(v_cache, (0, 2, 3, 1)).reshape(rows, kv_width, span)
        half_rot = head_dim // 4
        inv_freq = np.power(10000.0, -2.0 * np.arange(half_rot) / (2 * half_rot)).astype(np.float32)
        inv_freq = jnp.asarray(np.broadcast_to(inv_freq[:, None], (half_rot, 128)).copy())
        vmem = pl.BlockSpec(memory_space=pltpu.VMEM)
        hbm = pl.BlockSpec(memory_space=pl.ANY)
        n = len(CHUNKS)
        out, k_new, v_new = pl.pallas_call(
            attention_kernel,
            out_shape=(jax.ShapeDtypeStruct((rows, width), BF16),
                       jax.ShapeDtypeStruct((kv_width, rows), BF16),
                       jax.ShapeDtypeStruct((kv_width, rows), BF16)),
            in_specs=[hbm] * 12,
            out_specs=(hbm, hbm, hbm),
            scratch_shapes=[
                pltpu.VMEM((kv_width, rows), BF16),
                pltpu.VMEM((kv_width, rows), BF16),
                pltpu.SMEM((rows,), jnp.int32),
                pltpu.VMEM((1, rows), jnp.int32),
                pltpu.VMEM((half_rot, 128), F32),
                pltpu.VMEM((width // 128, 128), BF16),
                pltpu.VMEM((width // 128, 128), BF16),
                pltpu.VMEM((rows, width), BF16),
                pltpu.VMEM((width, q_width), BF16),
                pltpu.VMEM((width, kv_width), BF16),
                pltpu.VMEM((width, kv_width), BF16),
                pltpu.VMEM((q_width, width), BF16),
                pltpu.VMEM((SLOTS, GROUP, kv_width, span), BF16),
                pltpu.VMEM((SLOTS, GROUP, kv_width, span), BF16),
                pltpu.VMEM((rows, width), BF16),
                pltpu.VMEM((rows, 128), F32),
                pltpu.VMEM((rows, 128), F32),
                pltpu.VMEM((16 * PITCH, 128), F32),
                pltpu.VMEM((rows, kv_width), F32),
                pltpu.VMEM((rows, kv_width), F32),
                pltpu.VMEM((2, 16 * GROUP, span), BF16),
                pltpu.VMEM((2, 16 * GROUP, 128), F32),
                pltpu.VMEM((groups, BLOCK, 256), F32),
                pltpu.VMEM((groups // 2, BLOCK, 256), F32),
                pltpu.VMEM((sum(max(c // 4, 1) for c in CHUNKS), BLOCK, 256), F32),
                pltpu.VMEM((sum(max(c // 4, 1) for c in CHUNKS), BLOCK, 256), F32),
                pltpu.VMEM((sum(max(c // 4, 1) for c in CHUNKS), BLOCK, 256), F32),
                pltpu.VMEM((2 * (max(CHUNKS) // 4) * GROUP * 4, 128), F32),
                pltpu.VMEM((rows // 4, width // 2), F32),
                pltpu.VMEM((rows // 4, width // 2), F32),
                pltpu.VMEM((rows // 4, width // 2), F32),
                pltpu.VMEM((rows, width), F32),
                pltpu.SemaphoreType.DMA((SLOTS, 2)),
                pltpu.SemaphoreType.DMA((9 + rows // 128,)),
                pltpu.SemaphoreType.DMA((n,)),
                pltpu.SemaphoreType.DMA((9 + n,)),
                pltpu.SemaphoreType.DMA((n, 7)),
            ],
            compiler_params=pltpu.CompilerParams(
                collective_id=0, has_side_effects=True, vmem_limit_bytes=67043328),
        )(lengths, lengths.reshape(1, rows), inv_freq, ln_gain.reshape(width // 128, 128), ln_bias.reshape(width // 128, 128),
          hidden, w_q, w_k, w_v, w_o, keys, values)
        arrays = (out, k_new, v_new)
        out, k_new, v_new = pl.pallas_call(
            copy_kernel,
            out_shape=[jax.ShapeDtypeStruct(a.shape, a.dtype) for a in arrays],
            in_specs=[hbm] * 3,
            out_specs=[hbm] * 3,
            scratch_shapes=[pltpu.VMEM(a.shape, a.dtype) for a in arrays]
            + [pltpu.SemaphoreType.DMA((a.shape[0] // 64, 2)) for a in arrays],
            compiler_params=pltpu.CompilerParams(vmem_limit_bytes=67043328),
        )(*arrays)
        k_new = jnp.transpose(k_new.reshape(kv_local, head_dim, rows), (2, 0, 1))
        v_new = jnp.transpose(v_new.reshape(kv_local, head_dim, rows), (2, 0, 1))
        return out, k_new, v_new

    row_spec = P('dp', None)
    cache_spec = P('dp', 'sp', 'tp', None)
    head_spec = P('dp', 'tp', None)
    return jax.shard_map(local_step, mesh=mesh, in_specs=(row_spec, P(None), P(None), P(None, 'tp'), P(None, 'tp'), P(None, 'tp'), P('tp', None), cache_spec, cache_spec, P('dp')), out_specs=(row_spec, head_spec, head_spec), check_vma=False)
```

```python
import jax
import jax.numpy as jnp
import numpy as np
from jax import lax
from jax.experimental import pallas as pl
from jax.experimental.pallas import tpu as pltpu
from jax.sharding import PartitionSpec as P

MESH = pl.DeviceIdType.MESH
F32 = jnp.float32
BF16 = jnp.bfloat16
LOWEST = float(jnp.finfo(jnp.float32).min)

GROUP = 16
BLOCK = 4 * GROUP + 8

CHUNKS = (8, 4, 4, 4, 4, 4, 2, 2)
DIRECT = (7,)
INSIDE = ((3, 0, 1), (4, 0, 2), (5, 1, 1), (6, 1, 2), (7, 0, 3), (7, 2, 1), (8, 2, 2), (8, 1, 3), (9, 0, 4), (9, 3, 1),
          (10, 2, 3), (10, 3, 2), (10, 1, 4), (11, 4, 1), (12, 0, 5), (12, 4, 2), (12, 3, 3), (13, 2, 4), (13, 1, 5), (13,
          5, 1), (14, 5, 2), (14, 3, 4), (14, 6, 1))
AFTER = ((2, 5), (7, 1), (4, 3), (6, 2), (7, 2), (5, 3), (3, 5), (4, 4), (6, 3), (7, 3), (3, 6), (5, 4), (2, 6), (0, 6),
         (4, 5), (3, 7), (6, 4), (2, 7), (7, 4), (1, 6), (5, 5), (6, 5), (4, 6), (1, 7), (4, 7), (0, 7), (7, 5), (7, 6),
         (5, 6), (6, 6), (7, 7), (5, 7), (6, 7))
SLOTS = 7
TALL = 256
STATS = 32
PITCH = 520


def attention_kernel(len_hbm, len_row_hbm, inv_freq_hbm, gain_hbm, bias_hbm, hid_hbm, wq_hbm, wk_hbm, wv_hbm, wo_hbm, k_hbm, v_hbm,
                     out_hbm, knt_hbm, vnt_hbm,
                     knt_ref, vnt_ref, len_sm, len_row, inv_freq, gain, bias, hid, wq, wk, wv, wo, kring, vring, stage, cos_t, sin_t, qx, kn, vn,
                     prob, self_w, own, part, send2, mine, recv2, ctx, away, keep, recv3, total,
                     ring_sem, load_sem, out_sem, send_sem, recv_sem):
    rows, width = hid.shape
    groups = rows // GROUP
    span = k_hbm.shape[2]
    tp = lax.axis_index('tp')
    sp = lax.axis_index('sp')
    x, core = sp // 2, sp % 2

    def ring_copy(which, g):
        slot = lax.rem(g, SLOTS)
        src, ring = ((k_hbm, kring), (v_hbm, vring))[which]
        return pltpu.make_async_copy(src.at[pl.ds(g * GROUP, GROUP)], ring.at[slot], ring_sem.at[slot, which])

    blocks = rows // 128

    def load_hid(i):
        at = pl.ds(i * 128, 128)
        return pltpu.make_async_copy(hid_hbm.at[at], hid.at[at], load_sem.at[4 + i])

    load_wk = pltpu.make_async_copy(wk_hbm, wk, load_sem.at[0])
    load_wv = pltpu.make_async_copy(wv_hbm, wv, load_sem.at[1])
    load_wq = pltpu.make_async_copy(wq_hbm, wq, load_sem.at[2])

    def load_wo(i):
        at = pl.ds(i * (wo.shape[0] // 2), wo.shape[0] // 2)
        return pltpu.make_async_copy(wo_hbm.at[at], wo.at[at], load_sem.at[(3, 8 + blocks)[i]])

    small = [pltpu.make_async_copy(src, dst, load_sem.at[4 + blocks + i]) for i, (src, dst) in enumerate(
        ((len_row_hbm, len_row), (inv_freq_hbm, inv_freq), (gain_hbm, gain), (bias_hbm, bias), (len_hbm, len_sm)))]
    for copy in small:
        copy.start()
    for i in range(blocks):
        load_hid(i).start()
    load_wq.start()
    load_wk.start()
    load_wv.start()

    def device(dx, dcore, dtp):
        return {'sp': (x ^ dx) * 2 + (core ^ dcore), 'tp': tp ^ dtp}

    barrier = pltpu.get_barrier_semaphore()
    for peer in ((0, 1, 0), (1, 0, 0), (0, 0, 1), (1, 0, 1)):
        pl.semaphore_signal(barrier, inc=1, device_id=device(*peer), device_id_type=MESH)

    for copy in small:
        copy.wait()
    angle = inv_freq[:, 0:1] * len_row[0:1, :].astype(F32)
    cos_a, sin_a = jnp.cos(angle), jnp.sin(angle)
    one, zero = jnp.ones((32, rows), F32), jnp.zeros((32, rows), F32)
    cos_full = jnp.concatenate([cos_a, cos_a, one] * 2, axis=0)
    sin_full = jnp.concatenate([-sin_a, sin_a, zero] * 2, axis=0)
    for blk in range(rows // 128):
        cut = slice(blk * 128, blk * 128 + 128)
        cos_t[cut, :] = cos_full[:, cut].T
        sin_t[cut, :] = sin_full[:, cut].T

    gain_f, bias_f = gain[...].astype(F32), bias[...].astype(F32)
    gain_f = 1.0 + jnp.concatenate([gain_f[i:i + 1] for i in range(width // 128)], 1)
    bias_f = jnp.concatenate([bias_f[i:i + 1] for i in range(width // 128)], 1)

    def norm(i, _):
        for j in range(4):
            at = pl.ds(pl.multiple_of(i * 64 + j * 16, 16), 16)
            wide = hid[at, :].astype(F32)
            centred = wide - jnp.mean(wide, axis=-1, keepdims=True)
            var = jnp.mean(centred * centred, axis=-1, keepdims=True)
            stage[at, :] = (centred * lax.rsqrt(var + 1e-5) * gain_f + bias_f).astype(BF16)
        return 0

    for i in range(blocks):
        with jax.named_scope(f'load_hid{i}'):
            load_hid(i).wait()
        if i in (1, 3):
            for g in (range(1), range(1, SLOTS))[i // 2]:
                for which in range(2):
                    ring_copy(which, g).start()
        with jax.named_scope('norm'):
            lax.fori_loop(2 * i, 2 * i + 2, norm, 0)

    with jax.named_scope('load_w'):
        load_wk.wait()
        load_wv.wait()
        load_wq.wait()
    lane_rb = lax.broadcasted_iota(jnp.int32, (TALL, 128), 1)
    low_half = lane_rb < 64
    first_rot = (lane_rb % 64) < 16

    def rotate(u, cos_b, sin_b):
        partner = jnp.where(first_rot, pltpu.roll(u, 112, 1), pltpu.roll(u, 16, 1))
        return (u * cos_b + partner * sin_b).astype(BF16).astype(F32)

    def project(i, _):
        start = pl.multiple_of(i * TALL, TALL)
        at = pl.ds(start, TALL)
        normed = stage[at, :]
        cos_b, sin_b = cos_t[at, :], sin_t[at, :]
        for head in range(4):
            q = jnp.dot(normed, wq[:, head * 256:head * 256 + 256], preferred_element_type=F32)
            for j in range(2):
                u = rotate(q[:, j * 128:j * 128 + 128], cos_b, sin_b) * 0.125
                swap = pltpu.roll(u, 64, 1)
                if head % 2 == 0:
                    a, b = jnp.where(low_half, u, 0.0), jnp.where(low_half, swap, 0.0)
                else:
                    a, b = jnp.where(low_half, 0.0, swap), jnp.where(low_half, 0.0, u)
                r = head * 4 + 2 * j
                qx[pl.ds(pl.multiple_of(r * PITCH + start, 8), TALL), :] = a
                qx[pl.ds(pl.multiple_of((r + 1) * PITCH + start, 8), TALL), :] = b
        kp = jnp.dot(normed, wk[...], preferred_element_type=F32)
        vp = jnp.dot(normed, wv[...], preferred_element_type=F32)
        for j in range(2):
            cut = slice(j * 128, j * 128 + 128)
            ku = rotate(kp[:, cut], cos_b, sin_b)
            vu = vp[:, cut].astype(BF16).astype(F32)
            kn[at, cut] = ku
            vn[at, cut] = vu
            knt_ref[cut, at] = ku.T.astype(BF16)
            vnt_ref[cut, at] = vu.T.astype(BF16)
        return 0

    with jax.named_scope('project'):
        lax.fori_loop(0, rows // TALL, project, 0)
    new_copies = [pltpu.make_async_copy(src, dst, load_sem.at[4 + blocks + i]) for i, (src, dst) in enumerate(
        ((knt_ref, knt_hbm), (vnt_ref, vnt_hbm)))]
    for copy in new_copies:
        copy.start()
    with jax.named_scope('barrier'):
        pl.semaphore_wait(barrier, 4)

    lane = lax.broadcasted_iota(jnp.int32, (8, 128), 1)
    row = lax.broadcasted_iota(jnp.int32, (8, 128), 0)
    low = lane < 64
    keep_w = (row < 4) == low
    stat = lane % 8
    even = (lane % 2) == 0
    keep_s = (row < 4) == even
    pair_of = lane // 8
    pos = lax.broadcasted_iota(jnp.int32, (16, span), 1)
    zero8 = jnp.zeros((8, 128), F32)
    first_pos = sp * span

    def pack(a, b, pick, keep):
        same = jnp.where(pick, a, b)
        other = pltpu.roll(jnp.where(pick, b, a), 4, 0)
        return jnp.where(keep, same, other)

    def queries(b):
        qa = qx[pl.ds(b, 8, stride=PITCH), :]
        qb = qx[pl.ds(b + 8 * PITCH, 8, stride=PITCH), :]
        return qa, qb

    def score(g, j):
        qa, qb = queries(g * GROUP + j)
        q = jnp.concatenate([jnp.concatenate([qa, zero8], 1), jnp.concatenate([zero8, qb], 1)], 0).astype(BF16)
        return jnp.dot(q, kring[lax.rem(g, SLOTS), j], preferred_element_type=F32)

    def weigh(g, side, j, s):
        b = g * GROUP + j
        qa, qb = queries(b)
        left = len_sm[b] - first_pos
        s = jnp.where(pos < left, s, -jnp.inf)
        k_self = kn[pl.ds(b, 1), :]
        s_self = jnp.sum(jnp.concatenate([qa * k_self[:, :128], qb * k_self[:, 128:]], 0), axis=1, keepdims=True)
        owner = jnp.logical_and(left >= 0, left < span)
        s_self = s_self + jnp.where(owner, 0.0, -jnp.inf)
        top = jnp.maximum(jnp.maximum(jnp.max(s, axis=1, keepdims=True), s_self), LOWEST)
        w = jnp.exp(s - top)
        w_self = jnp.exp(s_self - top)
        denom = jnp.sum(w, axis=1, keepdims=True) + w_self
        prob[side, 16 * j:16 * j + 16, :] = w.astype(BF16)
        self_w[side, 16 * j:16 * j + 16, :] = jnp.broadcast_to(w_self, (16, 128))
        return jnp.where(stat < 2, top[:8], jnp.where(stat < 4, top[8:], jnp.where(stat < 6, denom[:8], denom[8:])))

    def value(g, side, j):
        v_self = vn[pl.ds(g * GROUP + j, 1), :]
        part_b = lax.dot_general(prob[side, 16 * j:16 * j + 16, :], vring[lax.rem(g, SLOTS), j],
                                 (((1,), (1,)), ((), ())), preferred_element_type=F32)
        ca = part_b[:8, :128] + self_w[side, 16 * j:16 * j + 8, :] * v_self[:, :128]
        cb = part_b[8:, 128:] + self_w[side, 16 * j + 8:16 * j + 16, :] * v_self[:, 128:]
        return ca, cb

    def pair_row(p):
        return 8 * p if 8 * p < STATS else 8 * p + 8

    def attend(score_g, value_g):
        if score_g is not None:
            g, side = score_g
            scores = [score(g, j) for j in range(GROUP)]
            tile = zero8
        for p in range(GROUP // 2):
            if value_g is not None:
                v, vside = value_g
                e, o = value(v, vside, 2 * p), value(v, vside, 2 * p + 1)
                r = pair_row(p)
                own[v, r:r + 8, 0:128] = pack(e[0], o[0], low, keep_w)
                own[v, r:r + 8, 128:256] = pack(e[1], o[1], low, keep_w)
            if score_g is not None:
                e = weigh(g, side, 2 * p, scores[2 * p])
                o = weigh(g, side, 2 * p + 1, scores[2 * p + 1])
                tile = jnp.where(pair_of == p, pack(e, o, even, keep_s), tile)
        if score_g is not None:
            own[g, STATS:STATS + 8, 0:128] = tile
            own[g, STATS:STATS + 8, 128:256] = zero8

    is_top = stat < 4

    def spread(f, p, t):
        c = p * 8 + 2 * t
        return jnp.where(low, jnp.broadcast_to(f[:, c:c + 1], (8, 128)), jnp.broadcast_to(f[:, c + 1:c + 2], (8, 128)))

    def factors(a_ref, a, b_ref, b):
        sa, sb = a_ref[a, STATS:STATS + 8, 0:128], b_ref[b, STATS:STATS + 8, 0:128]
        top = jnp.maximum(sa, sb)
        fa, fb = jnp.exp(sa - top), jnp.exp(sb - top)
        denom = sa * pltpu.roll(fa, 4, 1) + sb * pltpu.roll(fb, 4, 1)
        return fa, fb, denom, jnp.where(is_top, top, denom)

    def pairs(side, values):
        if side is None:
            return [pair_row(p) for p in range(GROUP // 2)], values
        rows_of = [pl.multiple_of((STATS + 8) * side + 8 * p, 8) for p in range(GROUP // 4)]
        return rows_of, tuple(jnp.where(side == 1, pltpu.roll(f, 96, 1), f) for f in values)

    def blend(a_ref, a, b_ref, b, found, side, out_ref, out):
        at, (fa, fb) = pairs(side, found[:2])
        for p, r in enumerate(at):
            for t in range(2):
                c = slice(t * 128, t * 128 + 128)
                r8 = pl.ds(r, 8)
                out_ref[out, r8, c] = a_ref[a, r8, c] * spread(fa, p, t) + b_ref[b, r8, c] * spread(fb, p, t)
        out_ref[out, STATS:STATS + 8, 0:128] = found[3]
        out_ref[out, STATS:STATS + 8, 128:256] = zero8

    def finish(a_ref, a, b_ref, b, side, unit):
        found = factors(a_ref, a, b_ref, b)
        at, (fa, fb, denom) = pairs(side, found[:3])
        for p, r in enumerate(at):
            for t in range(2):
                c = slice(t * 128, t * 128 + 128)
                r8 = pl.ds(r, 8)
                w = a_ref[a, r8, c] * spread(fa, p, t) + b_ref[b, r8, c] * spread(fb, p, t)
                base = t * (ctx.shape[0] // 2) + unit * 4 * GROUP + 8 * p
                ctx[base:base + 8, :] = w / spread(denom, p, 2 + t)

    starts = [sum(CHUNKS[:c]) for c in range(len(CHUNKS))]

    def remote(c, kind, src, dst, peer, arrival=None):
        sem = {0: 0, 1: 9 + c}[kind] if isinstance(kind, int) and kind < 2 else kind - 1
        return pltpu.make_async_remote_copy(
            src_ref=src, dst_ref=dst, send_sem=send_sem.at[sem],
            recv_sem=recv_sem.at[c, kind if arrival is None else arrival],
            device_id=device(*peer), device_id_type=MESH)

    units = [max(n // 4, 1) for n in CHUNKS]
    blocks_at = [sum(units[:c]) for c in range(len(CHUNKS))]
    columns = width // 2

    def quarter_rows(c):
        return CHUNKS[c] * GROUP // 4

    def quarters(c):
        return pl.ds(starts[c] * GROUP // 4, quarter_rows(c))

    def to_partner(c):
        n = CHUNKS[c] // 2
        src = own.at[pl.ds(starts[c] + (1 - core) * n, n)]
        return remote(c, 0, src, part.at[pl.ds(starts[c] // 2, n)], (0, 1, 0))

    def over_x(c):
        if CHUNKS[c] < 4:
            at = blocks_at[c], pl.ds(pl.multiple_of(STATS * (1 - x), 8), STATS + 8)
        else:
            at = pl.ds(blocks_at[c], units[c])
        return remote(c, 1, send2.at[at], recv2.at[at], (1, 0, 0))

    def over_y(c):
        return remote(c, 2, away.at[quarters(c)], recv3.at[quarters(c)], (0, 0, 1))

    def home(c, dx, dcore, dtp):
        n = quarter_rows(c)
        at = pl.ds(pl.multiple_of(starts[c] * GROUP + ((core ^ dcore) * 2 + (x ^ dx)) * n, 8), n)
        return total.at[at, pl.ds(pl.multiple_of((tp ^ dtp) * columns, columns), columns)]

    def spread_own(c, kind, peer):
        return remote(c, kind, home(c, 0, 0, 0), home(c, 0, 0, 0), peer)

    def forward(c, kind, origin):
        return remote(c, kind, home(c, *origin), home(c, *origin), (0, 1, 0), 3)

    first_peer, other_peer = (1 - core, 0, core), (core, 0, 1 - core)

    def sent(c):
        copies = [spread_own(c, 4, (1, 0, 0)), spread_own(c, 5, (0, 0, 1)), spread_own(c, 3, (0, 1, 0))]
        if c in DIRECT:
            copies.append(spread_own(c, 6, (1, 0, 1)))
        return copies

    def relay(c):
        return remote(c, 6, home(c, *first_peer), home(c, *first_peer), other_peer)

    def step1(c):
        to_partner(c).start()

    def step2(c):
        n = units[c]
        with jax.named_scope(f'wait2_{c}'):
            to_partner(c).wait_recv()
        work = []
        for dx in (1, 0):
            side = x ^ dx
            for i in range(n):
                if CHUNKS[c] < 4:
                    a, b, half = starts[c] + core, starts[c] // 2, side
                else:
                    a, b, half = starts[c] + (core * 2 + side) * n + i, starts[c] // 2 + side * n + i, None
                work.append((a, b, half, factors(own, a, part, b), (mine, send2)[dx], blocks_at[c] + i))
        for k, (a, b, half, found, out_ref, out) in enumerate(work):
            blend(own, a, part, b, found, half, out_ref, out)
            if k == n - 1:
                over_x(c).start()

    def step3(c):
        if c == 0:
            load_wo(0).wait()
            load_wo(1).wait()
        with jax.named_scope(f'wait3_{c}'):
            over_x(c).wait_recv()
        for i in range(units[c]):
            at = blocks_at[c] + i
            finish(mine, at, recv2, at, x if CHUNKS[c] < 4 else None, i)
        m = quarter_rows(c)
        side = ctx.shape[0] // 2
        lhs = [jnp.concatenate([ctx[pl.ds(t * side + g, m, stride=4), :] for t in range(2)], 1).astype(BF16) for g in range(4)]
        for out_ref, which in ((away, 1 - tp), (keep, tp)):
            for col in range(columns // 256):
                cut = pl.ds(pl.multiple_of(which * columns + col * 256, 256), 256)
                acc = None
                for g in range(4):
                    rhs = jnp.concatenate([wo[h * 256 + g * 64:h * 256 + g * 64 + 64, cut] for h in range(4)], 0)
                    term = jnp.dot(lhs[g], rhs, preferred_element_type=F32)
                    acc = term if acc is None else acc + term
                out_ref[quarters(c), col * 256:col * 256 + 256] = acc
            if out_ref is away:
                over_y(c).start()

    def step4(c):
        with jax.named_scope(f'wait4_{c}'):
            over_y(c).wait_recv()
        home(c, 0, 0, 0)[...] = keep[quarters(c), :] + recv3[quarters(c), :]
        for copy in sent(c):
            copy.start()

    def step5(c):
        with jax.named_scope(f'wait5_{c}'):
            spread_own(c, 4 + core, (0, 1, 0)).wait_recv()
        if c not in DIRECT:
            relay(c).start()
        forward(c, 7 + core, first_peer).start()

    def step6(c):
        with jax.named_scope(f'wait6a_{c}'):
            spread_own(c, 5 - core, (0, 1, 0)).wait_recv()
        forward(c, 8 - core, other_peer).start()
        with jax.named_scope(f'wait6b_{c}'):
            spread_own(c, 6, (0, 1, 0)).wait_recv()
        forward(c, 9, (1, 0, 1)).start()

    def out_copy(c):
        at = pl.ds(starts[c] * GROUP, CHUNKS[c] * GROUP)
        return pltpu.make_async_copy(stage.at[at], out_hbm.at[at], out_sem.at[c])

    def step7(c):
        with jax.named_scope(f'wait7_{c}'):
            four = total.at[pl.ds(starts[c] * GROUP, CHUNKS[c] * GROUP), pl.ds(0, columns)]
            remote(c, 3, four, four, (0, 1, 0)).wait_recv()

        def body(i, _):
            at = pl.ds(pl.multiple_of((starts[c] + i) * GROUP, GROUP), GROUP)
            stage[at, :] = (hid[at, :].astype(F32) + total[at, :]).astype(BF16)
            return 0

        lax.fori_loop(0, CHUNKS[c], body, 0)
        out_copy(c).start()

    def scoped(i, c):
        with jax.named_scope(f'step{i + 1}_{c}'):
            steps[i](c)

    steps = (step1, step2, step3, step4, step5, step6, step7)
    def wait_for(keys, values):
        for g in keys:
            ring_copy(0, g).wait()
        for g in values:
            ring_copy(1, g).wait()

    def refill(which, g):
        @pl.when(g + SLOTS < groups)
        def _():
            ring_copy(which, g + SLOTS).start()

    wait_for((0,), ())
    with jax.named_scope('attend'):
        attend((0, 0), None)
    refill(0, 0)

    def loop(i, _):
        g = 2 * i
        with jax.named_scope('ring_wait'):
            wait_for((g + 1, g + 2), (g, g + 1))
        with jax.named_scope('attend'):
            attend((g + 1, 1), (g, 0))
            attend((g + 2, 0), (g + 1, 1))
        refill(0, g + 1)
        refill(1, g)
        refill(0, g + 2)
        refill(1, g + 1)
        @pl.when(i == 3)
        def _():
            load_wo(0).start()
            load_wo(1).start()

        for when in sorted({e[0] for e in INSIDE}):
            @pl.when(i == when)
            def _():
                for at, c, k in INSIDE:
                    if at == when:
                        scoped(k - 1, c)
        return 0

    trips = groups // 2 - 1
    lax.fori_loop(0, trips, loop, 0)
    last = groups - 2
    with jax.named_scope('ring_wait'):
        wait_for((last + 1,), (last, last + 1))
    with jax.named_scope('attend'):
        attend((last + 1, 1), (last, 0))
        attend(None, (last + 1, 1))
    for c, k in AFTER:
        scoped(k - 1, c)
    with jax.named_scope('finish'):
        remote(0, 0, part, part, (0, 1, 0)).wait_send()
        for kind in range(2, 10):
            remote(0, kind, away, away, (0, 1, 0), 3).wait_send()
        for c in range(len(CHUNKS)):
            over_x(c).wait_send()
            out_copy(c).wait()
        for copy in new_copies:
            copy.wait()


def copy_kernel(*refs):
    n = len(refs) // 4
    sources, results, staged = refs[:n], refs[n:2 * n], refs[2 * n:3 * n]
    sems = refs[3 * n:]
    pieces = []
    for src, dst, mid, sem in zip(sources, results, staged, sems):
        count = src.shape[0] // 64
        for i in range(count):
            at = pl.ds(i * 64, 64)
            pieces.append((pltpu.make_async_copy(src.at[at], mid.at[at], sem.at[i, 0]),
                           pltpu.make_async_copy(mid.at[at], dst.at[at], sem.at[i, 1])))
    for load, _ in pieces:
        load.start()
    for load, save in pieces:
        load.wait()
        save.start()
    for _, save in pieces:
        save.wait()


def solution(mesh):
    def local_step(hidden, ln_gain, ln_bias, w_q, w_k, w_v, w_o, k_cache, v_cache, lengths):
        rows, span, kv_local, head_dim = k_cache.shape
        width = hidden.shape[1]
        kv_width = kv_local * head_dim
        q_width = w_q.shape[1]
        groups = rows // GROUP
        keys = jnp.transpose(k_cache, (0, 2, 3, 1)).reshape(rows, kv_width, span)
        values = jnp.transpose(v_cache, (0, 2, 3, 1)).reshape(rows, kv_width, span)
        half_rot = head_dim // 4
        inv_freq = np.power(10000.0, -2.0 * np.arange(half_rot) / (2 * half_rot)).astype(np.float32)
        inv_freq = jnp.asarray(np.broadcast_to(inv_freq[:, None], (half_rot, 128)).copy())
        vmem = pl.BlockSpec(memory_space=pltpu.VMEM)
        hbm = pl.BlockSpec(memory_space=pl.ANY)
        n = len(CHUNKS)
        out, k_new, v_new = pl.pallas_call(
            attention_kernel,
            out_shape=(jax.ShapeDtypeStruct((rows, width), BF16),
                       jax.ShapeDtypeStruct((kv_width, rows), BF16),
                       jax.ShapeDtypeStruct((kv_width, rows), BF16)),
            in_specs=[hbm] * 12,
            out_specs=(hbm, hbm, hbm),
            scratch_shapes=[
                pltpu.VMEM((kv_width, rows), BF16),
                pltpu.VMEM((kv_width, rows), BF16),
                pltpu.SMEM((rows,), jnp.int32),
                pltpu.VMEM((1, rows), jnp.int32),
                pltpu.VMEM((half_rot, 128), F32),
                pltpu.VMEM((width // 128, 128), BF16),
                pltpu.VMEM((width // 128, 128), BF16),
                pltpu.VMEM((rows, width), BF16),
                pltpu.VMEM((width, q_width), BF16),
                pltpu.VMEM((width, kv_width), BF16),
                pltpu.VMEM((width, kv_width), BF16),
                pltpu.VMEM((q_width, width), BF16),
                pltpu.VMEM((SLOTS, GROUP, kv_width, span), BF16),
                pltpu.VMEM((SLOTS, GROUP, kv_width, span), BF16),
                pltpu.VMEM((rows, width), BF16),
                pltpu.VMEM((rows, 128), F32),
                pltpu.VMEM((rows, 128), F32),
                pltpu.VMEM((16 * PITCH, 128), F32),
                pltpu.VMEM((rows, kv_width), F32),
                pltpu.VMEM((rows, kv_width), F32),
                pltpu.VMEM((2, 16 * GROUP, span), BF16),
                pltpu.VMEM((2, 16 * GROUP, 128), F32),
                pltpu.VMEM((groups, BLOCK, 256), F32),
                pltpu.VMEM((groups // 2, BLOCK, 256), F32),
                pltpu.VMEM((sum(max(c // 4, 1) for c in CHUNKS), BLOCK, 256), F32),
                pltpu.VMEM((sum(max(c // 4, 1) for c in CHUNKS), BLOCK, 256), F32),
                pltpu.VMEM((sum(max(c // 4, 1) for c in CHUNKS), BLOCK, 256), F32),
                pltpu.VMEM((2 * (max(CHUNKS) // 4) * GROUP * 4, 128), F32),
                pltpu.VMEM((rows // 4, width // 2), F32),
                pltpu.VMEM((rows // 4, width // 2), F32),
                pltpu.VMEM((rows // 4, width // 2), F32),
                pltpu.VMEM((rows, width), F32),
                pltpu.SemaphoreType.DMA((SLOTS, 2)),
                pltpu.SemaphoreType.DMA((9 + rows // 128,)),
                pltpu.SemaphoreType.DMA((n,)),
                pltpu.SemaphoreType.DMA((9 + n,)),
                pltpu.SemaphoreType.DMA((n, 7)),
            ],
            compiler_params=pltpu.CompilerParams(
                collective_id=0, has_side_effects=True, vmem_limit_bytes=67043328),
        )(lengths, lengths.reshape(1, rows), inv_freq, ln_gain.reshape(width // 128, 128), ln_bias.reshape(width // 128, 128),
          hidden, w_q, w_k, w_v, w_o, keys, values)
        arrays = (out, k_new, v_new)
        out, k_new, v_new = pl.pallas_call(
            copy_kernel,
            out_shape=[jax.ShapeDtypeStruct(a.shape, a.dtype) for a in arrays],
            in_specs=[hbm] * 3,
            out_specs=[hbm] * 3,
            scratch_shapes=[pltpu.VMEM(a.shape, a.dtype) for a in arrays]
            + [pltpu.SemaphoreType.DMA((a.shape[0] // 64, 2)) for a in arrays],
            compiler_params=pltpu.CompilerParams(vmem_limit_bytes=67043328),
        )(*arrays)
        k_new = jnp.transpose(k_new.reshape(kv_local, head_dim, rows), (2, 0, 1))
        v_new = jnp.transpose(v_new.reshape(kv_local, head_dim, rows), (2, 0, 1))
        return out, k_new, v_new

    row_spec = P('dp', None)
    cache_spec = P('dp', 'sp', 'tp', None)
    head_spec = P('dp', 'tp', None)
    return jax.shard_map(local_step, mesh=mesh, in_specs=(row_spec, P(None), P(None), P(None, 'tp'), P(None, 'tp'), P(None, 'tp'), P('tp', None), cache_spec, cache_spec, P('dp')), out_specs=(row_spec, head_spec, head_spec), check_vma=False)
```

```python
import jax
import jax.numpy as jnp
import numpy as np
from jax import lax
from jax.experimental import pallas as pl
from jax.experimental.pallas import tpu as pltpu
from jax.sharding import PartitionSpec as P

MESH = pl.DeviceIdType.MESH
F32 = jnp.float32
BF16 = jnp.bfloat16
LOWEST = float(jnp.finfo(jnp.float32).min)

GROUP = 16
BLOCK = 4 * GROUP + 8

CHUNKS = (8, 4, 4, 4, 4, 4, 2, 2)
DIRECT = (7,)
INSIDE = ((3, 0, 1), (4, 0, 2), (5, 1, 1), (6, 0, 3), (6, 1, 2), (7, 2, 1), (8, 2, 2), (8, 1, 3), (8, 0, 4), (9, 3, 1),
          (10, 3, 2), (10, 2, 3), (10, 0, 5), (10, 1, 4), (11, 3, 3), (11, 2, 4), (11, 4, 1), (12, 4, 2), (12, 0, 6), (13,
          3, 4), (13, 1, 5), (13, 5, 1), (14, 5, 2), (14, 2, 5), (14, 6, 1))
AFTER = ((3, 5), (7, 1), (4, 3), (6, 2), (7, 2), (5, 3), (3, 6), (1, 6), (4, 4), (6, 3), (7, 3), (2, 6), (5, 4), (1, 7),
         (6, 4), (7, 4), (4, 5), (5, 5), (2, 7), (3, 7), (6, 5), (4, 6), (7, 5), (7, 6), (5, 6), (6, 6), (0, 7), (4, 7),
         (5, 7), (6, 7), (7, 7))
SLOTS = 7
TALL = 256
STATS = 32
PITCH = 520


def attention_kernel(len_hbm, len_row_hbm, inv_freq_hbm, gain_hbm, bias_hbm, hid_hbm, wq_hbm, wk_hbm, wv_hbm, wo_hbm, k_hbm, v_hbm,
                     out_hbm, knt_hbm, vnt_hbm,
                     knt_ref, vnt_ref, len_sm, len_row, inv_freq, gain, bias, hid, wq, wk, wv, wo, kring, vring, stage, cos_t, sin_t, qx, kn, vn,
                     prob, self_w, own, part, send2, mine, recv2, ctx, away, keep, recv3, total,
                     ring_sem, load_sem, out_sem, send_sem, recv_sem):
    rows, width = hid.shape
    groups = rows // GROUP
    span = k_hbm.shape[2]
    tp = lax.axis_index('tp')
    sp = lax.axis_index('sp')
    x, core = sp // 2, sp % 2

    def ring_copy(which, g):
        slot = lax.rem(g, SLOTS)
        src, ring = ((k_hbm, kring), (v_hbm, vring))[which]
        return pltpu.make_async_copy(src.at[pl.ds(g * GROUP, GROUP)], ring.at[slot], ring_sem.at[slot, which])

    blocks = rows // 128

    def load_hid(i):
        at = pl.ds(i * 128, 128)
        return pltpu.make_async_copy(hid_hbm.at[at], hid.at[at], load_sem.at[4 + i])

    load_wk = pltpu.make_async_copy(wk_hbm, wk, load_sem.at[0])
    load_wv = pltpu.make_async_copy(wv_hbm, wv, load_sem.at[1])
    load_wq = pltpu.make_async_copy(wq_hbm, wq, load_sem.at[2])

    def load_wo(i):
        at = pl.ds(i * (wo.shape[0] // 2), wo.shape[0] // 2)
        return pltpu.make_async_copy(wo_hbm.at[at], wo.at[at], load_sem.at[(3, 8 + blocks)[i]])

    small = [pltpu.make_async_copy(src, dst, load_sem.at[4 + blocks + i]) for i, (src, dst) in enumerate(
        ((len_row_hbm, len_row), (inv_freq_hbm, inv_freq), (gain_hbm, gain), (bias_hbm, bias), (len_hbm, len_sm)))]
    for copy in small:
        copy.start()
    for i in range(blocks):
        load_hid(i).start()
    load_wq.start()
    load_wk.start()
    load_wv.start()

    def device(dx, dcore, dtp):
        return {'sp': (x ^ dx) * 2 + (core ^ dcore), 'tp': tp ^ dtp}

    barrier = pltpu.get_barrier_semaphore()
    for peer in ((0, 1, 0), (1, 0, 0), (0, 0, 1), (1, 0, 1)):
        pl.semaphore_signal(barrier, inc=1, device_id=device(*peer), device_id_type=MESH)

    for copy in small:
        copy.wait()
    angle = inv_freq[:, 0:1] * len_row[0:1, :].astype(F32)
    cos_a, sin_a = jnp.cos(angle), jnp.sin(angle)
    one, zero = jnp.ones((32, rows), F32), jnp.zeros((32, rows), F32)
    cos_full = jnp.concatenate([cos_a, cos_a, one] * 2, axis=0)
    sin_full = jnp.concatenate([-sin_a, sin_a, zero] * 2, axis=0)
    for blk in range(rows // 128):
        cut = slice(blk * 128, blk * 128 + 128)
        cos_t[cut, :] = cos_full[:, cut].T
        sin_t[cut, :] = sin_full[:, cut].T

    gain_f, bias_f = gain[...].astype(F32), bias[...].astype(F32)
    gain_f = 1.0 + jnp.concatenate([gain_f[i:i + 1] for i in range(width // 128)], 1)
    bias_f = jnp.concatenate([bias_f[i:i + 1] for i in range(width // 128)], 1)

    def norm(i, _):
        for j in range(4):
            at = pl.ds(pl.multiple_of(i * 64 + j * 16, 16), 16)
            wide = hid[at, :].astype(F32)
            centred = wide - jnp.mean(wide, axis=-1, keepdims=True)
            var = jnp.mean(centred * centred, axis=-1, keepdims=True)
            stage[at, :] = (centred * lax.rsqrt(var + 1e-5) * gain_f + bias_f).astype(BF16)
        return 0

    for i in range(blocks):
        with jax.named_scope(f'load_hid{i}'):
            load_hid(i).wait()
        if i in (1, 3):
            for g in (range(1), range(1, SLOTS))[i // 2]:
                for which in range(2):
                    ring_copy(which, g).start()
        with jax.named_scope('norm'):
            lax.fori_loop(2 * i, 2 * i + 2, norm, 0)

    with jax.named_scope('load_w'):
        load_wk.wait()
        load_wv.wait()
        load_wq.wait()
    lane_rb = lax.broadcasted_iota(jnp.int32, (TALL, 128), 1)
    low_half = lane_rb < 64
    first_rot = (lane_rb % 64) < 16

    def rotate(u, cos_b, sin_b):
        partner = jnp.where(first_rot, pltpu.roll(u, 112, 1), pltpu.roll(u, 16, 1))
        return (u * cos_b + partner * sin_b).astype(BF16).astype(F32)

    def project(i, _):
        start = pl.multiple_of(i * TALL, TALL)
        at = pl.ds(start, TALL)
        normed = stage[at, :]
        cos_b, sin_b = cos_t[at, :], sin_t[at, :]
        for head in range(4):
            q = jnp.dot(normed, wq[:, head * 256:head * 256 + 256], preferred_element_type=F32)
            for j in range(2):
                u = rotate(q[:, j * 128:j * 128 + 128], cos_b, sin_b) * 0.125
                swap = pltpu.roll(u, 64, 1)
                if head % 2 == 0:
                    a, b = jnp.where(low_half, u, 0.0), jnp.where(low_half, swap, 0.0)
                else:
                    a, b = jnp.where(low_half, 0.0, swap), jnp.where(low_half, 0.0, u)
                r = head * 4 + 2 * j
                qx[pl.ds(pl.multiple_of(r * PITCH + start, 8), TALL), :] = a
                qx[pl.ds(pl.multiple_of((r + 1) * PITCH + start, 8), TALL), :] = b
        kp = jnp.dot(normed, wk[...], preferred_element_type=F32)
        vp = jnp.dot(normed, wv[...], preferred_element_type=F32)
        for j in range(2):
            cut = slice(j * 128, j * 128 + 128)
            ku = rotate(kp[:, cut], cos_b, sin_b)
            vu = vp[:, cut].astype(BF16).astype(F32)
            kn[at, cut] = ku
            vn[at, cut] = vu
            knt_ref[cut, at] = ku.T.astype(BF16)
            vnt_ref[cut, at] = vu.T.astype(BF16)
        return 0

    with jax.named_scope('project'):
        lax.fori_loop(0, rows // TALL, project, 0)
    new_copies = [pltpu.make_async_copy(src, dst, load_sem.at[4 + blocks + i]) for i, (src, dst) in enumerate(
        ((knt_ref, knt_hbm), (vnt_ref, vnt_hbm)))]
    for copy in new_copies:
        copy.start()
    with jax.named_scope('barrier'):
        pl.semaphore_wait(barrier, 4)

    lane = lax.broadcasted_iota(jnp.int32, (8, 128), 1)
    row = lax.broadcasted_iota(jnp.int32, (8, 128), 0)
    low = lane < 64
    keep_w = (row < 4) == low
    stat = lane % 8
    even = (lane % 2) == 0
    keep_s = (row < 4) == even
    pair_of = lane // 8
    pos = lax.broadcasted_iota(jnp.int32, (16, span), 1)
    zero8 = jnp.zeros((8, 128), F32)
    first_pos = sp * span

    def pack(a, b, pick, keep):
        same = jnp.where(pick, a, b)
        other = pltpu.roll(jnp.where(pick, b, a), 4, 0)
        return jnp.where(keep, same, other)

    def queries(b):
        qa = qx[pl.ds(b, 8, stride=PITCH), :]
        qb = qx[pl.ds(b + 8 * PITCH, 8, stride=PITCH), :]
        return qa, qb

    def score(g, j):
        qa, qb = queries(g * GROUP + j)
        q = jnp.concatenate([jnp.concatenate([qa, zero8], 1), jnp.concatenate([zero8, qb], 1)], 0).astype(BF16)
        return jnp.dot(q, kring[lax.rem(g, SLOTS), j], preferred_element_type=F32)

    def weigh(g, side, j, s):
        b = g * GROUP + j
        qa, qb = queries(b)
        left = len_sm[b] - first_pos
        s = jnp.where(pos < left, s, -jnp.inf)
        k_self = kn[pl.ds(b, 1), :]
        s_self = jnp.sum(jnp.concatenate([qa * k_self[:, :128], qb * k_self[:, 128:]], 0), axis=1, keepdims=True)
        owner = jnp.logical_and(left >= 0, left < span)
        s_self = s_self + jnp.where(owner, 0.0, -jnp.inf)
        top = jnp.maximum(jnp.maximum(jnp.max(s, axis=1, keepdims=True), s_self), LOWEST)
        w = jnp.exp(s - top)
        w_self = jnp.exp(s_self - top)
        denom = jnp.sum(w, axis=1, keepdims=True) + w_self
        prob[side, 16 * j:16 * j + 16, :] = w.astype(BF16)
        self_w[side, 16 * j:16 * j + 16, :] = jnp.broadcast_to(w_self, (16, 128))
        return jnp.where(stat < 2, top[:8], jnp.where(stat < 4, top[8:], jnp.where(stat < 6, denom[:8], denom[8:])))

    def value(g, side, j):
        v_self = vn[pl.ds(g * GROUP + j, 1), :]
        part_b = lax.dot_general(prob[side, 16 * j:16 * j + 16, :], vring[lax.rem(g, SLOTS), j],
                                 (((1,), (1,)), ((), ())), preferred_element_type=F32)
        ca = part_b[:8, :128] + self_w[side, 16 * j:16 * j + 8, :] * v_self[:, :128]
        cb = part_b[8:, 128:] + self_w[side, 16 * j + 8:16 * j + 16, :] * v_self[:, 128:]
        return ca, cb

    def pair_row(p):
        return 8 * p if 8 * p < STATS else 8 * p + 8

    def attend(score_g, value_g):
        if score_g is not None:
            g, side = score_g
            scores = [score(g, j) for j in range(GROUP)]
            tile = zero8
        for p in range(GROUP // 2):
            if value_g is not None:
                v, vside = value_g
                e, o = value(v, vside, 2 * p), value(v, vside, 2 * p + 1)
                r = pair_row(p)
                own[v, r:r + 8, 0:128] = pack(e[0], o[0], low, keep_w)
                own[v, r:r + 8, 128:256] = pack(e[1], o[1], low, keep_w)
            if score_g is not None:
                e = weigh(g, side, 2 * p, scores[2 * p])
                o = weigh(g, side, 2 * p + 1, scores[2 * p + 1])
                tile = jnp.where(pair_of == p, pack(e, o, even, keep_s), tile)
        if score_g is not None:
            own[g, STATS:STATS + 8, 0:128] = tile
            own[g, STATS:STATS + 8, 128:256] = zero8

    is_top = stat < 4

    def spread(f, p, t):
        c = p * 8 + 2 * t
        return jnp.where(low, jnp.broadcast_to(f[:, c:c + 1], (8, 128)), jnp.broadcast_to(f[:, c + 1:c + 2], (8, 128)))

    def factors(a_ref, a, b_ref, b):
        sa, sb = a_ref[a, STATS:STATS + 8, 0:128], b_ref[b, STATS:STATS + 8, 0:128]
        top = jnp.maximum(sa, sb)
        fa, fb = jnp.exp(sa - top), jnp.exp(sb - top)
        denom = sa * pltpu.roll(fa, 4, 1) + sb * pltpu.roll(fb, 4, 1)
        return fa, fb, denom, jnp.where(is_top, top, denom)

    def pairs(side, values):
        if side is None:
            return [pair_row(p) for p in range(GROUP // 2)], values
        rows_of = [pl.multiple_of((STATS + 8) * side + 8 * p, 8) for p in range(GROUP // 4)]
        return rows_of, tuple(jnp.where(side == 1, pltpu.roll(f, 96, 1), f) for f in values)

    def blend(a_ref, a, b_ref, b, found, side, out_ref, out):
        at, (fa, fb) = pairs(side, found[:2])
        for p, r in enumerate(at):
            for t in range(2):
                c = slice(t * 128, t * 128 + 128)
                r8 = pl.ds(r, 8)
                out_ref[out, r8, c] = a_ref[a, r8, c] * spread(fa, p, t) + b_ref[b, r8, c] * spread(fb, p, t)
        out_ref[out, STATS:STATS + 8, 0:128] = found[3]
        out_ref[out, STATS:STATS + 8, 128:256] = zero8

    def finish(a_ref, a, b_ref, b, side, unit):
        found = factors(a_ref, a, b_ref, b)
        at, (fa, fb, denom) = pairs(side, found[:3])
        for p, r in enumerate(at):
            for t in range(2):
                c = slice(t * 128, t * 128 + 128)
                r8 = pl.ds(r, 8)
                w = a_ref[a, r8, c] * spread(fa, p, t) + b_ref[b, r8, c] * spread(fb, p, t)
                base = t * (ctx.shape[0] // 2) + unit * 4 * GROUP + 8 * p
                ctx[base:base + 8, :] = w / spread(denom, p, 2 + t)

    starts = [sum(CHUNKS[:c]) for c in range(len(CHUNKS))]

    def remote(c, kind, src, dst, peer, arrival=None):
        sem = {0: 0, 1: 9 + c}[kind] if isinstance(kind, int) and kind < 2 else kind - 1
        return pltpu.make_async_remote_copy(
            src_ref=src, dst_ref=dst, send_sem=send_sem.at[sem],
            recv_sem=recv_sem.at[c, kind if arrival is None else arrival],
            device_id=device(*peer), device_id_type=MESH)

    units = [max(n // 4, 1) for n in CHUNKS]
    blocks_at = [sum(units[:c]) for c in range(len(CHUNKS))]
    columns = width // 2

    def quarter_rows(c):
        return CHUNKS[c] * GROUP // 4

    def quarters(c):
        return pl.ds(starts[c] * GROUP // 4, quarter_rows(c))

    def to_partner(c):
        n = CHUNKS[c] // 2
        src = own.at[pl.ds(starts[c] + (1 - core) * n, n)]
        return remote(c, 0, src, part.at[pl.ds(starts[c] // 2, n)], (0, 1, 0))

    def over_x(c):
        if CHUNKS[c] < 4:
            at = blocks_at[c], pl.ds(pl.multiple_of(STATS * (1 - x), 8), STATS + 8)
        else:
            at = pl.ds(blocks_at[c], units[c])
        return remote(c, 1, send2.at[at], recv2.at[at], (1, 0, 0))

    def over_y(c):
        return remote(c, 2, away.at[quarters(c)], recv3.at[quarters(c)], (0, 0, 1))

    def home(c, dx, dcore, dtp):
        n = quarter_rows(c)
        at = pl.ds(pl.multiple_of(starts[c] * GROUP + ((core ^ dcore) * 2 + (x ^ dx)) * n, 8), n)
        return total.at[at, pl.ds(pl.multiple_of((tp ^ dtp) * columns, columns), columns)]

    def spread_own(c, kind, peer):
        return remote(c, kind, home(c, 0, 0, 0), home(c, 0, 0, 0), peer)

    def forward(c, kind, origin):
        return remote(c, kind, home(c, *origin), home(c, *origin), (0, 1, 0), 3)

    first_peer, other_peer = (1 - core, 0, core), (core, 0, 1 - core)

    def sent(c):
        copies = [spread_own(c, 4, (1, 0, 0)), spread_own(c, 5, (0, 0, 1)), spread_own(c, 3, (0, 1, 0))]
        if c in DIRECT:
            copies.append(spread_own(c, 6, (1, 0, 1)))
        return copies

    def relay(c):
        return remote(c, 6, home(c, *first_peer), home(c, *first_peer), other_peer)

    def step1(c):
        to_partner(c).start()

    def step2(c):
        n = units[c]
        with jax.named_scope(f'wait2_{c}'):
            to_partner(c).wait_recv()
        work = []
        for dx in (1, 0):
            side = x ^ dx
            for i in range(n):
                if CHUNKS[c] < 4:
                    a, b, half = starts[c] + core, starts[c] // 2, side
                else:
                    a, b, half = starts[c] + (core * 2 + side) * n + i, starts[c] // 2 + side * n + i, None
                work.append((a, b, half, factors(own, a, part, b), (mine, send2)[dx], blocks_at[c] + i))
        for k, (a, b, half, found, out_ref, out) in enumerate(work):
            blend(own, a, part, b, found, half, out_ref, out)
            if k == n - 1:
                over_x(c).start()

    def step3(c):
        if c == 0:
            load_wo(0).wait()
            load_wo(1).wait()
        with jax.named_scope(f'wait3_{c}'):
            over_x(c).wait_recv()
        for i in range(units[c]):
            at = blocks_at[c] + i
            finish(mine, at, recv2, at, x if CHUNKS[c] < 4 else None, i)
        m = quarter_rows(c)
        side = ctx.shape[0] // 2
        lhs = [jnp.concatenate([ctx[pl.ds(t * side + g, m, stride=4), :] for t in range(2)], 1).astype(BF16) for g in range(4)]
        for out_ref, which in ((away, 1 - tp), (keep, tp)):
            for col in range(columns // 256):
                cut = pl.ds(pl.multiple_of(which * columns + col * 256, 256), 256)
                acc = None
                for g in range(4):
                    rhs = jnp.concatenate([wo[h * 256 + g * 64:h * 256 + g * 64 + 64, cut] for h in range(4)], 0)
                    term = jnp.dot(lhs[g], rhs, preferred_element_type=F32)
                    acc = term if acc is None else acc + term
                out_ref[quarters(c), col * 256:col * 256 + 256] = acc
            if out_ref is away:
                over_y(c).start()

    def step4(c):
        with jax.named_scope(f'wait4_{c}'):
            over_y(c).wait_recv()
        home(c, 0, 0, 0)[...] = keep[quarters(c), :] + recv3[quarters(c), :]
        for copy in sent(c):
            copy.start()

    def step5(c):
        with jax.named_scope(f'wait5_{c}'):
            spread_own(c, 4 + core, (0, 1, 0)).wait_recv()
        if c not in DIRECT:
            relay(c).start()
        forward(c, 7 + core, first_peer).start()

    def step6(c):
        with jax.named_scope(f'wait6a_{c}'):
            spread_own(c, 5 - core, (0, 1, 0)).wait_recv()
        forward(c, 8 - core, other_peer).start()
        with jax.named_scope(f'wait6b_{c}'):
            spread_own(c, 6, (0, 1, 0)).wait_recv()
        forward(c, 9, (1, 0, 1)).start()

    def out_copy(c):
        at = pl.ds(starts[c] * GROUP, CHUNKS[c] * GROUP)
        return pltpu.make_async_copy(stage.at[at], out_hbm.at[at], out_sem.at[c])

    def step7(c):
        with jax.named_scope(f'wait7_{c}'):
            four = total.at[pl.ds(starts[c] * GROUP, CHUNKS[c] * GROUP), pl.ds(0, columns)]
            remote(c, 3, four, four, (0, 1, 0)).wait_recv()

        def body(i, _):
            at = pl.ds(pl.multiple_of((starts[c] + i) * GROUP, GROUP), GROUP)
            stage[at, :] = (hid[at, :].astype(F32) + total[at, :]).astype(BF16)
            return 0

        lax.fori_loop(0, CHUNKS[c], body, 0)
        out_copy(c).start()

    def scoped(i, c):
        with jax.named_scope(f'step{i + 1}_{c}'):
            steps[i](c)

    steps = (step1, step2, step3, step4, step5, step6, step7)
    def wait_for(keys, values):
        for g in keys:
            ring_copy(0, g).wait()
        for g in values:
            ring_copy(1, g).wait()

    def refill(which, g):
        @pl.when(g + SLOTS < groups)
        def _():
            ring_copy(which, g + SLOTS).start()

    wait_for((0,), ())
    with jax.named_scope('attend'):
        attend((0, 0), None)
    refill(0, 0)

    def loop(i, _):
        g = 2 * i
        with jax.named_scope('ring_wait'):
            wait_for((g + 1, g + 2), (g, g + 1))
        with jax.named_scope('attend'):
            attend((g + 1, 1), (g, 0))
            attend((g + 2, 0), (g + 1, 1))
        refill(0, g + 1)
        refill(1, g)
        refill(0, g + 2)
        refill(1, g + 1)
        @pl.when(i == 3)
        def _():
            load_wo(0).start()
            load_wo(1).start()

        for when in sorted({e[0] for e in INSIDE}):
            @pl.when(i == when)
            def _():
                for at, c, k in INSIDE:
                    if at == when:
                        scoped(k - 1, c)
        return 0

    trips = groups // 2 - 1
    lax.fori_loop(0, trips, loop, 0)
    last = groups - 2
    with jax.named_scope('ring_wait'):
        wait_for((last + 1,), (last, last + 1))
    with jax.named_scope('attend'):
        attend((last + 1, 1), (last, 0))
        attend(None, (last + 1, 1))
    for c, k in AFTER:
        scoped(k - 1, c)
    with jax.named_scope('finish'):
        remote(0, 0, part, part, (0, 1, 0)).wait_send()
        for kind in range(2, 10):
            remote(0, kind, away, away, (0, 1, 0), 3).wait_send()
        for c in range(len(CHUNKS)):
            over_x(c).wait_send()
            out_copy(c).wait()
        for copy in new_copies:
            copy.wait()


def copy_kernel(*refs):
    n = len(refs) // 4
    sources, results, staged = refs[:n], refs[n:2 * n], refs[2 * n:3 * n]
    sems = refs[3 * n:]
    pieces = []
    for src, dst, mid, sem in zip(sources, results, staged, sems):
        count = src.shape[0] // 64
        for i in range(count):
            at = pl.ds(i * 64, 64)
            pieces.append((pltpu.make_async_copy(src.at[at], mid.at[at], sem.at[i, 0]),
                           pltpu.make_async_copy(mid.at[at], dst.at[at], sem.at[i, 1])))
    for load, _ in pieces:
        load.start()
    for load, save in pieces:
        load.wait()
        save.start()
    for _, save in pieces:
        save.wait()


def solution(mesh):
    def local_step(hidden, ln_gain, ln_bias, w_q, w_k, w_v, w_o, k_cache, v_cache, lengths):
        rows, span, kv_local, head_dim = k_cache.shape
        width = hidden.shape[1]
        kv_width = kv_local * head_dim
        q_width = w_q.shape[1]
        groups = rows // GROUP
        keys = jnp.transpose(k_cache, (0, 2, 3, 1)).reshape(rows, kv_width, span)
        values = jnp.transpose(v_cache, (0, 2, 3, 1)).reshape(rows, kv_width, span)
        half_rot = head_dim // 4
        inv_freq = np.power(10000.0, -2.0 * np.arange(half_rot) / (2 * half_rot)).astype(np.float32)
        inv_freq = jnp.asarray(np.broadcast_to(inv_freq[:, None], (half_rot, 128)).copy())
        vmem = pl.BlockSpec(memory_space=pltpu.VMEM)
        hbm = pl.BlockSpec(memory_space=pl.ANY)
        n = len(CHUNKS)
        out, k_new, v_new = pl.pallas_call(
            attention_kernel,
            out_shape=(jax.ShapeDtypeStruct((rows, width), BF16),
                       jax.ShapeDtypeStruct((kv_width, rows), BF16),
                       jax.ShapeDtypeStruct((kv_width, rows), BF16)),
            in_specs=[hbm] * 12,
            out_specs=(hbm, hbm, hbm),
            scratch_shapes=[
                pltpu.VMEM((kv_width, rows), BF16),
                pltpu.VMEM((kv_width, rows), BF16),
                pltpu.SMEM((rows,), jnp.int32),
                pltpu.VMEM((1, rows), jnp.int32),
                pltpu.VMEM((half_rot, 128), F32),
                pltpu.VMEM((width // 128, 128), BF16),
                pltpu.VMEM((width // 128, 128), BF16),
                pltpu.VMEM((rows, width), BF16),
                pltpu.VMEM((width, q_width), BF16),
                pltpu.VMEM((width, kv_width), BF16),
                pltpu.VMEM((width, kv_width), BF16),
                pltpu.VMEM((q_width, width), BF16),
                pltpu.VMEM((SLOTS, GROUP, kv_width, span), BF16),
                pltpu.VMEM((SLOTS, GROUP, kv_width, span), BF16),
                pltpu.VMEM((rows, width), BF16),
                pltpu.VMEM((rows, 128), F32),
                pltpu.VMEM((rows, 128), F32),
                pltpu.VMEM((16 * PITCH, 128), F32),
                pltpu.VMEM((rows, kv_width), F32),
                pltpu.VMEM((rows, kv_width), F32),
                pltpu.VMEM((2, 16 * GROUP, span), BF16),
                pltpu.VMEM((2, 16 * GROUP, 128), F32),
                pltpu.VMEM((groups, BLOCK, 256), F32),
                pltpu.VMEM((groups // 2, BLOCK, 256), F32),
                pltpu.VMEM((sum(max(c // 4, 1) for c in CHUNKS), BLOCK, 256), F32),
                pltpu.VMEM((sum(max(c // 4, 1) for c in CHUNKS), BLOCK, 256), F32),
                pltpu.VMEM((sum(max(c // 4, 1) for c in CHUNKS), BLOCK, 256), F32),
                pltpu.VMEM((2 * (max(CHUNKS) // 4) * GROUP * 4, 128), F32),
                pltpu.VMEM((rows // 4, width // 2), F32),
                pltpu.VMEM((rows // 4, width // 2), F32),
                pltpu.VMEM((rows // 4, width // 2), F32),
                pltpu.VMEM((rows, width), F32),
                pltpu.SemaphoreType.DMA((SLOTS, 2)),
                pltpu.SemaphoreType.DMA((9 + rows // 128,)),
                pltpu.SemaphoreType.DMA((n,)),
                pltpu.SemaphoreType.DMA((9 + n,)),
                pltpu.SemaphoreType.DMA((n, 7)),
            ],
            compiler_params=pltpu.CompilerParams(
                collective_id=0, has_side_effects=True, vmem_limit_bytes=67043328),
        )(lengths, lengths.reshape(1, rows), inv_freq, ln_gain.reshape(width // 128, 128), ln_bias.reshape(width // 128, 128),
          hidden, w_q, w_k, w_v, w_o, keys, values)
        arrays = (out, k_new, v_new)
        out, k_new, v_new = pl.pallas_call(
            copy_kernel,
            out_shape=[jax.ShapeDtypeStruct(a.shape, a.dtype) for a in arrays],
            in_specs=[hbm] * 3,
            out_specs=[hbm] * 3,
            scratch_shapes=[pltpu.VMEM(a.shape, a.dtype) for a in arrays]
            + [pltpu.SemaphoreType.DMA((a.shape[0] // 64, 2)) for a in arrays],
            compiler_params=pltpu.CompilerParams(vmem_limit_bytes=67043328),
        )(*arrays)
        k_new = jnp.transpose(k_new.reshape(kv_local, head_dim, rows), (2, 0, 1))
        v_new = jnp.transpose(v_new.reshape(kv_local, head_dim, rows), (2, 0, 1))
        return out, k_new, v_new

    row_spec = P('dp', None)
    cache_spec = P('dp', 'sp', 'tp', None)
    head_spec = P('dp', 'tp', None)
    return jax.shard_map(local_step, mesh=mesh, in_specs=(row_spec, P(None), P(None), P(None, 'tp'), P(None, 'tp'), P(None, 'tp'), P('tp', None), cache_spec, cache_spec, P('dp')), out_specs=(row_spec, head_spec, head_spec), check_vma=False)
```
